32 devices in a mesh: shell: 2 (over x), pix: 16 (over z, y, core).
Axes of the slice: x: 2, y: 2, z: 4, core: 2. Of those that a mesh axis runs over, the one named last changes fastest.
Arguments:
- block_tile: int32 [4, 1024], P('shell'), may hold values from 0 to 2047, as said below
- cell_index: int32 [4, 1024, 512], P('shell', 'pix'), may hold values from 0 to 2047
- masses: bfloat16 [4, 1024, 512], P('shell', 'pix'), may hold values from 0.125 to 8, as said below
- plane_coef: float32 [4], P('shell'), may hold values from 0.1 to 0.4
- plane_dist: float32 [4], P('shell'), may hold values from 0.2 to 1
- source_inv: float32 [4], P('shell'), may hold values from 0.5 to 1
Outputs:
- convergence: float32 [4, 2048, 2048], P('shell', 'pix')
- shear_one: float32 [4, 2048, 2048], P('shell', 'pix')
- shear_two: float32 [4, 2048, 2048], P('shell', 'pix')
The draws below stay inside these ranges and needn't reach their ends.
Inputs may be any that keep to these rules, and one draw needn't show every extreme that they name: `block_tile`: each row is 16 aligned runs of 64 entries, one run per index of pix. The entries of a run are distinct, and at most 8 of them lie in one index's rows of tiles (tile b lies in the rows of index b // 128). In every plane some index receives exactly 8 tiles from every run. `masses`: positive particle weights.
All inputs are finite; a program needn't handle non-finite values.
Results may differ from the reference program's by a relative error of at most 0.0003.
Values sent between devices are 32-bit elements; how exact they have to be, the bound alone decides.
No kernel may reach another device: no remote copies, remote signals or barrier semaphores. Data moves between devices by JAX's collectives and lax.ppermute only.
A program may use at most 64 MiB of HBM per device.

```python
import math
import jax
import jax.numpy as jnp
from jax import lax

L = 2048
TR = 16
TC = 128
LT = 64
BPT = 4
PLANES = 4
TILES = 2048
TPO = 128
CAP = 8
N_PIX = 16


def draw_block_tile(key, part):
    owners = TILES // TPO
    slot_count = owners * CAP
    key_full = jax.random.fold_in(key, 11)
    key_order = jax.random.fold_in(key, 12)
    key_base = jax.random.fold_in(key, 13)
    full_owner = jax.random.randint(key_full, (PLANES, 1, 1), 0, owners)
    slot_ids = jnp.arange(slot_count)
    scores = jax.random.randint(key_order, (PLANES, owners, slot_count), 0, 1 << 20) * slot_count + slot_ids
    scores = jnp.where((slot_ids // CAP)[None, None, :] == full_owner, scores - (1 << 30), scores)
    chosen = jnp.argsort(scores, axis=-1)[:, :, :LT]
    owner_id = chosen // CAP
    rank_id = chosen % CAP
    base = jax.random.randint(key_base, (PLANES, owners, owners), 0, TPO)
    offset = jnp.take_along_axis(base, owner_id, axis=-1)
    tile_id = owner_id * TPO + (offset + rank_id) % TPO
    return tile_id.reshape(PLANES, owners * LT).astype(jnp.int32)


def draw_masses(key, part):
    owners = TILES // TPO
    scale_key = jax.random.fold_in(key, 21)
    single_key = jax.random.fold_in(key, 22)
    device_scale = jnp.exp(jax.random.uniform(scale_key, (PLANES, owners, 1, 1), jnp.float32, math.log(0.25), math.log(4.0)))
    particle = jnp.exp(jax.random.uniform(single_key, (PLANES, owners, LT, BPT * 128), jnp.float32, math.log(0.5), math.log(2.0)))
    return (device_scale * particle).reshape(PLANES, owners * LT, BPT * 128).astype(jnp.bfloat16)


def place_ends(result, own_key, low, high):
    extent = result.shape
    index_at = [jax.random.randint(jax.random.fold_in(own_key, axis), (), 0, extent[axis]) for axis in range(len(extent))]
    result = result.at[tuple(index_at)].set(low)
    longest = extent.index(max(extent))
    index_at[longest] = (index_at[longest] + 1) % extent[longest]
    return result.at[tuple(index_at)].set(high)


def levels(key, shape, split, least, top_value):
    factor_of = 1.0
    for axis_at, parts in split:
        heights = jax.random.uniform(jax.random.fold_in(jax.random.fold_in(key, 6), axis_at), (parts,), jnp.float32, least / len(split), top_value / len(split))
        factor_of = factor_of * jnp.repeat(jnp.exp(heights), shape[axis_at] // parts).reshape((-1,) + (1,) * (len(shape) - 1 - axis_at))
    return factor_of


def setup_inputs(seed: int = 0) -> dict:
    splits = jax.random.split(jax.random.key(seed), 7)
    return {
        "block_tile": draw_block_tile(jax.random.fold_in(splits[6], 71), 0),
        "cell_index": place_ends(jax.random.randint(splits[1], (PLANES, N_PIX * LT, BPT * 128), 0, TR * TC), jax.random.fold_in(splits[1], 1), 0, (TR * TC) - 1).astype(jnp.int32),
        "masses": draw_masses(jax.random.fold_in(splits[6], 71), 0),
        "plane_coef": jnp.clip(jnp.exp(math.log(0.4) - 1.3862944 * jax.random.uniform(splits[3], (PLANES,), jnp.float32) ** levels(splits[3], (PLANES,), ((0, 2),), -0.2, 0.2)), 0.1, 0.4),
        "plane_dist": jnp.clip(jnp.exp(math.log(1.0) - 1.609438 * jax.random.uniform(splits[4], (PLANES,), jnp.float32) ** levels(splits[4], (PLANES,), ((0, 2),), -0.2, 0.2)), 0.2, 1.0),
        "source_inv": jnp.clip(jnp.exp(math.log(1.0) - 0.6931472 * jax.random.uniform(splits[5], (PLANES,), jnp.float32) ** levels(splits[5], (PLANES,), ((0, 2),), -0.2, 0.2)), 0.5, 1.0),
    }


def reference(block_tile, cell_index, masses, plane_coef, plane_dist, source_inv):
    tiles_wide = L // TC

    def deposit(item):
        tile_ids, cell_ids, weights = item
        tile_col = tile_ids[:, None]
        pixel_row = (tile_col // tiles_wide) * TR + cell_ids // TC
        pixel_col = (tile_col % tiles_wide) * TC + cell_ids % TC
        flat_index = (pixel_row * L + pixel_col).reshape(-1).astype(jnp.int32)
        plane_sum = jnp.zeros((L * L,), jnp.float32).at[flat_index].add(weights.reshape(-1).astype(jnp.float32))
        plane_sum = plane_sum.reshape(L, L)
        mean_mass = jnp.sum(plane_sum) / (L * L)
        return plane_sum / mean_mass - 1.0

    contrast = lax.map(deposit, (block_tile, cell_index, masses))
    near_sum = jnp.cumsum(plane_coef[:, None, None] * contrast, axis=0)
    far_sum = jnp.cumsum((plane_coef * plane_dist)[:, None, None] * contrast, axis=0)
    convergence = near_sum - source_inv[:, None, None] * far_sum

    frequency = jnp.arange(L)
    signed = jnp.where(frequency >= L // 2, frequency - L, frequency).astype(jnp.float32)
    keep_mask = (frequency != L // 2).astype(jnp.float32)
    wave_x = signed[None, :]
    wave_y = signed[:, None]
    wave_power = jnp.maximum(wave_x * wave_x + wave_y * wave_y, 1.0)
    both_keep = keep_mask[None, :] * keep_mask[:, None]
    kernel_one = both_keep * (wave_x * wave_x - wave_y * wave_y) / wave_power
    kernel_two = both_keep * 2.0 * wave_x * wave_y / wave_power

    def shear(field):
        spectrum = jnp.fft.fft2(field)
        first = jnp.real(jnp.fft.ifft2(spectrum * kernel_one)).astype(jnp.float32)
        second = jnp.real(jnp.fft.ifft2(spectrum * kernel_two)).astype(jnp.float32)
        return first, second

    shear_one, shear_two = lax.map(shear, convergence)
    return convergence, shear_one, shear_two
```

```python
from functools import partial
import math

import jax
import jax.numpy as jnp
import numpy as np
from jax import lax
from jax.experimental import pallas as pl
from jax.experimental.pallas import tpu as pltpu
from jax.sharding import PartitionSpec as P

L = 2048
TR = 16
TC = 128


HIGHEST = lax.Precision.HIGHEST


def entering(value, axis, join, neutral):
    count, mine = (lax.axis_size(axis), lax.axis_index(axis))
    pieces = jax.tree.map(lambda part: lax.all_gather(part, axis), value)
    running = jax.tree.map(
        lambda part, zero: jnp.full_like(part, 0) + jnp.asarray(zero, part.dtype), value, neutral
    )

    def lap(position, running):
        longer = join(running, jax.tree.map(lambda part: part[position], pieces))
        return jax.tree.map(lambda new, old: jnp.where(position < mine, new, old), longer, running)

    return lax.fori_loop(0, count - 1, lap, running)


def dft_table(left_size, right_size, period, sign_value):
    left_idx = jnp.arange(left_size)[:, None]
    right_idx = jnp.arange(right_size)[None, :]
    angle = 2.0 * math.pi / period * (left_idx * right_idx % period).astype(jnp.float32)
    return (jnp.cos(angle), sign_value * jnp.sin(angle))


def mix_outer(table, real_part, imag_part):
    cosine, sine_part = table
    contract = partial(jnp.einsum, "ab,...bc->...ac", precision=HIGHEST)
    return (
        contract(cosine, real_part) - contract(sine_part, imag_part),
        contract(sine_part, real_part) + contract(cosine, imag_part),
    )


def mix_inner(table, real_part, imag_part):
    cosine, sine_part = table
    product = partial(jnp.matmul, precision=HIGHEST)
    return (
        product(real_part, cosine) - product(imag_part, sine_part),
        product(real_part, sine_part) + product(imag_part, cosine),
    )


def twist(table, real_part, imag_part):
    cosine, sine_part = table
    return (real_part * cosine - imag_part * sine_part, real_part * sine_part + imag_part * cosine)


def transform_last(real_part, imag_part, sign_value):
    length = real_part.shape[-1]
    inner = math.gcd(length, 128)
    outer = length // inner
    leading = real_part.shape[:-1]
    real_part = real_part.reshape(leading + (outer, inner))
    imag_part = imag_part.reshape(leading + (outer, inner))
    outer_table = dft_table(outer, outer, outer, sign_value)
    inner_table = dft_table(inner, inner, inner, sign_value)
    twiddle = dft_table(outer, inner, length, sign_value)
    if sign_value < 0:
        real_part, imag_part = mix_outer(outer_table, real_part, imag_part)
        real_part, imag_part = twist(twiddle, real_part, imag_part)
        real_part, imag_part = mix_inner(inner_table, real_part, imag_part)
    else:
        real_part, imag_part = mix_inner(inner_table, real_part, imag_part)
        real_part, imag_part = twist(twiddle, real_part, imag_part)
        real_part, imag_part = mix_outer(outer_table, real_part, imag_part)
    return (real_part.reshape(leading + (length,)), imag_part.reshape(leading + (length,)))


def frequency_of(position, length):
    inner = math.gcd(length, 128)
    outer = length // inner
    frequency = position // inner + outer * (position % inner)
    signed = jnp.where(frequency >= length // 2, frequency - length, frequency).astype(jnp.float32)
    keep_mask = (frequency != length // 2).astype(jnp.float32)
    return (signed, keep_mask)


def add_pairs(earlier_pair, later_pair):
    return (earlier_pair[0] + later_pair[0], earlier_pair[1] + later_pair[1])


def deposit_group(item):
    cell_ids, weights = item
    tile_rows = cell_ids // TC
    tile_cols = cell_ids % TC
    row_hot = jnp.where(
        tile_rows[:, None, :] == jnp.arange(TR)[None, :, None],
        weights[:, None, :],
        jnp.zeros((), jnp.bfloat16),
    )
    col_hot = (tile_cols[:, :, None] == jnp.arange(TC)[None, None, :]).astype(jnp.bfloat16)
    return jnp.einsum("grk,gkc->grc", row_hot, col_hot, preferred_element_type=jnp.float32)


def rows_to_sending(packed, groups, slab, cols_own):
    count, fields = (packed.shape[0], packed.shape[1])
    return (
        packed.reshape(count, fields, slab, groups, cols_own)
        .transpose(3, 0, 1, 4, 2)
        .reshape(groups, count, fields, cols_own * slab)
    )


def arrived_to_columns(arrived, groups, slab, cols_own):
    count, fields = (arrived.shape[1], arrived.shape[2])
    return (
        arrived.reshape(groups, count, fields, cols_own, slab)
        .transpose(1, 2, 3, 0, 4)
        .reshape(count, fields, cols_own, groups * slab)
    )


def columns_to_sending(stacked, groups, slab, cols_own):
    count, fields = (stacked.shape[0], stacked.shape[1])
    return (
        stacked.reshape(count, fields, cols_own, groups, slab)
        .transpose(3, 0, 1, 2, 4)
        .reshape(groups, count, fields, cols_own * slab)
    )


def landed_to_rows(landed, groups, slab, cols_own):
    count, fields = (landed.shape[1], landed.shape[2])
    return (
        landed.reshape(groups, count, fields, cols_own, slab)
        .transpose(1, 2, 4, 0, 3)
        .reshape(count, fields, slab, groups * cols_own)
    )


def local(block_tile, cell_index, masses, plane_coef, plane_dist, source_inv):
    groups = lax.axis_size("pix")
    my_index = lax.axis_index("pix")
    planes, local_tiles, per_tile = cell_index.shape
    slab = L // groups
    per_owner = slab // TR * (L // TC)
    cap = max(1, 2 * local_tiles // groups)
    flat = TR * TC
    batch_tiles = 8
    deposited = lax.map(
        deposit_group,
        (cell_index.reshape(-1, batch_tiles, per_tile), masses.reshape(-1, batch_tiles, per_tile)),
    )
    tile_sums = deposited.reshape(planes, local_tiles, flat)
    table = block_tile.reshape(planes, groups, local_tiles)
    owner = table // per_owner
    earlier = jnp.arange(local_tiles)[:, None] < jnp.arange(local_tiles)[None, :]
    same_owner = owner[:, :, :, None] == owner[:, :, None, :]
    rank = jnp.sum(jnp.where(same_owner & earlier[None, None], 1, 0), axis=2)
    slot = owner * cap + rank
    my_slots = lax.dynamic_index_in_dim(slot, my_index, axis=1, keepdims=False)
    slot_grid = jnp.arange(groups)[:, None] * cap + jnp.arange(cap)[None, :]
    send_hot = (my_slots[:, None, None, :] == slot_grid[None, :, :, None]).astype(jnp.float32)
    outgoing = jnp.einsum("pnct,ptf->npcf", send_hot, tile_sums, precision=HIGHEST)
    incoming = lax.all_to_all(outgoing, "pix", split_axis=0, concat_axis=0, tiled=True)
    local_index = table - my_index * per_owner
    is_mine = owner == my_index
    tile_hot = (is_mine[..., None] & (local_index[..., None] == jnp.arange(per_owner))).astype(
        jnp.float32
    )
    slot_hot = (rank[..., None] == jnp.arange(cap)).astype(jnp.float32)
    placing = jnp.einsum("pstl,pstc->plsc", tile_hot, slot_hot, precision=HIGHEST)
    slab_tiles = jnp.einsum("plsc,spcf->plf", placing, incoming, precision=HIGHEST)
    density = (
        slab_tiles.reshape(planes, slab // TR, L // TC, TR, TC)
        .transpose(0, 1, 3, 2, 4)
        .reshape(planes, slab, L)
    )
    total = lax.psum(jnp.sum(density, axis=(1, 2)), "pix")
    contrast = density / (total / (L * L))[:, None, None] - 1.0
    near_local = jnp.cumsum(plane_coef[:, None, None] * contrast, axis=0)
    far_local = jnp.cumsum((plane_coef * plane_dist)[:, None, None] * contrast, axis=0)
    blank = jnp.zeros((slab, L), jnp.float32)
    near_before, far_before = entering(
        (near_local[-1], far_local[-1]), "shell", add_pairs, (blank, blank)
    )
    convergence = near_before + near_local - source_inv[:, None, None] * (far_before + far_local)
    cols_own = L // groups
    wave_x, keep_x = frequency_of(my_index * cols_own + jnp.arange(cols_own), L)
    wave_y, keep_y = frequency_of(jnp.arange(L), L)
    wave_x = wave_x[:, None]
    wave_y = wave_y[None, :]
    both_keep = keep_x[:, None] * keep_y[None, :]
    wave_power = jnp.maximum(wave_x * wave_x + wave_y * wave_y, 1.0)
    kernel_one = both_keep * (wave_x * wave_x - wave_y * wave_y) / wave_power
    kernel_two = both_keep * 2.0 * wave_x * wave_y / wave_power
    scale = 1.0 / (L * L)
    spec_real, spec_imag = transform_last(convergence[0::2], convergence[1::2], -1.0)
    sending = rows_to_sending(jnp.stack([spec_real, spec_imag], axis=1), groups, slab, cols_own)
    arrived = lax.all_to_all(sending, "pix", split_axis=0, concat_axis=0, tiled=True)
    columns = arrived_to_columns(arrived, groups, slab, cols_own)
    row_real, row_imag = transform_last(columns[:, 0], columns[:, 1], -1.0)
    first_real, first_imag = transform_last(row_real * kernel_one, row_imag * kernel_one, 1.0)
    second_real, second_imag = transform_last(row_real * kernel_two, row_imag * kernel_two, 1.0)
    stacked = jnp.stack([first_real, first_imag, second_real, second_imag], axis=1)
    landed = lax.all_to_all(
        columns_to_sending(stacked, groups, slab, cols_own),
        "pix",
        split_axis=0,
        concat_axis=0,
        tiled=True,
    )
    row_layout = landed_to_rows(landed, groups, slab, cols_own)
    even_one, odd_one = transform_last(row_layout[:, 0], row_layout[:, 1], 1.0)
    even_two, odd_two = transform_last(row_layout[:, 2], row_layout[:, 3], 1.0)
    shear_one = jnp.stack([even_one, odd_one], axis=1).reshape(planes, slab, L)
    shear_two = jnp.stack([even_two, odd_two], axis=1).reshape(planes, slab, L)
    return (convergence, shear_one * scale, shear_two * scale)


def bf16_pair(value):
    high = value.astype(jnp.bfloat16)
    return (high, (value - high.astype(jnp.float32)).astype(jnp.bfloat16))


def dft_block(size, sign_value):
    turn = 2.0 * np.pi / size * (np.outer(np.arange(size), np.arange(size)) % size)
    cosine, sine = (np.cos(turn), sign_value * np.sin(turn))
    whole = np.block([[cosine, sine], [-sine, cosine]]).astype(np.float32)
    high = whole.astype(jnp.bfloat16)
    low = (whole - high.astype(np.float32)).astype(jnp.bfloat16)
    return np.stack([high, low])


def twiddle_pair(outer, inner):
    turn = 2.0 * np.pi / (outer * inner) * np.outer(np.arange(outer), np.arange(inner))
    return np.stack([np.cos(turn), np.sin(turn)]).astype(np.float32)


def quarter(values, sign_value):
    (ar, ai), (br, bi), (cr, ci), (dr, di) = values
    pr, pi, mr, mi = (ar + cr, ai + ci, ar - cr, ai - ci)
    qr, qi, nr, ni = (br + dr, bi + di, br - dr, bi - di)
    if sign_value < 0:
        return [(pr + qr, pi + qi), (mr + ni, mi - nr), (pr - qr, pi - qi), (mr - ni, mi + nr)]
    return [(pr + qr, pi + qi), (mr - ni, mi + nr), (pr - qr, pi - qi), (mr + ni, mi - nr)]


def rotate(value, step, sign_value):
    real_part, imag_part = value
    if step == 0:
        return value
    if step == 4:
        return (-sign_value * imag_part, sign_value * real_part)
    cosine = math.cos(2.0 * math.pi * step / 16)
    sine = sign_value * math.sin(2.0 * math.pi * step / 16)
    return (real_part * cosine - imag_part * sine, real_part * sine + imag_part * cosine)


def sixteen(values, sign_value):
    inner = [quarter([values[4 * a + b] for a in range(4)], sign_value) for b in range(4)]
    result = [None] * 16
    for k in range(4):
        turned = [rotate(inner[b][k], b * k, sign_value) for b in range(4)]
        for place, value in enumerate(quarter(turned, sign_value)):
            result[k + 4 * place] = value
    return result


def dot3(left, right, left_is_table):
    mul = partial(jnp.dot, preferred_element_type=jnp.float32)
    (lh, ll), (rh, rl) = (left, right)
    return mul(lh, rh) + (mul(ll, rh) + mul(lh, rl))


def pack_kernel(groups, cap, chunks, per_owner, me_ref, table_ref, cell_ref, mass_ref, out_ref, count_ref, cell_f, mass_f):
    planes, local_tiles, per_tile = cell_ref.shape
    out_ref[...] = jnp.zeros(out_ref.shape, jnp.float32)
    cell_f[...] = cell_ref[...].astype(jnp.float32)
    mass_f[...] = mass_ref[...].astype(jnp.float32)
    base = me_ref[0] * local_tiles
    for plane in range(planes):

        @pl.loop(0, groups)
        def _(slot):
            count_ref[slot] = 0

        @pl.loop(0, local_tiles // 8)
        def _(bunch):
            lists = [source[plane, pl.ds(pl.multiple_of(bunch * 8, 8), 8), :] for source in (cell_f, mass_f)]
            for at in range(8):
                owner = lax.div(table_ref[plane, base + bunch * 8 + at], per_owner)
                rank = count_ref[owner]
                count_ref[owner] = rank + 1
                for kind, values in enumerate(lists):
                    for chunk in range(chunks):
                        row = (2 * plane + kind) * chunks * cap + chunk * cap + rank
                        out_ref[owner, pl.ds(row, 1), :] = values[at : at + 1, chunk * TC : (chunk + 1) * TC]

        total = jnp.sum(mass_f[plane], axis=0, keepdims=True)
        total = jnp.sum(total, axis=1, keepdims=True)
        line = jnp.broadcast_to(total, (1, TC))
        for owner in range(groups):
            out_ref[owner, planes * 2 * chunks * cap + plane : planes * 2 * chunks * cap + plane + 1, :] = line


def deposit_kernel(cap, chunks, slots_ref, recv_ref, out_ref):
    planes = out_ref.shape[0]
    groups = recv_ref.shape[0]
    out_ref[...] = jnp.zeros(out_ref.shape, jnp.float32)
    low = lax.broadcasted_iota(jnp.int32, (TR, TC), 0).astype(jnp.float32)
    lines = [(low + float(TR * part)).astype(jnp.bfloat16) for part in range(TC // TR)]
    one = jnp.ones((TR, TC), jnp.bfloat16)
    none = jnp.zeros((TR, TC), jnp.bfloat16)

    def spread(value, slot):
        return jnp.broadcast_to(value[slot : slot + 1, :], (TR, TC)).astype(jnp.bfloat16)

    for plane in range(planes):

        @pl.loop(0, groups)
        def _(source):
            start = plane * 2 * chunks * cap
            cells = [recv_ref[source, start + k * cap : start + (k + 1) * cap, :] for k in range(chunks)]
            start = start + chunks * cap
            weights = [recv_ref[source, start + k * cap : start + (k + 1) * cap, :] for k in range(chunks)]
            rows = [jnp.floor(cell * (1.0 / TC)) for cell in cells]
            cols = [cell - row * float(TC) for cell, row in zip(cells, rows)]
            sums = []
            for slot in range(cap):
                row_hot = [
                    jnp.where(lines[0] == spread(rows[k], slot), spread(weights[k], slot), none) for k in range(chunks)
                ]
                col_hot = []
                for k in range(chunks):
                    col = spread(cols[k], slot)
                    col_hot.append(jnp.concatenate([jnp.where(line == col, one, none) for line in lines], axis=0))
                sums.append(
                    lax.dot_general(
                        jnp.concatenate(row_hot, axis=1),
                        jnp.concatenate(col_hot, axis=1),
                        (((1,), (1,)), ((), ())),
                        preferred_element_type=jnp.float32,
                    )
                )
            for slot in range(cap):
                tile = slots_ref[(plane * groups + source) * cap + slot]
                out_ref[plane, tile] = out_ref[plane, tile] + sums[slot]


def rows_kernel(parts, weight_ref, *refs):
    dens = refs[:parts]
    totals = refs[parts : 2 * parts]
    twiddle_ref, table_ref, conv_ref, out_ref, high_ref, low_ref = refs[2 * parts :]
    planes, slab, length = conv_ref.shape
    outer = length // TC
    scales = []
    for part in range(parts):
        total = jnp.sum(totals[part][...], axis=0)
        total = jnp.where(total > 0.0, total, 1.0)
        scales.append(float(length * length) / total)
    factors = [
        [
            jnp.broadcast_to(weight_ref[i, part * planes + j] * scales[part][j : j + 1, :], (TR, TC))
            for part in range(parts)
            for j in range(planes)
        ]
        for i in range(planes)
    ]
    shift = [weight_ref[i, parts * planes] for i in range(planes)]

    @pl.loop(0, slab // TR)
    def _(line):
        values = []
        here = pl.ds(line * TR, TR)
        for col in range(outer):
            tiles = [dens[part][j, line * outer + col] for part in range(parts) for j in range(planes)]
            pair = []
            for i in range(planes):
                field = tiles[0] * factors[i][0]
                for tile, factor in zip(tiles[1:], factors[i][1:]):
                    field = field + tile * factor
                field = field - shift[i]
                conv_ref[i, here, col * TC : (col + 1) * TC] = field
                pair.append(field)
            values.append(tuple(pair))
        for place, (real_part, imag_part) in enumerate(sixteen(values, -1.0)):
            if place:
                cosine = twiddle_ref[0, place : place + 1, :]
                sine = twiddle_ref[1, place : place + 1, :]
                real_part, imag_part = (
                    real_part * cosine + imag_part * sine,
                    imag_part * cosine - real_part * sine,
                )
            for at, value in enumerate((real_part, imag_part)):
                high, low = bf16_pair(value)
                high_ref[place, here, at * TC : (at + 1) * TC] = high
                low_ref[place, here, at * TC : (at + 1) * TC] = low

    table = (table_ref[0], table_ref[1])
    for place in range(outer):
        done = dot3((high_ref[place], low_ref[place]), table, False)
        out_ref[place, 0] = done[:, :TC]
        out_ref[place, 1] = done[:, TC:]


def columns_kernel(me_ref, in_ref, turn_ref, forward_ref, back_ref, out_ref, high_ref, low_ref, back_f):
    outer, _, inner, lanes = in_ref.shape
    length = outer * inner

    def turned(place, here, value, sign_value):
        if place == 0:
            return value
        real_part, imag_part = value
        cosine = jnp.broadcast_to(turn_ref[0, here, place : place + 1], (TR, lanes))
        sine = jnp.broadcast_to(turn_ref[1, here, place : place + 1], (TR, lanes)) * sign_value
        return (real_part * cosine - imag_part * sine, real_part * sine + imag_part * cosine)

    @pl.loop(0, inner // TR)
    def _(line):
        here = pl.ds(line * TR, TR)
        there = pl.ds(inner + line * TR, TR)
        values = [(in_ref[place, 0, here, :], in_ref[place, 1, here, :]) for place in range(outer)]
        for place, value in enumerate(sixteen(values, -1.0)):
            real_part, imag_part = turned(place, here, value, -1.0)
            for spot, part in ((here, real_part), (there, imag_part)):
                high, low = bf16_pair(part)
                high_ref[spot, place * lanes : (place + 1) * lanes] = high
                low_ref[spot, place * lanes : (place + 1) * lanes] = low

    forward = (forward_ref[0], forward_ref[1])
    back = (back_ref[0], back_ref[1])
    half = length // 2
    wave_v = lax.broadcasted_iota(jnp.int32, (inner, lanes), 1) * outer + me_ref[0]
    keep_v = wave_v != half
    sv = jnp.where(wave_v >= half, wave_v - length, wave_v).astype(jnp.float32)
    line_u = lax.broadcasted_iota(jnp.int32, (inner, lanes), 0) * outer
    for pair in range(outer // 2):
        span = slice(pair * 2 * lanes, (pair + 1) * 2 * lanes)
        spectrum = dot3(forward, (high_ref[:, span], low_ref[:, span]), True)
        for at in range(2):
            place = 2 * pair + at
            real_part = spectrum[:inner, at * lanes : (at + 1) * lanes]
            imag_part = spectrum[inner:, at * lanes : (at + 1) * lanes]
            wave_u = line_u + place
            su = jnp.where(wave_u >= half, wave_u - length, wave_u).astype(jnp.float32)
            keep = jnp.where(keep_v & (wave_u != half), 1.0 / (float(length) * float(length)), 0.0)
            factor = keep / jnp.maximum(sv * sv + su * su, 1.0)
            first = factor * (sv * sv - su * su)
            second = factor * (2.0 * sv * su)
            stacked = jnp.concatenate(
                [
                    jnp.concatenate([real_part * first, real_part * second], axis=1),
                    jnp.concatenate([imag_part * first, imag_part * second], axis=1),
                ],
                axis=0,
            )
            back_f[place] = dot3(back, bf16_pair(stacked), True)

    @pl.loop(0, inner // TR)
    def _(line):
        here = pl.ds(line * TR, TR)
        there = pl.ds(inner + line * TR, TR)
        for field in range(2):
            side = slice(field * lanes, (field + 1) * lanes)
            values = [
                turned(place, here, (back_f[place, here, side], back_f[place, there, side]), 1.0)
                for place in range(outer)
            ]
            for place, (real_part, imag_part) in enumerate(sixteen(values, 1.0)):
                out_ref[place, 2 * field, here, :] = real_part
                out_ref[place, 2 * field + 1, here, :] = imag_part


def inverse_rows_kernel(in_ref, twiddle_ref, table_ref, first_ref, second_ref, back_f):
    outer, _, slab, lanes = in_ref.shape
    table = (table_ref[0], table_ref[1])
    for field, out_ref in enumerate((first_ref, second_ref)):
        for place in range(outer):
            joined = jnp.concatenate([in_ref[place, 2 * field], in_ref[place, 2 * field + 1]], axis=1)
            back_f[place] = dot3(bf16_pair(joined), table, False)

        @pl.loop(0, slab // TR)
        def _(line):
            here = pl.ds(line * TR, TR)
            values = []
            for place in range(outer):
                real_part = back_f[place, here, :lanes]
                imag_part = back_f[place, here, lanes:]
                if place:
                    cosine = twiddle_ref[0, place : place + 1, :]
                    sine = twiddle_ref[1, place : place + 1, :]
                    real_part, imag_part = (
                        real_part * cosine - imag_part * sine,
                        real_part * sine + imag_part * cosine,
                    )
                values.append((real_part, imag_part))
            for place, (real_part, imag_part) in enumerate(sixteen(values, 1.0)):
                out_ref[0, here, place * lanes : (place + 1) * lanes] = real_part
                out_ref[1, here, place * lanes : (place + 1) * lanes] = imag_part


VMEM = pl.BlockSpec(memory_space=pltpu.VMEM)
SMEM = pl.BlockSpec(memory_space=pltpu.SMEM)
ROOM = pltpu.CompilerParams(vmem_limit_bytes=48 * 1024 * 1024)


def slot_tiles(table, me, per_owner, cap):
    local_tiles = table.shape[-1]
    mine = table // per_owner == me
    earlier = jnp.arange(local_tiles)[:, None] < jnp.arange(local_tiles)[None, :]
    rank = jnp.sum(jnp.where(mine[..., :, None] & earlier, 1, 0), axis=-2)
    chosen = mine[..., None, :] & (rank[..., None, :] == jnp.arange(cap)[:, None])
    spot = table - me * per_owner
    return jnp.sum(jnp.where(chosen, spot[..., None, :], 0), axis=-1).reshape(-1)


def local_tiled(block_tile, cell_index, masses, plane_coef, plane_dist, source_inv):
    groups = lax.axis_size("pix")
    shells = lax.axis_size("shell")
    me = lax.axis_index("pix")
    planes, local_tiles, per_tile = cell_index.shape
    slab = L // groups
    outer = L // TC
    per_owner = slab // TR * outer
    cap = max(1, 2 * local_tiles // groups)
    chunks = per_tile // TC
    lines = planes * 2 * chunks * cap
    me_list = me.reshape(1).astype(jnp.int32)

    sent = pl.pallas_call(
        partial(pack_kernel, groups, cap, chunks, per_owner),
        in_specs=[SMEM, SMEM, VMEM, VMEM],
        out_specs=VMEM,
        out_shape=jax.ShapeDtypeStruct((groups, lines + 8, TC), jnp.float32),
        scratch_shapes=[
            pltpu.SMEM((groups,), jnp.int32),
            pltpu.VMEM(cell_index.shape, jnp.float32),
            pltpu.VMEM(cell_index.shape, jnp.float32),
        ],
        compiler_params=ROOM,
        name="pack",
    )(me_list, block_tile, cell_index, masses)
    recv = lax.all_to_all(sent, "pix", split_axis=0, concat_axis=0, tiled=True)
    near_of = plane_coef
    far_of = plane_coef * plane_dist
    note = jnp.concatenate([block_tile.astype(jnp.float32), near_of[:, None], far_of[:, None]], axis=1)

    own = jnp.arange(planes)
    until = own[None, :] <= own[:, None]
    weights = [jnp.where(until, near_of[None, :] - source_inv[:, None] * far_of[None, :], 0.0)]
    arrivals = [recv]
    slots = [slot_tiles(block_tile.reshape(planes, groups, local_tiles), me, per_owner, cap)]
    for step in range(1, shells):
        pairs = [(at, at + step) for at in range(shells - step)]
        other = lax.ppermute(note, "shell", pairs)
        arrivals.append(lax.ppermute(recv, "shell", pairs))
        tiles = other[:, : groups * local_tiles].astype(jnp.int32).reshape(planes, groups, local_tiles)
        slots.append(slot_tiles(tiles, me, per_owner, cap))
        weights.append(other[:, -2][None, :] - source_inv[:, None] * other[:, -1][None, :])
    weight = jnp.concatenate(weights, axis=1)
    weight = jnp.concatenate([weight, jnp.sum(weight, axis=1, keepdims=True)], axis=1)

    deposit = pl.pallas_call(
        partial(deposit_kernel, cap, chunks),
        in_specs=[SMEM, VMEM],
        out_specs=VMEM,
        out_shape=jax.ShapeDtypeStruct((planes, per_owner, TR, TC), jnp.float32),
        compiler_params=ROOM,
        name="deposit",
    )
    dens = [deposit(spot, arrival) for spot, arrival in zip(slots, arrivals)]
    parts = len(dens)
    totals = [arrival[:, lines:, :] for arrival in arrivals]
    twiddle = jnp.asarray(twiddle_pair(outer, TC))
    forward = jnp.asarray(dft_block(TC, -1.0))
    back = jnp.asarray(dft_block(TC, 1.0))
    convergence, row_sent = pl.pallas_call(
        partial(rows_kernel, parts),
        in_specs=[SMEM] + [VMEM] * (2 * parts + 2),
        out_specs=(VMEM, VMEM),
        out_shape=(
            jax.ShapeDtypeStruct((planes, slab, L), jnp.float32),
            jax.ShapeDtypeStruct((groups, 2, slab, TC), jnp.float32),
        ),
        scratch_shapes=[
            pltpu.VMEM((outer, slab, 2 * TC), jnp.bfloat16),
            pltpu.VMEM((outer, slab, 2 * TC), jnp.bfloat16),
        ],
        compiler_params=ROOM,
        name="rows",
    )(weight, *dens, *totals, twiddle, forward)
    arrived = lax.all_to_all(row_sent, "pix", split_axis=0, concat_axis=0, tiled=True)
    col_sent = pl.pallas_call(
        columns_kernel,
        in_specs=[SMEM] + [VMEM] * 4,
        out_specs=VMEM,
        out_shape=jax.ShapeDtypeStruct((groups, 4, slab, TC), jnp.float32),
        scratch_shapes=[
            pltpu.VMEM((2 * slab, L), jnp.bfloat16),
            pltpu.VMEM((2 * slab, L), jnp.bfloat16),
            pltpu.VMEM((outer, 2 * slab, 2 * TC), jnp.float32),
        ],
        compiler_params=ROOM,
        name="columns",
    )(me_list, arrived, jnp.asarray(twiddle_pair(outer, TC).transpose(0, 2, 1)), back, forward)
    landed = lax.all_to_all(col_sent, "pix", split_axis=0, concat_axis=0, tiled=True)
    shear_one, shear_two = pl.pallas_call(
        inverse_rows_kernel,
        in_specs=[VMEM] * 3,
        out_specs=(VMEM, VMEM),
        out_shape=(
            jax.ShapeDtypeStruct((planes, slab, L), jnp.float32),
            jax.ShapeDtypeStruct((planes, slab, L), jnp.float32),
        ),
        scratch_shapes=[pltpu.VMEM((outer, slab, 2 * TC), jnp.float32)],
        compiler_params=ROOM,
        name="inverse_rows",
    )(landed, twiddle, back)
    return (convergence, shear_one, shear_two)


def solution(mesh):
    placed = (
        P("shell", None),
        P("shell", "pix", None),
        P("shell", "pix", None),
        P("shell"),
        P("shell"),
        P("shell"),
    )
    tiled = mesh.shape["pix"] * TC == L
    return jax.shard_map(
        local_tiled if tiled else local,
        mesh=mesh,
        in_specs=placed,
        out_specs=(P("shell", "pix", None), P("shell", "pix", None), P("shell", "pix", None)),
        check_vma=False,
    )
```

```python
from functools import partial
import math

import jax
import jax.numpy as jnp
import numpy as np
from jax import lax
from jax.experimental import pallas as pl
from jax.experimental.pallas import tpu as pltpu
from jax.sharding import PartitionSpec as P

L = 2048
TR = 16
TC = 128


HIGHEST = lax.Precision.HIGHEST


def entering(value, axis, join, neutral):
    count, mine = (lax.axis_size(axis), lax.axis_index(axis))
    pieces = jax.tree.map(lambda part: lax.all_gather(part, axis), value)
    running = jax.tree.map(
        lambda part, zero: jnp.full_like(part, 0) + jnp.asarray(zero, part.dtype), value, neutral
    )

    def lap(position, running):
        longer = join(running, jax.tree.map(lambda part: part[position], pieces))
        return jax.tree.map(lambda new, old: jnp.where(position < mine, new, old), longer, running)

    return lax.fori_loop(0, count - 1, lap, running)


def dft_table(left_size, right_size, period, sign_value):
    left_idx = jnp.arange(left_size)[:, None]
    right_idx = jnp.arange(right_size)[None, :]
    angle = 2.0 * math.pi / period * (left_idx * right_idx % period).astype(jnp.float32)
    return (jnp.cos(angle), sign_value * jnp.sin(angle))


def mix_outer(table, real_part, imag_part):
    cosine, sine_part = table
    contract = partial(jnp.einsum, "ab,...bc->...ac", precision=HIGHEST)
    return (
        contract(cosine, real_part) - contract(sine_part, imag_part),
        contract(sine_part, real_part) + contract(cosine, imag_part),
    )


def mix_inner(table, real_part, imag_part):
    cosine, sine_part = table
    product = partial(jnp.matmul, precision=HIGHEST)
    return (
        product(real_part, cosine) - product(imag_part, sine_part),
        product(real_part, sine_part) + product(imag_part, cosine),
    )


def twist(table, real_part, imag_part):
    cosine, sine_part = table
    return (real_part * cosine - imag_part * sine_part, real_part * sine_part + imag_part * cosine)


def transform_last(real_part, imag_part, sign_value):
    length = real_part.shape[-1]
    inner = math.gcd(length, 128)
    outer = length // inner
    leading = real_part.shape[:-1]
    real_part = real_part.reshape(leading + (outer, inner))
    imag_part = imag_part.reshape(leading + (outer, inner))
    outer_table = dft_table(outer, outer, outer, sign_value)
    inner_table = dft_table(inner, inner, inner, sign_value)
    twiddle = dft_table(outer, inner, length, sign_value)
    if sign_value < 0:
        real_part, imag_part = mix_outer(outer_table, real_part, imag_part)
        real_part, imag_part = twist(twiddle, real_part, imag_part)
        real_part, imag_part = mix_inner(inner_table, real_part, imag_part)
    else:
        real_part, imag_part = mix_inner(inner_table, real_part, imag_part)
        real_part, imag_part = twist(twiddle, real_part, imag_part)
        real_part, imag_part = mix_outer(outer_table, real_part, imag_part)
    return (real_part.reshape(leading + (length,)), imag_part.reshape(leading + (length,)))


def frequency_of(position, length):
    inner = math.gcd(length, 128)
    outer = length // inner
    frequency = position // inner + outer * (position % inner)
    signed = jnp.where(frequency >= length // 2, frequency - length, frequency).astype(jnp.float32)
    keep_mask = (frequency != length // 2).astype(jnp.float32)
    return (signed, keep_mask)


def add_pairs(earlier_pair, later_pair):
    return (earlier_pair[0] + later_pair[0], earlier_pair[1] + later_pair[1])


def deposit_group(item):
    cell_ids, weights = item
    tile_rows = cell_ids // TC
    tile_cols = cell_ids % TC
    row_hot = jnp.where(
        tile_rows[:, None, :] == jnp.arange(TR)[None, :, None],
        weights[:, None, :],
        jnp.zeros((), jnp.bfloat16),
    )
    col_hot = (tile_cols[:, :, None] == jnp.arange(TC)[None, None, :]).astype(jnp.bfloat16)
    return jnp.einsum("grk,gkc->grc", row_hot, col_hot, preferred_element_type=jnp.float32)


def rows_to_sending(packed, groups, slab, cols_own):
    count, fields = (packed.shape[0], packed.shape[1])
    return (
        packed.reshape(count, fields, slab, groups, cols_own)
        .transpose(3, 0, 1, 4, 2)
        .reshape(groups, count, fields, cols_own * slab)
    )


def arrived_to_columns(arrived, groups, slab, cols_own):
    count, fields = (arrived.shape[1], arrived.shape[2])
    return (
        arrived.reshape(groups, count, fields, cols_own, slab)
        .transpose(1, 2, 3, 0, 4)
        .reshape(count, fields, cols_own, groups * slab)
    )


def columns_to_sending(stacked, groups, slab, cols_own):
    count, fields = (stacked.shape[0], stacked.shape[1])
    return (
        stacked.reshape(count, fields, cols_own, groups, slab)
        .transpose(3, 0, 1, 2, 4)
        .reshape(groups, count, fields, cols_own * slab)
    )


def landed_to_rows(landed, groups, slab, cols_own):
    count, fields = (landed.shape[1], landed.shape[2])
    return (
        landed.reshape(groups, count, fields, cols_own, slab)
        .transpose(1, 2, 4, 0, 3)
        .reshape(count, fields, slab, groups * cols_own)
    )


def local(block_tile, cell_index, masses, plane_coef, plane_dist, source_inv):
    groups = lax.axis_size("pix")
    my_index = lax.axis_index("pix")
    planes, local_tiles, per_tile = cell_index.shape
    slab = L // groups
    per_owner = slab // TR * (L // TC)
    cap = max(1, 2 * local_tiles // groups)
    flat = TR * TC
    batch_tiles = 8
    deposited = lax.map(
        deposit_group,
        (cell_index.reshape(-1, batch_tiles, per_tile), masses.reshape(-1, batch_tiles, per_tile)),
    )
    tile_sums = deposited.reshape(planes, local_tiles, flat)
    table = block_tile.reshape(planes, groups, local_tiles)
    owner = table // per_owner
    earlier = jnp.arange(local_tiles)[:, None] < jnp.arange(local_tiles)[None, :]
    same_owner = owner[:, :, :, None] == owner[:, :, None, :]
    rank = jnp.sum(jnp.where(same_owner & earlier[None, None], 1, 0), axis=2)
    slot = owner * cap + rank
    my_slots = lax.dynamic_index_in_dim(slot, my_index, axis=1, keepdims=False)
    slot_grid = jnp.arange(groups)[:, None] * cap + jnp.arange(cap)[None, :]
    send_hot = (my_slots[:, None, None, :] == slot_grid[None, :, :, None]).astype(jnp.float32)
    outgoing = jnp.einsum("pnct,ptf->npcf", send_hot, tile_sums, precision=HIGHEST)
    incoming = lax.all_to_all(outgoing, "pix", split_axis=0, concat_axis=0, tiled=True)
    local_index = table - my_index * per_owner
    is_mine = owner == my_index
    tile_hot = (is_mine[..., None] & (local_index[..., None] == jnp.arange(per_owner))).astype(
        jnp.float32
    )
    slot_hot = (rank[..., None] == jnp.arange(cap)).astype(jnp.float32)
    placing = jnp.einsum("pstl,pstc->plsc", tile_hot, slot_hot, precision=HIGHEST)
    slab_tiles = jnp.einsum("plsc,spcf->plf", placing, incoming, precision=HIGHEST)
    density = (
        slab_tiles.reshape(planes, slab // TR, L // TC, TR, TC)
        .transpose(0, 1, 3, 2, 4)
        .reshape(planes, slab, L)
    )
    total = lax.psum(jnp.sum(density, axis=(1, 2)), "pix")
    contrast = density / (total / (L * L))[:, None, None] - 1.0
    near_local = jnp.cumsum(plane_coef[:, None, None] * contrast, axis=0)
    far_local = jnp.cumsum((plane_coef * plane_dist)[:, None, None] * contrast, axis=0)
    blank = jnp.zeros((slab, L), jnp.float32)
    near_before, far_before = entering(
        (near_local[-1], far_local[-1]), "shell", add_pairs, (blank, blank)
    )
    convergence = near_before + near_local - source_inv[:, None, None] * (far_before + far_local)
    cols_own = L // groups
    wave_x, keep_x = frequency_of(my_index * cols_own + jnp.arange(cols_own), L)
    wave_y, keep_y = frequency_of(jnp.arange(L), L)
    wave_x = wave_x[:, None]
    wave_y = wave_y[None, :]
    both_keep = keep_x[:, None] * keep_y[None, :]
    wave_power = jnp.maximum(wave_x * wave_x + wave_y * wave_y, 1.0)
    kernel_one = both_keep * (wave_x * wave_x - wave_y * wave_y) / wave_power
    kernel_two = both_keep * 2.0 * wave_x * wave_y / wave_power
    scale = 1.0 / (L * L)
    spec_real, spec_imag = transform_last(convergence[0::2], convergence[1::2], -1.0)
    sending = rows_to_sending(jnp.stack([spec_real, spec_imag], axis=1), groups, slab, cols_own)
    arrived = lax.all_to_all(sending, "pix", split_axis=0, concat_axis=0, tiled=True)
    columns = arrived_to_columns(arrived, groups, slab, cols_own)
    row_real, row_imag = transform_last(columns[:, 0], columns[:, 1], -1.0)
    first_real, first_imag = transform_last(row_real * kernel_one, row_imag * kernel_one, 1.0)
    second_real, second_imag = transform_last(row_real * kernel_two, row_imag * kernel_two, 1.0)
    stacked = jnp.stack([first_real, first_imag, second_real, second_imag], axis=1)
    landed = lax.all_to_all(
        columns_to_sending(stacked, groups, slab, cols_own),
        "pix",
        split_axis=0,
        concat_axis=0,
        tiled=True,
    )
    row_layout = landed_to_rows(landed, groups, slab, cols_own)
    even_one, odd_one = transform_last(row_layout[:, 0], row_layout[:, 1], 1.0)
    even_two, odd_two = transform_last(row_layout[:, 2], row_layout[:, 3], 1.0)
    shear_one = jnp.stack([even_one, odd_one], axis=1).reshape(planes, slab, L)
    shear_two = jnp.stack([even_two, odd_two], axis=1).reshape(planes, slab, L)
    return (convergence, shear_one * scale, shear_two * scale)


def bf16_pair(value):
    high = value.astype(jnp.bfloat16)
    return (high, (value - high.astype(jnp.float32)).astype(jnp.bfloat16))


def dft_block(size, sign_value):
    turn = 2.0 * np.pi / size * (np.outer(np.arange(size), np.arange(size)) % size)
    cosine, sine = (np.cos(turn), sign_value * np.sin(turn))
    whole = np.block([[cosine, sine], [-sine, cosine]]).astype(np.float32)
    high = whole.astype(jnp.bfloat16)
    low = (whole - high.astype(np.float32)).astype(jnp.bfloat16)
    return np.stack([high, low])


def twiddle_pair(outer, inner):
    turn = 2.0 * np.pi / (outer * inner) * np.outer(np.arange(outer), np.arange(inner))
    return np.stack([np.cos(turn), np.sin(turn)]).astype(np.float32)


def quarter(values, sign_value):
    (ar, ai), (br, bi), (cr, ci), (dr, di) = values
    pr, pi, mr, mi = (ar + cr, ai + ci, ar - cr, ai - ci)
    qr, qi, nr, ni = (br + dr, bi + di, br - dr, bi - di)
    if sign_value < 0:
        return [(pr + qr, pi + qi), (mr + ni, mi - nr), (pr - qr, pi - qi), (mr - ni, mi + nr)]
    return [(pr + qr, pi + qi), (mr - ni, mi + nr), (pr - qr, pi - qi), (mr + ni, mi - nr)]


def rotate(value, step, sign_value):
    real_part, imag_part = value
    if step == 0:
        return value
    if step == 4:
        return (-sign_value * imag_part, sign_value * real_part)
    cosine = math.cos(2.0 * math.pi * step / 16)
    sine = sign_value * math.sin(2.0 * math.pi * step / 16)
    return (real_part * cosine - imag_part * sine, real_part * sine + imag_part * cosine)


def sixteen(values, sign_value, count=16):
    inner = [quarter([values[4 * a + b] for a in range(4)], sign_value) for b in range(4)]
    result = [None] * 16
    for k in range(4):
        turned_values = [rotate(inner[b][k], b * k, sign_value) for b in range(4)]
        for place, value in enumerate(quarter(turned_values, sign_value)):
            result[k + 4 * place] = value
    return result[:count]


def dot3(left, right):
    mul = partial(jnp.dot, preferred_element_type=jnp.float32)
    (left_high, left_low), (right_high, right_low) = (left, right)
    return mul(left_high, right_high) + (mul(left_low, right_high) + mul(left_high, right_low))


def widen_kernel(cell_ref, mass_ref, out_ref):
    out_ref[0] = cell_ref[...].astype(jnp.float32)
    out_ref[1] = mass_ref[...].astype(jnp.float32)


def pack_kernel(half, cap, per_owner, from_ref, table_ref, raw_ref, out_ref, count_ref):
    _, planes, local_tiles, per_tile = raw_ref.shape
    groups = out_ref.shape[0]
    chunks = per_tile // TC
    lines = 2 * chunks * cap
    out_ref[...] = jnp.zeros(out_ref.shape, jnp.float32)
    base = from_ref[0] * local_tiles
    for plane in range(planes):

        @pl.loop(0, groups)
        def _(slot):
            count_ref[slot] = 0

        @pl.loop(0, local_tiles // 8)
        def _(bunch):
            here = pl.ds(pl.multiple_of(bunch * 8, 8), 8)
            lists = [raw_ref[kind, plane, here, :] for kind in range(2)]
            for at in range(8):
                owner = lax.div(table_ref[plane, base + bunch * 8 + at], per_owner)
                low = lax.rem(owner, half)
                side = lax.rem(lax.div(owner, half) + lax.rem(low, 2), 2)
                place = side * half + low
                rank = count_ref[place]
                count_ref[place] = rank + 1
                for kind, values in enumerate(lists):
                    for chunk in range(chunks):
                        row = plane * lines + kind * chunks * cap + chunk * cap + rank
                        out_ref[place, pl.ds(row, 1), :] = values[at : at + 1, chunk * TC : (chunk + 1) * TC]

        total = jnp.sum(raw_ref[1, plane], axis=0, keepdims=True)
        total = jnp.sum(total, axis=1, keepdims=True)
        line = jnp.broadcast_to(total, (1, TC))
        for place in range(groups):
            out_ref[place, planes * lines + plane : planes * lines + plane + 1, :] = line


def deposit_kernel(cap, chunks, slots_ref, recv_ref, out_ref):
    out_ref[...] = jnp.zeros(out_ref.shape, jnp.float32)
    all_planes = out_ref.shape[0]
    planes = all_planes // 2
    half = recv_ref.shape[0] // 2
    width = 32
    bunch = 4
    parts = TC // width
    low = lax.broadcasted_iota(jnp.int32, (TR, TC), 0).astype(jnp.float32)
    lines = [(low + float(TR * part)).astype(jnp.bfloat16) for part in range(parts)]
    one = jnp.ones((TR, TC), jnp.bfloat16)
    none = jnp.zeros((TR, TC), jnp.bfloat16)

    def spread(value, slot):
        return jnp.broadcast_to(value[slot : slot + 1, :], (TR, TC)).astype(jnp.bfloat16)

    for plane in range(all_planes):
        start = (plane % planes) * 2 * chunks * cap

        @pl.loop(0, half, unroll=4)
        def _(source):
            place = (plane // planes) * half + source
            cells = [recv_ref[place, start + k * cap : start + (k + 1) * cap, :] for k in range(chunks)]
            weights = [
                recv_ref[place, start + (chunks + k) * cap : start + (chunks + k + 1) * cap, :] for k in range(chunks)
            ]
            rows = [jnp.floor(cell * (1.0 / TC)) for cell in cells]
            strips = [jnp.floor(cell * (1.0 / width)) for cell in cells]
            cols = [cell - strip * float(width) for cell, strip in zip(cells, strips)]
            rows = [row + (strip - row * float(parts)) * float(TR) for row, strip in zip(rows, strips)]
            sums = []
            for first in range(0, cap, bunch):
                row_hot = []
                col_hot = []
                for k in range(chunks):
                    row_lines = []
                    col_lines = []
                    for slot in range(first, first + bunch):
                        row = spread(rows[k], slot)
                        weight = spread(weights[k], slot)
                        row_lines += [jnp.where(lines[at] == row, weight, none) for at in range(parts)]
                        col = spread(cols[k], slot)
                        col_lines += [jnp.where(lines[at] == col, one, none) for at in range(width // TR)]
                    row_hot.append(jnp.concatenate(row_lines, axis=0))
                    col_hot.append(jnp.concatenate(col_lines, axis=0))
                done = lax.dot_general(
                    jnp.concatenate(row_hot, axis=1),
                    jnp.concatenate(col_hot, axis=1),
                    (((1,), (1,)), ((), ())),
                    preferred_element_type=jnp.float32,
                )
                for at in range(bunch):
                    base = at * TR * parts
                    side = slice(at * width, (at + 1) * width)
                    strips_of = [done[base + j * TR : base + (j + 1) * TR, side] for j in range(parts)]
                    sums.append(jnp.concatenate(strips_of, axis=1))
            for slot in range(cap):
                tile = slots_ref[(plane * half + source) * cap + slot]
                out_ref[plane, tile] = out_ref[plane, tile] + sums[slot]


def rows_kernel(
    cap, chunks, weight_ref, side_ref, slots_ref, near_dens_ref, near_ref, far_ref, twiddle_ref, table_ref,
    mine_ref, other_ref, out_ref, high_ref, low_ref, far_dens_ref,
):
    step = pl.program_id(0)
    pl.when(step == 0)(lambda: deposit_kernel(cap, chunks, slots_ref, far_ref, far_dens_ref))
    first_line = 2 * (far_dens_ref.shape[0] // 2) * cap * chunks
    planes, slab, length = mine_ref.shape
    all_planes = far_dens_ref.shape[0]
    outer = length // TC
    first_tile = step * (slab // TR * outer)
    half = near_ref.shape[0] // 2
    scales = []
    for plane in range(all_planes):
        line = plane % planes
        total = jnp.zeros((1, TC), jnp.float32)
        for source in range(half):
            place = (plane // planes) * half + source
            total = total + near_ref[place, line : line + 1, :]
            total = total + far_ref[place, first_line + line : first_line + line + 1, :]
        scales.append(float(length * length) / total)
    table = (table_ref[0], table_ref[1])
    for side, conv_ref in enumerate((mine_ref, other_ref)):
        here_maps = [side * planes + i for i in range(planes)]
        factors = [
            [jnp.broadcast_to(weight_ref[i, j] * scales[j], (TR, TC)) for j in range(all_planes)] for i in here_maps
        ]
        shift = [weight_ref[i, all_planes] for i in here_maps]

        for line in range(slab // TR):
            values = []
            here = slice(line * TR, (line + 1) * TR)
            for col in range(outer):
                at = line * outer + col
                tiles = [near_dens_ref[j, at] + far_dens_ref[j, first_tile + at] for j in range(all_planes)]
                pair = []
                for i in range(planes):
                    field = tiles[0] * factors[i][0]
                    for tile, factor in zip(tiles[1:], factors[i][1:]):
                        field = field + tile * factor
                    field = field - shift[i]
                    conv_ref[i, here, col * TC : (col + 1) * TC] = field
                    pair.append(field)
                values.append(tuple(pair))
            for place, (real_part, imag_part) in enumerate(sixteen(values, -1.0)):
                if place:
                    cosine = twiddle_ref[0, place : place + 1, :]
                    sine = twiddle_ref[1, place : place + 1, :]
                    real_part, imag_part = (
                        real_part * cosine + imag_part * sine,
                        imag_part * cosine - real_part * sine,
                    )
                spot = slice(place * slab + line * TR, place * slab + (line + 1) * TR)
                for at, value in enumerate((real_part, imag_part)):
                    high, low = bf16_pair(value)
                    high_ref[spot, at * TC : (at + 1) * TC] = high
                    low_ref[spot, at * TC : (at + 1) * TC] = low

        base = side_ref[side] * half
        done = dot3((high_ref[...], low_ref[...]), table)
        for place in range(outer):
            here = slice(place * slab, (place + 1) * slab)
            out_ref[base + place // 2, place % 2, 0] = done[here, :TC]
            out_ref[base + place // 2, place % 2, 1] = done[here, TC:]


def turned(turn_ref, place, here, value, sign_value):
    if place == 0:
        return value
    real_part, imag_part = value
    shape = real_part.shape
    cosine = jnp.broadcast_to(turn_ref[0, here, place : place + 1], shape)
    sine = jnp.broadcast_to(turn_ref[1, here, place : place + 1], shape) * sign_value
    return (real_part * cosine - imag_part * sine, real_part * sine + imag_part * cosine)


def columns_kernel(
    order, me_ref, in_ref, turn_ref, forward_ref, back_ref, out_ref, high_ref, low_ref, spectrum_ref, back_f
):
    outer, _, _, inner, lanes = in_ref.shape
    length = outer * inner
    forward = (forward_ref[0], forward_ref[1])
    back = (back_ref[0], back_ref[1])

    @pl.loop(0, inner // TR)
    def _(line):
        here = pl.ds(line * TR, TR)
        there = pl.ds(inner + line * TR, TR)
        values = [(in_ref[place, 0, 0, here, :], in_ref[place, 0, 1, here, :]) for place in order]
        for place, value in enumerate(sixteen(values, -1.0)):
            for spot, part in zip((here, there), turned(turn_ref, place, here, value, -1.0)):
                high, low = bf16_pair(part)
                high_ref[spot, place * lanes : (place + 1) * lanes] = high
                low_ref[spot, place * lanes : (place + 1) * lanes] = low

    for bunch in range(outer // 2):
        span = slice(bunch * 2 * lanes, (bunch + 1) * 2 * lanes)
        spectrum_ref[:, span] = dot3(forward, (high_ref[:, span], low_ref[:, span]))

    middle = length // 2
    wave_v = lax.broadcasted_iota(jnp.int32, (inner, lanes), 1) * outer + (2 * me_ref[0] + pl.program_id(0))
    keep_v = wave_v != middle
    sv = jnp.where(wave_v >= middle, wave_v - length, wave_v).astype(jnp.float32)
    line_u = lax.broadcasted_iota(jnp.int32, (inner, lanes), 0) * outer
    flip = jnp.where(me_ref[1] > 0, -1.0, 1.0)
    for place in range(outer):
        side = slice(place * lanes, (place + 1) * lanes)
        wave_u = line_u + place
        su = jnp.where(wave_u >= middle, wave_u - length, wave_u).astype(jnp.float32)
        scale = 1.0 / (float(length) * float(length))
        keep = jnp.where(keep_v & (wave_u != middle), scale * flip if place % 2 else scale, 0.0)
        factor = keep / jnp.maximum(sv * sv + su * su, 1.0)
        first = factor * (sv * sv - su * su)
        second = factor * (2.0 * sv * su)
        real_part = spectrum_ref[:inner, side]
        imag_part = spectrum_ref[inner:, side]
        stacked = jnp.concatenate(
            [
                jnp.concatenate([real_part * first, real_part * second], axis=1),
                jnp.concatenate([imag_part * first, imag_part * second], axis=1),
            ],
            axis=0,
        )
        back_f[place] = dot3(back, bf16_pair(stacked))

    half = outer // 2

    @pl.loop(0, inner // TR)
    def _(line):
        here = pl.ds(line * TR, TR)
        there = pl.ds(inner + line * TR, TR)
        for field in range(2):
            side = slice(field * lanes, (field + 1) * lanes)
            values = [
                turned(turn_ref, place, here, (back_f[place, here, side], back_f[place, there, side]), 1.0)
                for place in range(outer)
            ]
            for low, (real_part, imag_part) in enumerate(sixteen(values, 1.0, half)):
                out_ref[low, 0, field, 0, here, :] = real_part
                out_ref[low, 0, field, 1, here, :] = imag_part


def inverse_rows_kernel(in_ref, twiddle_ref, table_ref, first_ref, second_ref, back_f):
    half, _, _, _, slab, lanes = in_ref.shape
    outer = 2 * half
    table = (table_ref[0], table_ref[1])
    for field, out_ref in enumerate((first_ref, second_ref)):
        joined = [
            jnp.concatenate([in_ref[place // 2, place % 2, field, part] for place in range(outer)], axis=0)
            for part in range(2)
        ]
        back_f[...] = dot3(bf16_pair(jnp.concatenate(joined, axis=1)), table)
        for line in range(slab // TR):
            here = slice(line * TR, (line + 1) * TR)
            values = []
            for place in range(outer):
                spot = slice(place * slab + line * TR, place * slab + (line + 1) * TR)
                real_part = back_f[spot, :lanes]
                imag_part = back_f[spot, lanes:]
                if place:
                    cosine = twiddle_ref[0, place : place + 1, :]
                    sine = twiddle_ref[1, place : place + 1, :]
                    real_part, imag_part = (
                        real_part * cosine - imag_part * sine,
                        real_part * sine + imag_part * cosine,
                    )
                values.append((real_part, imag_part))
            for place, (real_part, imag_part) in enumerate(sixteen(values, 1.0)):
                out_ref[0, here, place * lanes : (place + 1) * lanes] = real_part
                out_ref[1, here, place * lanes : (place + 1) * lanes] = imag_part


VMEM = pl.BlockSpec(memory_space=pltpu.VMEM)
SMEM = pl.BlockSpec(memory_space=pltpu.SMEM)


def room(mib):
    return pltpu.CompilerParams(vmem_limit_bytes=mib * 1024 * 1024)


def whole(shape):
    return pl.BlockSpec(shape, lambda step: (0,) * len(shape))


def slot_tiles(table, held, per_owner, cap):
    local_tiles = table.shape[-1]
    mine = table // per_owner == held
    earlier = jnp.arange(local_tiles)[:, None] < jnp.arange(local_tiles)[None, :]
    rank = jnp.sum(jnp.where(mine[..., :, None] & earlier, 1, 0), axis=-2)
    chosen = mine[..., None, :] & (rank[..., None, :] == jnp.arange(cap)[:, None])
    spot = table - held * per_owner
    return jnp.sum(jnp.where(chosen, spot[..., None, :], 0), axis=-1)


def cube_exchange(value):
    return lax.all_to_all(value, ("shell", "low"), split_axis=0, concat_axis=0, tiled=True)


def local_cube(block_tile, cell_index, masses, plane_coef, plane_dist, source_inv):
    half = lax.axis_size("low")
    groups = 2 * half
    shell = lax.axis_index("shell")
    upper = lax.axis_index("upper")
    low = lax.axis_index("low")
    planes, local_tiles, per_tile = cell_index.shape
    slab = L // groups
    outer = L // TC
    per_owner = slab // TR * outer
    cap = max(1, 2 * local_tiles // groups)
    chunks = per_tile // TC
    lines = 2 * chunks * cap * planes
    part = (shell + low) % 2
    held = part * half + low
    order = [((s // half + s % 2) % 2) * half + s % half for s in range(groups)]

    raw = pl.pallas_call(
        widen_kernel,
        in_specs=[VMEM, VMEM],
        out_specs=VMEM,
        out_shape=jax.ShapeDtypeStruct((2, planes, local_tiles, per_tile), jnp.float32),
        compiler_params=room(8),
        name="widen",
    )(cell_index, masses)
    raw_far = lax.ppermute(raw, "upper", [(0, 1), (1, 0)])

    def pack(source, lists):
        return pl.pallas_call(
            partial(pack_kernel, half, cap, per_owner),
            in_specs=[SMEM, SMEM, VMEM],
            out_specs=VMEM,
            out_shape=jax.ShapeDtypeStruct((groups, lines + 8, TC), jnp.float32),
            scratch_shapes=[pltpu.SMEM((groups,), jnp.int32)],
            compiler_params=room(12),
            name="pack",
        )(source.reshape(1).astype(jnp.int32), block_tile, lists)

    near = cube_exchange(pack(upper * half + low, raw))
    far = cube_exchange(pack((1 - upper) * half + low, raw_far))

    note = jnp.concatenate(
        [block_tile.astype(jnp.float32), plane_coef[:, None], (plane_coef * plane_dist)[:, None], source_inv[:, None]],
        axis=1,
    )
    other = lax.ppermute(note, "shell", [(0, 1), (1, 0)])
    both = jnp.where(shell == 0, jnp.concatenate([note, other]), jnp.concatenate([other, note]))
    tiles = slot_tiles(
        both[:, : groups * local_tiles].astype(jnp.int32).reshape(2 * planes, groups, local_tiles), held, per_owner, cap
    )
    tiles = tiles.reshape(2 * planes, 2, half, cap)
    near_slots = lax.dynamic_index_in_dim(tiles, upper, axis=1, keepdims=False).reshape(-1)
    far_slots = lax.dynamic_index_in_dim(tiles, 1 - upper, axis=1, keepdims=False).reshape(-1)
    maps = jnp.concatenate([shell * planes + jnp.arange(planes), (1 - shell) * planes + jnp.arange(planes)])
    inverse = jnp.concatenate([note[:, -1], other[:, -1]])
    weight = jnp.where(
        jnp.arange(2 * planes)[None, :] <= maps[:, None], both[None, :, -3] - inverse[:, None] * both[None, :, -2], 0.0
    )
    weight = jnp.concatenate([weight, jnp.sum(weight, axis=1, keepdims=True)], axis=1)

    near_dens = pl.pallas_call(
        partial(deposit_kernel, cap, chunks),
        in_specs=[SMEM, VMEM],
        out_specs=VMEM,
        out_shape=pltpu.HBM((2 * planes, per_owner, TR, TC), jnp.float32),
        compiler_params=room(16),
        name="deposit",
    )(near_slots, near)
    twiddle = jnp.asarray(twiddle_pair(outer, TC))
    turn = jnp.asarray(twiddle_pair(outer, TC).transpose(0, 2, 1))
    minus = jnp.asarray(dft_block(TC, -1.0))
    plus = jnp.asarray(dft_block(TC, 1.0))
    field = jax.ShapeDtypeStruct((planes, slab, L), jnp.float32)
    some = 2 * TR
    conv_mine, conv_other, row_sent = pl.pallas_call(
        partial(rows_kernel, cap, chunks),
        grid=(slab // some,),
        in_specs=[
            SMEM,
            SMEM,
            SMEM,
            pl.BlockSpec((2 * planes, some // TR * outer, TR, TC), lambda step: (0, step, 0, 0)),
            pl.BlockSpec((groups, 8, TC), lambda step: (0, lines // 8, 0)),
            whole(far.shape),
            whole(twiddle.shape),
            whole(minus.shape),
        ],
        out_specs=(
            pl.BlockSpec((planes, some, L), lambda step: (0, step, 0)),
            pl.BlockSpec((planes, some, L), lambda step: (0, step, 0)),
            pl.BlockSpec((groups, 2, 2, some, TC), lambda step: (0, 0, 0, step, 0)),
        ),
        out_shape=(
            pltpu.HBM(field.shape, field.dtype),
            pltpu.HBM(field.shape, field.dtype),
            pltpu.HBM((groups, 2, 2, slab, TC), jnp.float32),
        ),
        scratch_shapes=[
            pltpu.VMEM((outer * some, 2 * TC), jnp.bfloat16),
            pltpu.VMEM((outer * some, 2 * TC), jnp.bfloat16),
            pltpu.VMEM((2 * planes, per_owner, TR, TC), jnp.float32),
        ],
        compiler_params=room(28),
        name="rows",
    )(weight, jnp.stack([shell, 1 - shell]).astype(jnp.int32), far_slots, near_dens, near, far, twiddle, minus)
    arrived = lax.all_to_all(row_sent, ("shell", "low"), split_axis=0, concat_axis=0, tiled=True)
    swaps = []
    for side in range(2):
        for top in range(2):
            for at in range(half):
                if (side + at) % 2 == top:
                    swaps.append(((side * 2 + top) * half + at, ((1 - side) * 2 + top) * half + at))
    conv_held = lax.ppermute(conv_other, ("shell", "upper", "low"), swaps)
    convergence = jnp.where(part == upper, conv_mine, conv_held)
    col_sent = pl.pallas_call(
        partial(columns_kernel, order),
        grid=(2,),
        in_specs=[
            SMEM,
            pl.BlockSpec((groups, 1, 2, slab, TC), lambda step: (0, step, 0, 0, 0)),
            whole(turn.shape),
            whole(plus.shape),
            whole(minus.shape),
        ],
        out_specs=pl.BlockSpec((half, 1, 2, 2, slab, TC), lambda step: (0, step, 0, 0, 0, 0)),
        out_shape=pltpu.HBM((half, 2, 2, 2, slab, TC), jnp.float32),
        scratch_shapes=[
            pltpu.VMEM((2 * slab, L), jnp.bfloat16),
            pltpu.VMEM((2 * slab, L), jnp.bfloat16),
            pltpu.VMEM((2 * slab, L), jnp.float32),
            pltpu.VMEM((outer, 2 * slab, 2 * TC), jnp.float32),
        ],
        compiler_params=room(32),
        name="columns",
    )(jnp.stack([low, upper]).astype(jnp.int32), arrived, turn, plus, minus)
    landed = lax.all_to_all(col_sent, "low", split_axis=0, concat_axis=0, tiled=True)
    shear_one, shear_two = pl.pallas_call(
        inverse_rows_kernel,
        grid=(slab // some,),
        in_specs=[
            pl.BlockSpec((half, 2, 2, 2, some, TC), lambda step: (0, 0, 0, 0, step, 0)),
            whole(twiddle.shape),
            whole(plus.shape),
        ],
        out_specs=(
            pl.BlockSpec((planes, some, L), lambda step: (0, step, 0)),
            pl.BlockSpec((planes, some, L), lambda step: (0, step, 0)),
        ),
        out_shape=(field, field),
        scratch_shapes=[pltpu.VMEM((outer * some, 2 * TC), jnp.float32)],
        compiler_params=room(24),
        name="inverse_rows",
    )(landed, twiddle, plus)
    return (convergence, shear_one, shear_two)


def solution(mesh):
    shells, groups = (mesh.shape["shell"], mesh.shape["pix"])
    body, pix = (local, "pix")
    if shells == 2 and groups * TC == L:
        body, pix = (local_cube, ("upper", "low"))
        mesh = type(mesh)(mesh.devices.reshape(shells, 2, groups // 2), ("shell", "upper", "low"))
    placed = (P("shell", None), P("shell", pix, None), P("shell", pix, None), P("shell"), P("shell"), P("shell"))
    out = P("shell", pix, None)

    def step(*arrays):
        return body(*arrays)

    return jax.shard_map(step, mesh=mesh, in_specs=placed, out_specs=(out, out, out), check_vma=False)
```

```python
from functools import partial
import math

import jax
import jax.numpy as jnp
import numpy as np
from jax import lax
from jax.experimental import pallas as pl
from jax.experimental.pallas import tpu as pltpu
from jax.sharding import PartitionSpec as P

L = 2048
TR = 16
TC = 128


HIGHEST = lax.Precision.HIGHEST


def entering(value, axis, join, neutral):
    count, mine = (lax.axis_size(axis), lax.axis_index(axis))
    pieces = jax.tree.map(lambda part: lax.all_gather(part, axis), value)
    running = jax.tree.map(
        lambda part, zero: jnp.full_like(part, 0) + jnp.asarray(zero, part.dtype), value, neutral
    )

    def lap(position, running):
        longer = join(running, jax.tree.map(lambda part: part[position], pieces))
        return jax.tree.map(lambda new, old: jnp.where(position < mine, new, old), longer, running)

    return lax.fori_loop(0, count - 1, lap, running)


def dft_table(left_size, right_size, period, sign_value):
    left_idx = jnp.arange(left_size)[:, None]
    right_idx = jnp.arange(right_size)[None, :]
    angle = 2.0 * math.pi / period * (left_idx * right_idx % period).astype(jnp.float32)
    return (jnp.cos(angle), sign_value * jnp.sin(angle))


def mix_outer(table, real_part, imag_part):
    cosine, sine_part = table
    contract = partial(jnp.einsum, "ab,...bc->...ac", precision=HIGHEST)
    return (
        contract(cosine, real_part) - contract(sine_part, imag_part),
        contract(sine_part, real_part) + contract(cosine, imag_part),
    )


def mix_inner(table, real_part, imag_part):
    cosine, sine_part = table
    product = partial(jnp.matmul, precision=HIGHEST)
    return (
        product(real_part, cosine) - product(imag_part, sine_part),
        product(real_part, sine_part) + product(imag_part, cosine),
    )


def twist(table, real_part, imag_part):
    cosine, sine_part = table
    return (real_part * cosine - imag_part * sine_part, real_part * sine_part + imag_part * cosine)


def transform_last(real_part, imag_part, sign_value):
    length = real_part.shape[-1]
    inner = math.gcd(length, 128)
    outer = length // inner
    leading = real_part.shape[:-1]
    real_part = real_part.reshape(leading + (outer, inner))
    imag_part = imag_part.reshape(leading + (outer, inner))
    outer_table = dft_table(outer, outer, outer, sign_value)
    inner_table = dft_table(inner, inner, inner, sign_value)
    twiddle = dft_table(outer, inner, length, sign_value)
    if sign_value < 0:
        real_part, imag_part = mix_outer(outer_table, real_part, imag_part)
        real_part, imag_part = twist(twiddle, real_part, imag_part)
        real_part, imag_part = mix_inner(inner_table, real_part, imag_part)
    else:
        real_part, imag_part = mix_inner(inner_table, real_part, imag_part)
        real_part, imag_part = twist(twiddle, real_part, imag_part)
        real_part, imag_part = mix_outer(outer_table, real_part, imag_part)
    return (real_part.reshape(leading + (length,)), imag_part.reshape(leading + (length,)))


def frequency_of(position, length):
    inner = math.gcd(length, 128)
    outer = length // inner
    frequency = position // inner + outer * (position % inner)
    signed = jnp.where(frequency >= length // 2, frequency - length, frequency).astype(jnp.float32)
    keep_mask = (frequency != length // 2).astype(jnp.float32)
    return (signed, keep_mask)


def add_pairs(earlier_pair, later_pair):
    return (earlier_pair[0] + later_pair[0], earlier_pair[1] + later_pair[1])


def deposit_group(item):
    cell_ids, weights = item
    tile_rows = cell_ids // TC
    tile_cols = cell_ids % TC
    row_hot = jnp.where(
        tile_rows[:, None, :] == jnp.arange(TR)[None, :, None],
        weights[:, None, :],
        jnp.zeros((), jnp.bfloat16),
    )
    col_hot = (tile_cols[:, :, None] == jnp.arange(TC)[None, None, :]).astype(jnp.bfloat16)
    return jnp.einsum("grk,gkc->grc", row_hot, col_hot, preferred_element_type=jnp.float32)


def rows_to_sending(packed, groups, slab, cols_own):
    count, fields = (packed.shape[0], packed.shape[1])
    return (
        packed.reshape(count, fields, slab, groups, cols_own)
        .transpose(3, 0, 1, 4, 2)
        .reshape(groups, count, fields, cols_own * slab)
    )


def arrived_to_columns(arrived, groups, slab, cols_own):
    count, fields = (arrived.shape[1], arrived.shape[2])
    return (
        arrived.reshape(groups, count, fields, cols_own, slab)
        .transpose(1, 2, 3, 0, 4)
        .reshape(count, fields, cols_own, groups * slab)
    )


def columns_to_sending(stacked, groups, slab, cols_own):
    count, fields = (stacked.shape[0], stacked.shape[1])
    return (
        stacked.reshape(count, fields, cols_own, groups, slab)
        .transpose(3, 0, 1, 2, 4)
        .reshape(groups, count, fields, cols_own * slab)
    )


def landed_to_rows(landed, groups, slab, cols_own):
    count, fields = (landed.shape[1], landed.shape[2])
    return (
        landed.reshape(groups, count, fields, cols_own, slab)
        .transpose(1, 2, 4, 0, 3)
        .reshape(count, fields, slab, groups * cols_own)
    )


def local(block_tile, cell_index, masses, plane_coef, plane_dist, source_inv):
    groups = lax.axis_size("pix")
    my_index = lax.axis_index("pix")
    planes, local_tiles, per_tile = cell_index.shape
    slab = L // groups
    per_owner = slab // TR * (L // TC)
    cap = max(1, 2 * local_tiles // groups)
    flat = TR * TC
    batch_tiles = 8
    deposited = lax.map(
        deposit_group,
        (cell_index.reshape(-1, batch_tiles, per_tile), masses.reshape(-1, batch_tiles, per_tile)),
    )
    tile_sums = deposited.reshape(planes, local_tiles, flat)
    table = block_tile.reshape(planes, groups, local_tiles)
    owner = table // per_owner
    earlier = jnp.arange(local_tiles)[:, None] < jnp.arange(local_tiles)[None, :]
    same_owner = owner[:, :, :, None] == owner[:, :, None, :]
    rank = jnp.sum(jnp.where(same_owner & earlier[None, None], 1, 0), axis=2)
    slot = owner * cap + rank
    my_slots = lax.dynamic_index_in_dim(slot, my_index, axis=1, keepdims=False)
    slot_grid = jnp.arange(groups)[:, None] * cap + jnp.arange(cap)[None, :]
    send_hot = (my_slots[:, None, None, :] == slot_grid[None, :, :, None]).astype(jnp.float32)
    outgoing = jnp.einsum("pnct,ptf->npcf", send_hot, tile_sums, precision=HIGHEST)
    incoming = lax.all_to_all(outgoing, "pix", split_axis=0, concat_axis=0, tiled=True)
    local_index = table - my_index * per_owner
    is_mine = owner == my_index
    tile_hot = (is_mine[..., None] & (local_index[..., None] == jnp.arange(per_owner))).astype(
        jnp.float32
    )
    slot_hot = (rank[..., None] == jnp.arange(cap)).astype(jnp.float32)
    placing = jnp.einsum("pstl,pstc->plsc", tile_hot, slot_hot, precision=HIGHEST)
    slab_tiles = jnp.einsum("plsc,spcf->plf", placing, incoming, precision=HIGHEST)
    density = (
        slab_tiles.reshape(planes, slab // TR, L // TC, TR, TC)
        .transpose(0, 1, 3, 2, 4)
        .reshape(planes, slab, L)
    )
    total = lax.psum(jnp.sum(density, axis=(1, 2)), "pix")
    contrast = density / (total / (L * L))[:, None, None] - 1.0
    near_local = jnp.cumsum(plane_coef[:, None, None] * contrast, axis=0)
    far_local = jnp.cumsum((plane_coef * plane_dist)[:, None, None] * contrast, axis=0)
    blank = jnp.zeros((slab, L), jnp.float32)
    near_before, far_before = entering(
        (near_local[-1], far_local[-1]), "shell", add_pairs, (blank, blank)
    )
    convergence = near_before + near_local - source_inv[:, None, None] * (far_before + far_local)
    cols_own = L // groups
    wave_x, keep_x = frequency_of(my_index * cols_own + jnp.arange(cols_own), L)
    wave_y, keep_y = frequency_of(jnp.arange(L), L)
    wave_x = wave_x[:, None]
    wave_y = wave_y[None, :]
    both_keep = keep_x[:, None] * keep_y[None, :]
    wave_power = jnp.maximum(wave_x * wave_x + wave_y * wave_y, 1.0)
    kernel_one = both_keep * (wave_x * wave_x - wave_y * wave_y) / wave_power
    kernel_two = both_keep * 2.0 * wave_x * wave_y / wave_power
    scale = 1.0 / (L * L)
    spec_real, spec_imag = transform_last(convergence[0::2], convergence[1::2], -1.0)
    sending = rows_to_sending(jnp.stack([spec_real, spec_imag], axis=1), groups, slab, cols_own)
    arrived = lax.all_to_all(sending, "pix", split_axis=0, concat_axis=0, tiled=True)
    columns = arrived_to_columns(arrived, groups, slab, cols_own)
    row_real, row_imag = transform_last(columns[:, 0], columns[:, 1], -1.0)
    first_real, first_imag = transform_last(row_real * kernel_one, row_imag * kernel_one, 1.0)
    second_real, second_imag = transform_last(row_real * kernel_two, row_imag * kernel_two, 1.0)
    stacked = jnp.stack([first_real, first_imag, second_real, second_imag], axis=1)
    landed = lax.all_to_all(
        columns_to_sending(stacked, groups, slab, cols_own),
        "pix",
        split_axis=0,
        concat_axis=0,
        tiled=True,
    )
    row_layout = landed_to_rows(landed, groups, slab, cols_own)
    even_one, odd_one = transform_last(row_layout[:, 0], row_layout[:, 1], 1.0)
    even_two, odd_two = transform_last(row_layout[:, 2], row_layout[:, 3], 1.0)
    shear_one = jnp.stack([even_one, odd_one], axis=1).reshape(planes, slab, L)
    shear_two = jnp.stack([even_two, odd_two], axis=1).reshape(planes, slab, L)
    return (convergence, shear_one * scale, shear_two * scale)


def bf16_pair(value):
    high = value.astype(jnp.bfloat16)
    return (high, (value - high.astype(jnp.float32)).astype(jnp.bfloat16))


def dft_block(size, sign_value):
    turn = 2.0 * np.pi / size * (np.outer(np.arange(size), np.arange(size)) % size)
    cosine, sine = (np.cos(turn), sign_value * np.sin(turn))
    whole = np.block([[cosine, sine], [-sine, cosine]]).astype(np.float32)
    high = whole.astype(jnp.bfloat16)
    low = (whole - high.astype(np.float32)).astype(jnp.bfloat16)
    return np.stack([high, low])


def twiddle_pair(outer, inner):
    turn = 2.0 * np.pi / (outer * inner) * np.outer(np.arange(outer), np.arange(inner))
    return np.stack([np.cos(turn), np.sin(turn)]).astype(np.float32)


def quarter(values, sign_value):
    (ar, ai), (br, bi), (cr, ci), (dr, di) = values
    pr, pi, mr, mi = (ar + cr, ai + ci, ar - cr, ai - ci)
    qr, qi, nr, ni = (br + dr, bi + di, br - dr, bi - di)
    if sign_value < 0:
        return [(pr + qr, pi + qi), (mr + ni, mi - nr), (pr - qr, pi - qi), (mr - ni, mi + nr)]
    return [(pr + qr, pi + qi), (mr - ni, mi + nr), (pr - qr, pi - qi), (mr + ni, mi - nr)]


def rotate(value, step, sign_value):
    real_part, imag_part = value
    if step == 0:
        return value
    if step == 4:
        return (-sign_value * imag_part, sign_value * real_part)
    cosine = math.cos(2.0 * math.pi * step / 16)
    sine = sign_value * math.sin(2.0 * math.pi * step / 16)
    return (real_part * cosine - imag_part * sine, real_part * sine + imag_part * cosine)


def sixteen(values, sign_value, count=16):
    inner = [quarter([values[4 * a + b] for a in range(4)], sign_value) for b in range(4)]
    result = [None] * 16
    for k in range(4):
        turned_values = [rotate(inner[b][k], b * k, sign_value) for b in range(4)]
        for place, value in enumerate(quarter(turned_values, sign_value)):
            result[k + 4 * place] = value
    return result[:count]


def dot3(left, right):
    mul = partial(jnp.dot, preferred_element_type=jnp.float32)
    (left_high, left_low), (right_high, right_low) = (left, right)
    return mul(left_high, right_high) + (mul(left_low, right_high) + mul(left_high, right_low))


def widen_kernel(cell_ref, mass_ref, out_ref):
    out_ref[0] = cell_ref[...].astype(jnp.float32)
    out_ref[1] = mass_ref[...].astype(jnp.float32)


def pack_kernel(half, cap, per_owner, which, at_ref, table_ref, raw_ref, out_ref, count_ref):
    _, planes, local_tiles, per_tile = raw_ref.shape
    groups = out_ref.shape[0]
    chunks = per_tile // TC
    lines = 2 * chunks * cap
    out_ref[...] = jnp.zeros(out_ref.shape, jnp.float32)
    base = at_ref[which] * local_tiles
    for plane in range(planes):

        @pl.loop(0, groups)
        def _(slot):
            count_ref[slot] = 0

        @pl.loop(0, local_tiles // 8)
        def _(bunch):
            here = pl.ds(pl.multiple_of(bunch * 8, 8), 8)
            lists = [raw_ref[kind, plane, here, :] for kind in range(2)]
            for at in range(8):
                owner = lax.div(table_ref[plane, base + bunch * 8 + at], per_owner)
                low = lax.rem(owner, half)
                side = lax.rem(lax.div(owner, half) + lax.rem(low, 2), 2)
                place = side * half + low
                rank = count_ref[place]
                count_ref[place] = rank + 1
                for kind, values in enumerate(lists):
                    for chunk in range(chunks):
                        row = plane * lines + kind * chunks * cap + chunk * cap + rank
                        out_ref[place, pl.ds(row, 1), :] = values[at : at + 1, chunk * TC : (chunk + 1) * TC]

        total = jnp.sum(raw_ref[1, plane], axis=0, keepdims=True)
        total = jnp.sum(total, axis=1, keepdims=True)
        line = jnp.broadcast_to(total, (1, TC))
        for place in range(groups):
            out_ref[place, planes * lines + plane : planes * lines + plane + 1, :] = line


def deposit_kernel(cap, chunks, slots_ref, recv_ref, out_ref):
    out_ref[...] = jnp.zeros(out_ref.shape, jnp.float32)
    all_planes = out_ref.shape[0]
    planes = all_planes // 2
    half = recv_ref.shape[0] // 2
    width = 32
    bunch = 4
    parts = TC // width
    low = lax.broadcasted_iota(jnp.int32, (TR, TC), 0).astype(jnp.float32)
    lines = [(low + float(TR * part)).astype(jnp.bfloat16) for part in range(parts)]
    one = jnp.ones((TR, TC), jnp.bfloat16)
    none = jnp.zeros((TR, TC), jnp.bfloat16)

    def spread(value, slot):
        return jnp.broadcast_to(value[slot : slot + 1, :], (TR, TC)).astype(jnp.bfloat16)

    for plane in range(all_planes):
        start = (plane % planes) * 2 * chunks * cap

        @pl.loop(0, half, unroll=4)
        def _(source):
            place = (plane // planes) * half + source
            cells = [recv_ref[place, start + k * cap : start + (k + 1) * cap, :] for k in range(chunks)]
            weights = [
                recv_ref[place, start + (chunks + k) * cap : start + (chunks + k + 1) * cap, :] for k in range(chunks)
            ]
            rows = [jnp.floor(cell * (1.0 / TC)) for cell in cells]
            strips = [jnp.floor(cell * (1.0 / width)) for cell in cells]
            cols = [cell - strip * float(width) for cell, strip in zip(cells, strips)]
            rows = [row + (strip - row * float(parts)) * float(TR) for row, strip in zip(rows, strips)]
            sums = []
            for first in range(0, cap, bunch):
                row_hot = []
                col_hot = []
                for k in range(chunks):
                    row_lines = []
                    col_lines = []
                    for slot in range(first, first + bunch):
                        row = spread(rows[k], slot)
                        weight = spread(weights[k], slot)
                        row_lines += [jnp.where(lines[at] == row, weight, none) for at in range(parts)]
                        col = spread(cols[k], slot)
                        col_lines += [jnp.where(lines[at] == col, one, none) for at in range(width // TR)]
                    row_hot.append(jnp.concatenate(row_lines, axis=0))
                    col_hot.append(jnp.concatenate(col_lines, axis=0))
                done = lax.dot_general(
                    jnp.concatenate(row_hot, axis=1),
                    jnp.concatenate(col_hot, axis=1),
                    (((1,), (1,)), ((), ())),
                    preferred_element_type=jnp.float32,
                )
                for at in range(bunch):
                    base = at * TR * parts
                    side = slice(at * width, (at + 1) * width)
                    strips_of = [done[base + j * TR : base + (j + 1) * TR, side] for j in range(parts)]
                    sums.append(jnp.concatenate(strips_of, axis=1))
            for slot in range(cap):
                tile = slots_ref[(plane * half + source) * cap + slot]
                out_ref[plane, tile] = out_ref[plane, tile] + sums[slot]


def rows_kernel(
    cap, chunks, weight_ref, at_ref, slots_ref, near_dens_ref, near_ref, far_ref, twiddle_ref, table_ref,
    mine_ref, other_ref, out_ref, high_ref, low_ref, far_dens_ref,
):
    step = pl.program_id(0)
    pl.when(step == 0)(lambda: deposit_kernel(cap, chunks, slots_ref, far_ref, far_dens_ref))
    first_line = 2 * (far_dens_ref.shape[0] // 2) * cap * chunks
    planes, slab, length = mine_ref.shape
    all_planes = far_dens_ref.shape[0]
    outer = length // TC
    first_tile = step * (slab // TR * outer)
    half = near_ref.shape[0] // 2
    scales = []
    for plane in range(all_planes):
        line = plane % planes
        total = jnp.zeros((1, TC), jnp.float32)
        for source in range(half):
            place = (plane // planes) * half + source
            total = total + near_ref[place, line : line + 1, :]
            total = total + far_ref[place, first_line + line : first_line + line + 1, :]
        scales.append(float(length * length) / total)
    table = (table_ref[0], table_ref[1])
    for side, conv_ref in enumerate((mine_ref, other_ref)):
        here_maps = [side * planes + i for i in range(planes)]
        factors = [
            [jnp.broadcast_to(weight_ref[i, j] * scales[j], (TR, TC)) for j in range(all_planes)] for i in here_maps
        ]
        shift = [weight_ref[i, all_planes] for i in here_maps]

        for line in range(slab // TR):
            values = []
            here = slice(line * TR, (line + 1) * TR)
            for col in range(outer):
                at = line * outer + col
                tiles = [near_dens_ref[j, at] + far_dens_ref[j, first_tile + at] for j in range(all_planes)]
                pair = []
                for i in range(planes):
                    field = tiles[0] * factors[i][0]
                    for tile, factor in zip(tiles[1:], factors[i][1:]):
                        field = field + tile * factor
                    field = field - shift[i]
                    conv_ref[i, here, col * TC : (col + 1) * TC] = field
                    pair.append(field)
                values.append(tuple(pair))
            for place, (real_part, imag_part) in enumerate(sixteen(values, -1.0)):
                if place:
                    cosine = twiddle_ref[0, place : place + 1, :]
                    sine = twiddle_ref[1, place : place + 1, :]
                    real_part, imag_part = (
                        real_part * cosine + imag_part * sine,
                        imag_part * cosine - real_part * sine,
                    )
                spot = slice(place * slab + line * TR, place * slab + (line + 1) * TR)
                for at, value in enumerate((real_part, imag_part)):
                    high, low = bf16_pair(value)
                    high_ref[spot, at * TC : (at + 1) * TC] = high
                    low_ref[spot, at * TC : (at + 1) * TC] = low

        base = at_ref[2 + side] * half
        done = dot3((high_ref[...], low_ref[...]), table)
        for place in range(outer):
            here = slice(place * slab, (place + 1) * slab)
            out_ref[base + place // 2, place % 2, 0] = done[here, :TC]
            out_ref[base + place // 2, place % 2, 1] = done[here, TC:]


def turned(turn_ref, place, here, value, sign_value):
    if place == 0:
        return value
    real_part, imag_part = value
    shape = real_part.shape
    cosine = jnp.broadcast_to(turn_ref[0, here, place : place + 1], shape)
    sine = jnp.broadcast_to(turn_ref[1, here, place : place + 1], shape) * sign_value
    return (real_part * cosine - imag_part * sine, real_part * sine + imag_part * cosine)


def columns_kernel(
    order, at_ref, in_ref, turn_ref, forward_ref, back_ref, out_ref, high_ref, low_ref, spectrum_ref, back_f
):
    outer, _, _, inner, lanes = in_ref.shape
    length = outer * inner
    forward = (forward_ref[0], forward_ref[1])
    back = (back_ref[0], back_ref[1])

    @pl.loop(0, inner // TR)
    def _(line):
        here = pl.ds(line * TR, TR)
        there = pl.ds(inner + line * TR, TR)
        values = [(in_ref[place, 0, 0, here, :], in_ref[place, 0, 1, here, :]) for place in order]
        for place, value in enumerate(sixteen(values, -1.0)):
            for spot, part in zip((here, there), turned(turn_ref, place, here, value, -1.0)):
                high, low = bf16_pair(part)
                high_ref[spot, place * lanes : (place + 1) * lanes] = high
                low_ref[spot, place * lanes : (place + 1) * lanes] = low

    for bunch in range(outer // 2):
        span = slice(bunch * 2 * lanes, (bunch + 1) * 2 * lanes)
        spectrum_ref[:, span] = dot3(forward, (high_ref[:, span], low_ref[:, span]))

    middle = length // 2
    wave_v = lax.broadcasted_iota(jnp.int32, (inner, lanes), 1) * outer + (2 * at_ref[4] + pl.program_id(0))
    keep_v = wave_v != middle
    sv = jnp.where(wave_v >= middle, wave_v - length, wave_v).astype(jnp.float32)
    line_u = lax.broadcasted_iota(jnp.int32, (inner, lanes), 0) * outer
    flip = jnp.where(at_ref[5] > 0, -1.0, 1.0)
    for place in range(outer):
        side = slice(place * lanes, (place + 1) * lanes)
        wave_u = line_u + place
        su = jnp.where(wave_u >= middle, wave_u - length, wave_u).astype(jnp.float32)
        scale = 1.0 / (float(length) * float(length))
        keep = jnp.where(keep_v & (wave_u != middle), scale * flip if place % 2 else scale, 0.0)
        factor = keep / jnp.maximum(sv * sv + su * su, 1.0)
        first = factor * (sv * sv - su * su)
        second = factor * (2.0 * sv * su)
        real_part = spectrum_ref[:inner, side]
        imag_part = spectrum_ref[inner:, side]
        stacked = jnp.concatenate(
            [
                jnp.concatenate([real_part * first, real_part * second], axis=1),
                jnp.concatenate([imag_part * first, imag_part * second], axis=1),
            ],
            axis=0,
        )
        back_f[place] = dot3(back, bf16_pair(stacked))

    half = outer // 2

    @pl.loop(0, inner // TR)
    def _(line):
        here = pl.ds(line * TR, TR)
        there = pl.ds(inner + line * TR, TR)
        for field in range(2):
            side = slice(field * lanes, (field + 1) * lanes)
            values = [
                turned(turn_ref, place, here, (back_f[place, here, side], back_f[place, there, side]), 1.0)
                for place in range(outer)
            ]
            for low, (real_part, imag_part) in enumerate(sixteen(values, 1.0, half)):
                out_ref[low, 0, field, 0, here, :] = real_part
                out_ref[low, 0, field, 1, here, :] = imag_part


def inverse_rows_kernel(in_ref, twiddle_ref, table_ref, first_ref, second_ref, back_f):
    half, _, _, _, slab, lanes = in_ref.shape
    outer = 2 * half
    table = (table_ref[0], table_ref[1])
    for field, out_ref in enumerate((first_ref, second_ref)):
        joined = [
            jnp.concatenate([in_ref[place // 2, place % 2, field, part] for place in range(outer)], axis=0)
            for part in range(2)
        ]
        back_f[...] = dot3(bf16_pair(jnp.concatenate(joined, axis=1)), table)
        for line in range(slab // TR):
            here = slice(line * TR, (line + 1) * TR)
            values = []
            for place in range(outer):
                spot = slice(place * slab + line * TR, place * slab + (line + 1) * TR)
                real_part = back_f[spot, :lanes]
                imag_part = back_f[spot, lanes:]
                if place:
                    cosine = twiddle_ref[0, place : place + 1, :]
                    sine = twiddle_ref[1, place : place + 1, :]
                    real_part, imag_part = (
                        real_part * cosine - imag_part * sine,
                        real_part * sine + imag_part * cosine,
                    )
                values.append((real_part, imag_part))
            for place, (real_part, imag_part) in enumerate(sixteen(values, 1.0)):
                out_ref[0, here, place * lanes : (place + 1) * lanes] = real_part
                out_ref[1, here, place * lanes : (place + 1) * lanes] = imag_part


VMEM = pl.BlockSpec(memory_space=pltpu.VMEM)
SMEM = pl.BlockSpec(memory_space=pltpu.SMEM)


def room(mib):
    return pltpu.CompilerParams(vmem_limit_bytes=mib * 1024 * 1024)


def whole(shape):
    return pl.BlockSpec(shape, lambda step: (0,) * len(shape))


def slot_tiles(table, held, per_owner, cap):
    local_tiles = table.shape[-1]
    mine = table // per_owner == held
    earlier = jnp.arange(local_tiles)[:, None] < jnp.arange(local_tiles)[None, :]
    rank = jnp.sum(jnp.where(mine[..., :, None] & earlier, 1, 0), axis=-2)
    chosen = mine[..., None, :] & (rank[..., None, :] == jnp.arange(cap)[:, None])
    spot = table - held * per_owner
    return jnp.sum(jnp.where(chosen, spot[..., None, :], 0), axis=-1)


def cube_exchange(value):
    return lax.all_to_all(value, ("shell", "low"), split_axis=0, concat_axis=0, tiled=True)


def local_cube(block_tile, cell_index, masses, plane_coef, plane_dist, source_inv):
    half = lax.axis_size("low")
    groups = 2 * half
    shell = lax.axis_index("shell")
    upper = lax.axis_index("upper")
    low = lax.axis_index("low")
    planes, local_tiles, per_tile = cell_index.shape
    slab = L // groups
    outer = L // TC
    per_owner = slab // TR * outer
    cap = max(1, 2 * local_tiles // groups)
    chunks = per_tile // TC
    lines = 2 * chunks * cap * planes
    part = (shell + low) % 2
    held = part * half + low
    order = [((s // half + s % 2) % 2) * half + s % half for s in range(groups)]

    raw = pl.pallas_call(
        widen_kernel,
        in_specs=[VMEM, VMEM],
        out_specs=VMEM,
        out_shape=jax.ShapeDtypeStruct((2, planes, local_tiles, per_tile), jnp.float32),
        compiler_params=room(8),
        name="widen",
    )(cell_index, masses)
    raw_far = lax.ppermute(raw, "upper", [(0, 1), (1, 0)])

    here = jnp.stack([upper * half + low, (1 - upper) * half + low, shell, 1 - shell, low, upper]).astype(jnp.int32)

    def pack(which, lists):
        return pl.pallas_call(
            partial(pack_kernel, half, cap, per_owner, which),
            in_specs=[SMEM, SMEM, VMEM],
            out_specs=VMEM,
            out_shape=jax.ShapeDtypeStruct((groups, lines + 8, TC), jnp.float32),
            scratch_shapes=[pltpu.SMEM((groups,), jnp.int32)],
            compiler_params=room(12),
            name="pack",
        )(here, block_tile, lists)

    near = cube_exchange(pack(0, raw))
    far = cube_exchange(pack(1, raw_far))

    note = jnp.concatenate(
        [block_tile.astype(jnp.float32), plane_coef[:, None], (plane_coef * plane_dist)[:, None], source_inv[:, None]],
        axis=1,
    )
    other = lax.ppermute(note, "shell", [(0, 1), (1, 0)])
    both = jnp.where(shell == 0, jnp.concatenate([note, other]), jnp.concatenate([other, note]))
    tiles = slot_tiles(
        both[:, : groups * local_tiles].astype(jnp.int32).reshape(2 * planes, groups, local_tiles), held, per_owner, cap
    )
    tiles = tiles.reshape(2 * planes, 2, half, cap)
    near_slots = lax.dynamic_index_in_dim(tiles, upper, axis=1, keepdims=False).reshape(-1)
    far_slots = lax.dynamic_index_in_dim(tiles, 1 - upper, axis=1, keepdims=False).reshape(-1)
    maps = jnp.concatenate([shell * planes + jnp.arange(planes), (1 - shell) * planes + jnp.arange(planes)])
    inverse = jnp.concatenate([note[:, -1], other[:, -1]])
    weight = jnp.where(
        jnp.arange(2 * planes)[None, :] <= maps[:, None], both[None, :, -3] - inverse[:, None] * both[None, :, -2], 0.0
    )
    weight = jnp.concatenate([weight, jnp.sum(weight, axis=1, keepdims=True)], axis=1)

    near_dens = pl.pallas_call(
        partial(deposit_kernel, cap, chunks),
        in_specs=[SMEM, VMEM],
        out_specs=VMEM,
        out_shape=pltpu.HBM((2 * planes, per_owner, TR, TC), jnp.float32),
        compiler_params=room(16),
        name="deposit",
    )(near_slots, near)
    twiddle = jnp.asarray(twiddle_pair(outer, TC))
    turn = jnp.asarray(twiddle_pair(outer, TC).transpose(0, 2, 1))
    minus = jnp.asarray(dft_block(TC, -1.0))
    plus = jnp.asarray(dft_block(TC, 1.0))
    field = jax.ShapeDtypeStruct((planes, slab, L), jnp.float32)
    some = 2 * TR
    conv_mine, conv_other, row_sent = pl.pallas_call(
        partial(rows_kernel, cap, chunks),
        grid=(slab // some,),
        in_specs=[
            SMEM,
            SMEM,
            SMEM,
            pl.BlockSpec((2 * planes, some // TR * outer, TR, TC), lambda step: (0, step, 0, 0)),
            pl.BlockSpec((groups, 8, TC), lambda step: (0, lines // 8, 0)),
            whole(far.shape),
            whole(twiddle.shape),
            whole(minus.shape),
        ],
        out_specs=(
            pl.BlockSpec((planes, some, L), lambda step: (0, step, 0)),
            pl.BlockSpec((planes, some, L), lambda step: (0, step, 0)),
            pl.BlockSpec((groups, 2, 2, some, TC), lambda step: (0, 0, 0, step, 0)),
        ),
        out_shape=(
            pltpu.HBM(field.shape, field.dtype),
            pltpu.HBM(field.shape, field.dtype),
            pltpu.HBM((groups, 2, 2, slab, TC), jnp.float32),
        ),
        scratch_shapes=[
            pltpu.VMEM((outer * some, 2 * TC), jnp.bfloat16),
            pltpu.VMEM((outer * some, 2 * TC), jnp.bfloat16),
            pltpu.VMEM((2 * planes, per_owner, TR, TC), jnp.float32),
        ],
        compiler_params=room(28),
        name="rows",
    )(weight, here, far_slots, near_dens, near, far, twiddle, minus)
    arrived = lax.all_to_all(row_sent, ("shell", "low"), split_axis=0, concat_axis=0, tiled=True)
    swaps = []
    for side in range(2):
        for top in range(2):
            for at in range(half):
                if (side + at) % 2 == top:
                    swaps.append(((side * 2 + top) * half + at, ((1 - side) * 2 + top) * half + at))
    conv_held = lax.ppermute(conv_other, ("shell", "upper", "low"), swaps)
    convergence = jnp.where(part == upper, conv_mine, conv_held)
    col_sent = pl.pallas_call(
        partial(columns_kernel, order),
        grid=(2,),
        in_specs=[
            SMEM,
            pl.BlockSpec((groups, 1, 2, slab, TC), lambda step: (0, step, 0, 0, 0)),
            whole(turn.shape),
            whole(plus.shape),
            whole(minus.shape),
        ],
        out_specs=pl.BlockSpec((half, 1, 2, 2, slab, TC), lambda step: (0, step, 0, 0, 0, 0)),
        out_shape=pltpu.HBM((half, 2, 2, 2, slab, TC), jnp.float32),
        scratch_shapes=[
            pltpu.VMEM((2 * slab, L), jnp.bfloat16),
            pltpu.VMEM((2 * slab, L), jnp.bfloat16),
            pltpu.VMEM((2 * slab, L), jnp.float32),
            pltpu.VMEM((outer, 2 * slab, 2 * TC), jnp.float32),
        ],
        compiler_params=room(32),
        name="columns",
    )(here, arrived, turn, plus, minus)
    landed = lax.all_to_all(col_sent, "low", split_axis=0, concat_axis=0, tiled=True)
    shear_one, shear_two = pl.pallas_call(
        inverse_rows_kernel,
        grid=(slab // some,),
        in_specs=[
            pl.BlockSpec((half, 2, 2, 2, some, TC), lambda step: (0, 0, 0, 0, step, 0)),
            whole(twiddle.shape),
            whole(plus.shape),
        ],
        out_specs=(
            pl.BlockSpec((planes, some, L), lambda step: (0, step, 0)),
            pl.BlockSpec((planes, some, L), lambda step: (0, step, 0)),
        ),
        out_shape=(field, field),
        scratch_shapes=[pltpu.VMEM((outer * some, 2 * TC), jnp.float32)],
        compiler_params=room(24),
        name="inverse_rows",
    )(landed, twiddle, plus)
    return (convergence, shear_one, shear_two)


def solution(mesh):
    shells, groups = (mesh.shape["shell"], mesh.shape["pix"])
    body, pix = (local, "pix")
    if shells == 2 and groups * TC == L:
        body, pix = (local_cube, ("upper", "low"))
        mesh = type(mesh)(mesh.devices.reshape(shells, 2, groups // 2), ("shell", "upper", "low"))
    placed = (P("shell", None), P("shell", pix, None), P("shell", pix, None), P("shell"), P("shell"), P("shell"))
    out = P("shell", pix, None)

    def step(*arrays):
        return body(*arrays)

    return jax.shard_map(step, mesh=mesh, in_specs=placed, out_specs=(out, out, out), check_vma=False)
```

```python
from functools import partial
import math

import jax
import jax.numpy as jnp
import numpy as np
from jax import lax
from jax.experimental import pallas as pl
from jax.experimental.pallas import tpu as pltpu
from jax.sharding import PartitionSpec as P

L = 2048
TR = 16
TC = 128


HIGHEST = lax.Precision.HIGHEST


def entering(value, axis, join, neutral):
    count, mine = (lax.axis_size(axis), lax.axis_index(axis))
    pieces = jax.tree.map(lambda part: lax.all_gather(part, axis), value)
    running = jax.tree.map(
        lambda part, zero: jnp.full_like(part, 0) + jnp.asarray(zero, part.dtype), value, neutral
    )

    def lap(position, running):
        longer = join(running, jax.tree.map(lambda part: part[position], pieces))
        return jax.tree.map(lambda new, old: jnp.where(position < mine, new, old), longer, running)

    return lax.fori_loop(0, count - 1, lap, running)


def dft_table(left_size, right_size, period, sign_value):
    left_idx = jnp.arange(left_size)[:, None]
    right_idx = jnp.arange(right_size)[None, :]
    angle = 2.0 * math.pi / period * (left_idx * right_idx % period).astype(jnp.float32)
    return (jnp.cos(angle), sign_value * jnp.sin(angle))


def mix_outer(table, real_part, imag_part):
    cosine, sine_part = table
    contract = partial(jnp.einsum, "ab,...bc->...ac", precision=HIGHEST)
    return (
        contract(cosine, real_part) - contract(sine_part, imag_part),
        contract(sine_part, real_part) + contract(cosine, imag_part),
    )


def mix_inner(table, real_part, imag_part):
    cosine, sine_part = table
    product = partial(jnp.matmul, precision=HIGHEST)
    return (
        product(real_part, cosine) - product(imag_part, sine_part),
        product(real_part, sine_part) + product(imag_part, cosine),
    )


def twist(table, real_part, imag_part):
    cosine, sine_part = table
    return (real_part * cosine - imag_part * sine_part, real_part * sine_part + imag_part * cosine)


def transform_last(real_part, imag_part, sign_value):
    length = real_part.shape[-1]
    inner = math.gcd(length, 128)
    outer = length // inner
    leading = real_part.shape[:-1]
    real_part = real_part.reshape(leading + (outer, inner))
    imag_part = imag_part.reshape(leading + (outer, inner))
    outer_table = dft_table(outer, outer, outer, sign_value)
    inner_table = dft_table(inner, inner, inner, sign_value)
    twiddle = dft_table(outer, inner, length, sign_value)
    if sign_value < 0:
        real_part, imag_part = mix_outer(outer_table, real_part, imag_part)
        real_part, imag_part = twist(twiddle, real_part, imag_part)
        real_part, imag_part = mix_inner(inner_table, real_part, imag_part)
    else:
        real_part, imag_part = mix_inner(inner_table, real_part, imag_part)
        real_part, imag_part = twist(twiddle, real_part, imag_part)
        real_part, imag_part = mix_outer(outer_table, real_part, imag_part)
    return (real_part.reshape(leading + (length,)), imag_part.reshape(leading + (length,)))


def frequency_of(position, length):
    inner = math.gcd(length, 128)
    outer = length // inner
    frequency = position // inner + outer * (position % inner)
    signed = jnp.where(frequency >= length // 2, frequency - length, frequency).astype(jnp.float32)
    keep_mask = (frequency != length // 2).astype(jnp.float32)
    return (signed, keep_mask)


def add_pairs(earlier_pair, later_pair):
    return (earlier_pair[0] + later_pair[0], earlier_pair[1] + later_pair[1])


def deposit_group(item):
    cell_ids, weights = item
    tile_rows = cell_ids // TC
    tile_cols = cell_ids % TC
    row_hot = jnp.where(
        tile_rows[:, None, :] == jnp.arange(TR)[None, :, None],
        weights[:, None, :],
        jnp.zeros((), jnp.bfloat16),
    )
    col_hot = (tile_cols[:, :, None] == jnp.arange(TC)[None, None, :]).astype(jnp.bfloat16)
    return jnp.einsum("grk,gkc->grc", row_hot, col_hot, preferred_element_type=jnp.float32)


def rows_to_sending(packed, groups, slab, cols_own):
    count, fields = (packed.shape[0], packed.shape[1])
    return (
        packed.reshape(count, fields, slab, groups, cols_own)
        .transpose(3, 0, 1, 4, 2)
        .reshape(groups, count, fields, cols_own * slab)
    )


def arrived_to_columns(arrived, groups, slab, cols_own):
    count, fields = (arrived.shape[1], arrived.shape[2])
    return (
        arrived.reshape(groups, count, fields, cols_own, slab)
        .transpose(1, 2, 3, 0, 4)
        .reshape(count, fields, cols_own, groups * slab)
    )


def columns_to_sending(stacked, groups, slab, cols_own):
    count, fields = (stacked.shape[0], stacked.shape[1])
    return (
        stacked.reshape(count, fields, cols_own, groups, slab)
        .transpose(3, 0, 1, 2, 4)
        .reshape(groups, count, fields, cols_own * slab)
    )


def landed_to_rows(landed, groups, slab, cols_own):
    count, fields = (landed.shape[1], landed.shape[2])
    return (
        landed.reshape(groups, count, fields, cols_own, slab)
        .transpose(1, 2, 4, 0, 3)
        .reshape(count, fields, slab, groups * cols_own)
    )


def local(block_tile, cell_index, masses, plane_coef, plane_dist, source_inv):
    groups = lax.axis_size("pix")
    my_index = lax.axis_index("pix")
    planes, local_tiles, per_tile = cell_index.shape
    slab = L // groups
    per_owner = slab // TR * (L // TC)
    cap = max(1, 2 * local_tiles // groups)
    flat = TR * TC
    batch_tiles = 8
    deposited = lax.map(
        deposit_group,
        (cell_index.reshape(-1, batch_tiles, per_tile), masses.reshape(-1, batch_tiles, per_tile)),
    )
    tile_sums = deposited.reshape(planes, local_tiles, flat)
    table = block_tile.reshape(planes, groups, local_tiles)
    owner = table // per_owner
    earlier = jnp.arange(local_tiles)[:, None] < jnp.arange(local_tiles)[None, :]
    same_owner = owner[:, :, :, None] == owner[:, :, None, :]
    rank = jnp.sum(jnp.where(same_owner & earlier[None, None], 1, 0), axis=2)
    slot = owner * cap + rank
    my_slots = lax.dynamic_index_in_dim(slot, my_index, axis=1, keepdims=False)
    slot_grid = jnp.arange(groups)[:, None] * cap + jnp.arange(cap)[None, :]
    send_hot = (my_slots[:, None, None, :] == slot_grid[None, :, :, None]).astype(jnp.float32)
    outgoing = jnp.einsum("pnct,ptf->npcf", send_hot, tile_sums, precision=HIGHEST)
    incoming = lax.all_to_all(outgoing, "pix", split_axis=0, concat_axis=0, tiled=True)
    local_index = table - my_index * per_owner
    is_mine = owner == my_index
    tile_hot = (is_mine[..., None] & (local_index[..., None] == jnp.arange(per_owner))).astype(
        jnp.float32
    )
    slot_hot = (rank[..., None] == jnp.arange(cap)).astype(jnp.float32)
    placing = jnp.einsum("pstl,pstc->plsc", tile_hot, slot_hot, precision=HIGHEST)
    slab_tiles = jnp.einsum("plsc,spcf->plf", placing, incoming, precision=HIGHEST)
    density = (
        slab_tiles.reshape(planes, slab // TR, L // TC, TR, TC)
        .transpose(0, 1, 3, 2, 4)
        .reshape(planes, slab, L)
    )
    total = lax.psum(jnp.sum(density, axis=(1, 2)), "pix")
    contrast = density / (total / (L * L))[:, None, None] - 1.0
    near_local = jnp.cumsum(plane_coef[:, None, None] * contrast, axis=0)
    far_local = jnp.cumsum((plane_coef * plane_dist)[:, None, None] * contrast, axis=0)
    blank = jnp.zeros((slab, L), jnp.float32)
    near_before, far_before = entering(
        (near_local[-1], far_local[-1]), "shell", add_pairs, (blank, blank)
    )
    convergence = near_before + near_local - source_inv[:, None, None] * (far_before + far_local)
    cols_own = L // groups
    wave_x, keep_x = frequency_of(my_index * cols_own + jnp.arange(cols_own), L)
    wave_y, keep_y = frequency_of(jnp.arange(L), L)
    wave_x = wave_x[:, None]
    wave_y = wave_y[None, :]
    both_keep = keep_x[:, None] * keep_y[None, :]
    wave_power = jnp.maximum(wave_x * wave_x + wave_y * wave_y, 1.0)
    kernel_one = both_keep * (wave_x * wave_x - wave_y * wave_y) / wave_power
    kernel_two = both_keep * 2.0 * wave_x * wave_y / wave_power
    scale = 1.0 / (L * L)
    spec_real, spec_imag = transform_last(convergence[0::2], convergence[1::2], -1.0)
    sending = rows_to_sending(jnp.stack([spec_real, spec_imag], axis=1), groups, slab, cols_own)
    arrived = lax.all_to_all(sending, "pix", split_axis=0, concat_axis=0, tiled=True)
    columns = arrived_to_columns(arrived, groups, slab, cols_own)
    row_real, row_imag = transform_last(columns[:, 0], columns[:, 1], -1.0)
    first_real, first_imag = transform_last(row_real * kernel_one, row_imag * kernel_one, 1.0)
    second_real, second_imag = transform_last(row_real * kernel_two, row_imag * kernel_two, 1.0)
    stacked = jnp.stack([first_real, first_imag, second_real, second_imag], axis=1)
    landed = lax.all_to_all(
        columns_to_sending(stacked, groups, slab, cols_own),
        "pix",
        split_axis=0,
        concat_axis=0,
        tiled=True,
    )
    row_layout = landed_to_rows(landed, groups, slab, cols_own)
    even_one, odd_one = transform_last(row_layout[:, 0], row_layout[:, 1], 1.0)
    even_two, odd_two = transform_last(row_layout[:, 2], row_layout[:, 3], 1.0)
    shear_one = jnp.stack([even_one, odd_one], axis=1).reshape(planes, slab, L)
    shear_two = jnp.stack([even_two, odd_two], axis=1).reshape(planes, slab, L)
    return (convergence, shear_one * scale, shear_two * scale)


def bf16_pair(value):
    high = value.astype(jnp.bfloat16)
    return (high, (value - high.astype(jnp.float32)).astype(jnp.bfloat16))


def dft_block(size, sign_value):
    turn = 2.0 * np.pi / size * (np.outer(np.arange(size), np.arange(size)) % size)
    cosine, sine = (np.cos(turn), sign_value * np.sin(turn))
    whole = np.block([[cosine, sine], [-sine, cosine]]).astype(np.float32)
    high = whole.astype(jnp.bfloat16)
    low = (whole - high.astype(np.float32)).astype(jnp.bfloat16)
    return np.stack([high, low])


def twiddle_pair(outer, inner):
    turn = 2.0 * np.pi / (outer * inner) * np.outer(np.arange(outer), np.arange(inner))
    return np.stack([np.cos(turn), np.sin(turn)]).astype(np.float32)


def quarter(values, sign_value):
    (ar, ai), (br, bi), (cr, ci), (dr, di) = values
    pr, pi, mr, mi = (ar + cr, ai + ci, ar - cr, ai - ci)
    qr, qi, nr, ni = (br + dr, bi + di, br - dr, bi - di)
    if sign_value < 0:
        return [(pr + qr, pi + qi), (mr + ni, mi - nr), (pr - qr, pi - qi), (mr - ni, mi + nr)]
    return [(pr + qr, pi + qi), (mr - ni, mi + nr), (pr - qr, pi - qi), (mr + ni, mi - nr)]


def rotate(value, step, sign_value):
    real_part, imag_part = value
    if step == 0:
        return value
    if step == 4:
        return (-sign_value * imag_part, sign_value * real_part)
    cosine = math.cos(2.0 * math.pi * step / 16)
    sine = sign_value * math.sin(2.0 * math.pi * step / 16)
    return (real_part * cosine - imag_part * sine, real_part * sine + imag_part * cosine)


def sixteen(values, sign_value, count=16):
    inner = [quarter([values[4 * a + b] for a in range(4)], sign_value) for b in range(4)]
    result = [None] * 16
    for k in range(4):
        turned_values = [rotate(inner[b][k], b * k, sign_value) for b in range(4)]
        for place, value in enumerate(quarter(turned_values, sign_value)):
            result[k + 4 * place] = value
    return result[:count]


def dot3(left, right):
    mul = partial(jnp.dot, preferred_element_type=jnp.float32)
    (left_high, left_low), (right_high, right_low) = (left, right)
    return mul(left_high, right_high) + (mul(left_low, right_high) + mul(left_high, right_low))


def widen_kernel(cell_ref, mass_ref, out_ref):
    out_ref[0] = cell_ref[...].astype(jnp.float32)
    out_ref[1] = mass_ref[...].astype(jnp.float32)


def divided(value, count):
    return value >> (count.bit_length() - 1) if count & (count - 1) == 0 else lax.div(value, count)


def pack_kernel(half, cap, per_owner, which, at_ref, table_ref, raw_ref, out_ref, *count_refs):
    _, planes, local_tiles, per_tile = raw_ref.shape
    groups = out_ref.shape[0]
    chunks = per_tile // TC
    lines = 2 * chunks * cap
    out_ref[...] = jnp.zeros(out_ref.shape, jnp.float32)
    base = at_ref[which] * local_tiles
    for place in range(groups):
        for count_ref in count_refs:
            count_ref[place] = 0

    @pl.loop(0, local_tiles // 8)
    def _(bunch):
        here = pl.ds(pl.multiple_of(bunch * 8, 8), 8)
        lists = [[raw_ref[kind, plane, here, :] for kind in range(2)] for plane in range(planes)]
        for at in range(8):
            for plane, count_ref in enumerate(count_refs):
                owner = divided(table_ref[plane, base + bunch * 8 + at], per_owner)
                upper = divided(owner, half)
                low = owner - upper * half
                place = ((upper + low) & 1) * half + low
                rank = count_ref[place]
                count_ref[place] = rank + 1
                for kind, values in enumerate(lists[plane]):
                    for chunk in range(chunks):
                        row = plane * lines + kind * chunks * cap + chunk * cap + rank
                        out_ref[place, pl.ds(row, 1), :] = values[at : at + 1, chunk * TC : (chunk + 1) * TC]

    for plane in range(planes):
        total = jnp.sum(raw_ref[1, plane], axis=0, keepdims=True)
        total = jnp.sum(total, axis=1, keepdims=True)
        line = jnp.broadcast_to(total, (1, TC))
        for place in range(groups):
            out_ref[place, planes * lines + plane : planes * lines + plane + 1, :] = line


def deposit_kernel(cap, chunks, slots_ref, recv_ref, out_ref):
    out_ref[...] = jnp.zeros(out_ref.shape, jnp.float32)
    all_planes = out_ref.shape[0]
    planes = all_planes // 2
    half = recv_ref.shape[0] // 2
    width = 32
    bunch = 4
    parts = TC // width
    low = lax.broadcasted_iota(jnp.int32, (TR, TC), 0).astype(jnp.float32)
    lines = [(low + float(TR * part)).astype(jnp.bfloat16) for part in range(parts)]
    one = jnp.ones((TR, TC), jnp.bfloat16)
    none = jnp.zeros((TR, TC), jnp.bfloat16)

    def spread(value, slot):
        return jnp.broadcast_to(value[slot : slot + 1, :], (TR, TC)).astype(jnp.bfloat16)

    for plane in range(all_planes):
        start = (plane % planes) * 2 * chunks * cap

        @pl.loop(0, half, unroll=True)
        def _(source):
            place = (plane // planes) * half + source
            cells = [recv_ref[place, start + k * cap : start + (k + 1) * cap, :] for k in range(chunks)]
            weights = [
                recv_ref[place, start + (chunks + k) * cap : start + (chunks + k + 1) * cap, :] for k in range(chunks)
            ]
            rows = [jnp.floor(cell * (1.0 / TC)) for cell in cells]
            strips = [jnp.floor(cell * (1.0 / width)) for cell in cells]
            cols = [cell - strip * float(width) for cell, strip in zip(cells, strips)]
            rows = [row + (strip - row * float(parts)) * float(TR) for row, strip in zip(rows, strips)]
            sums = []
            for first in range(0, cap, bunch):
                row_hot = []
                col_hot = []
                for k in range(chunks):
                    row_lines = []
                    col_lines = []
                    for slot in range(first, first + bunch):
                        row = spread(rows[k], slot)
                        weight = spread(weights[k], slot)
                        row_lines += [jnp.where(lines[at] == row, weight, none) for at in range(parts)]
                        col = spread(cols[k], slot)
                        col_lines += [jnp.where(lines[at] == col, one, none) for at in range(width // TR)]
                    row_hot.append(jnp.concatenate(row_lines, axis=0))
                    col_hot.append(jnp.concatenate(col_lines, axis=0))
                done = lax.dot_general(
                    jnp.concatenate(row_hot, axis=1),
                    jnp.concatenate(col_hot, axis=1),
                    (((1,), (1,)), ((), ())),
                    preferred_element_type=jnp.float32,
                )
                for at in range(bunch):
                    base = at * TR * parts
                    side = slice(at * width, (at + 1) * width)
                    strips_of = [done[base + j * TR : base + (j + 1) * TR, side] for j in range(parts)]
                    sums.append(jnp.concatenate(strips_of, axis=1))
            for slot in range(cap):
                tile = slots_ref[(plane * half + source) * cap + slot]
                out_ref[plane, tile] = out_ref[plane, tile] + sums[slot]


def rows_kernel(
    cap, chunks, weight_ref, at_ref, slots_ref, near_dens_ref, near_ref, far_ref, twiddle_ref, table_ref,
    mine_ref, other_ref, out_ref, high_ref, low_ref, far_dens_ref, dens_ref, maps_ref, copied,
):
    step = pl.program_id(0)

    @pl.when(step == 0)
    def _():
        fetch = pltpu.make_async_copy(near_dens_ref, dens_ref, copied)
        fetch.start()
        deposit_kernel(cap, chunks, slots_ref, far_ref, far_dens_ref)
        fetch.wait()

    planes, slab, length = mine_ref.shape
    all_planes = far_dens_ref.shape[0]
    first_line = planes * 2 * cap * chunks
    outer = length // TC
    first_tile = step * (slab // TR * outer)
    half = near_ref.shape[0] // 2
    scales = []
    for plane in range(all_planes):
        line = plane % planes
        total = jnp.zeros((1, TC), jnp.float32)
        for source in range(half):
            place = (plane // planes) * half + source
            total = total + near_ref[place, line : line + 1, :]
            total = total + far_ref[place, first_line + line : first_line + line + 1, :]
        scales.append(float(length * length) / total)
    factors = [
        [jnp.broadcast_to(weight_ref[i, j] * scales[j], (TR, TC)) for j in range(i + 1)] for i in range(all_planes)
    ]
    shift = [weight_ref[i, all_planes] for i in range(all_planes)]
    first_shell = at_ref[2] == 0
    for line in range(slab // TR):
        here = slice(line * TR, (line + 1) * TR)
        for col in range(outer):
            at = line * outer + col
            tiles = [dens_ref[j, first_tile + at] + far_dens_ref[j, first_tile + at] for j in range(all_planes)]
            maps = []
            for i in range(all_planes):
                field = tiles[0] * factors[i][0]
                for j in range(1, i + 1):
                    field = field + tiles[j] * factors[i][j]
                maps.append(field - shift[i])
                maps_ref[i, at] = maps[i]
            side = slice(col * TC, (col + 1) * TC)
            for i in range(planes):
                mine_ref[i, here, side] = jnp.where(first_shell, maps[i], maps[planes + i])
                other_ref[i, here, side] = jnp.where(first_shell, maps[planes + i], maps[i])

    table = (table_ref[0], table_ref[1])
    for pair in range(all_planes // 2):
        for line in range(slab // TR):
            values = [tuple(maps_ref[2 * pair + i, line * outer + col] for i in range(2)) for col in range(outer)]
            for place, (real_part, imag_part) in enumerate(sixteen(values, -1.0)):
                if place:
                    cosine = twiddle_ref[0, place : place + 1, :]
                    sine = twiddle_ref[1, place : place + 1, :]
                    real_part, imag_part = (
                        real_part * cosine + imag_part * sine,
                        imag_part * cosine - real_part * sine,
                    )
                spot = slice(place * slab + line * TR, place * slab + (line + 1) * TR)
                for at, value in enumerate((real_part, imag_part)):
                    high, low = bf16_pair(value)
                    high_ref[pair, spot, at * TC : (at + 1) * TC] = high
                    low_ref[pair, spot, at * TC : (at + 1) * TC] = low

        done = dot3((high_ref[pair], low_ref[pair]), table)
        for place in range(outer):
            here = slice(place * slab, (place + 1) * slab)
            out_ref[pair * half + place // 2, place % 2, 0] = done[here, :TC]
            out_ref[pair * half + place // 2, place % 2, 1] = done[here, TC:]


def turned(turn_ref, place, here, value, sign_value):
    if place == 0:
        return value
    real_part, imag_part = value
    shape = real_part.shape
    cosine = jnp.broadcast_to(turn_ref[0, here, place : place + 1], shape)
    sine = jnp.broadcast_to(turn_ref[1, here, place : place + 1], shape) * sign_value
    return (real_part * cosine - imag_part * sine, real_part * sine + imag_part * cosine)


def filters_kernel(length, at_ref, out_ref):
    _, _, outer, inner, lanes = out_ref.shape
    middle = length // 2
    wave_v = lax.broadcasted_iota(jnp.int32, (inner, lanes), 1) * outer + (2 * at_ref[4] + pl.program_id(0))
    keep_v = wave_v != middle
    sv = jnp.where(wave_v >= middle, wave_v - length, wave_v).astype(jnp.float32)
    line_u = lax.broadcasted_iota(jnp.int32, (inner, lanes), 0) * outer
    flip = jnp.where(at_ref[5] > 0, -1.0, 1.0)
    for place in range(outer):
        wave_u = line_u + place
        su = jnp.where(wave_u >= middle, wave_u - length, wave_u).astype(jnp.float32)
        scale = 1.0 / (float(length) * float(length))
        keep = jnp.where(keep_v & (wave_u != middle), scale * flip if place % 2 else scale, 0.0)
        factor = keep / jnp.maximum(sv * sv + su * su, 1.0)
        out_ref[0, 0, place] = factor * (sv * sv - su * su)
        out_ref[0, 1, place] = factor * (2.0 * sv * su)


def columns_kernel(
    order, filters_ref, in_ref, turn_ref, forward_ref, back_ref, out_ref,
    high_ref, low_ref, spectrum_ref, back_f, filter_ref, copied,
):
    fetch = pltpu.make_async_copy(filters_ref.at[pl.program_id(0)], filter_ref, copied)
    fetch.start()
    outer, _, _, inner, lanes = in_ref.shape
    forward = (forward_ref[0], forward_ref[1])
    back = (back_ref[0], back_ref[1])

    @pl.loop(0, inner // TR, unroll=True)
    def _(line):
        here = pl.ds(line * TR, TR)
        there = pl.ds(inner + line * TR, TR)
        values = [(in_ref[place, 0, 0, here, :], in_ref[place, 0, 1, here, :]) for place in order]
        for place, value in enumerate(sixteen(values, -1.0)):
            for spot, part in zip((here, there), turned(turn_ref, place, here, value, -1.0)):
                high, low = bf16_pair(part)
                high_ref[spot, place * lanes : (place + 1) * lanes] = high
                low_ref[spot, place * lanes : (place + 1) * lanes] = low

    for bunch in range(outer // 2):
        span = slice(bunch * 2 * lanes, (bunch + 1) * 2 * lanes)
        spectrum_ref[:, span] = dot3(forward, (high_ref[:, span], low_ref[:, span]))

    fetch.wait()
    for place in range(outer):
        side = slice(place * lanes, (place + 1) * lanes)
        first = filter_ref[0, place]
        second = filter_ref[1, place]
        real_part = spectrum_ref[:inner, side]
        imag_part = spectrum_ref[inner:, side]
        stacked = jnp.concatenate(
            [
                jnp.concatenate([real_part * first, real_part * second], axis=1),
                jnp.concatenate([imag_part * first, imag_part * second], axis=1),
            ],
            axis=0,
        )
        back_f[place] = dot3(back, bf16_pair(stacked))

    half = outer // 2

    @pl.loop(0, inner // TR, unroll=True)
    def _(line):
        here = pl.ds(line * TR, TR)
        there = pl.ds(inner + line * TR, TR)
        for field in range(2):
            side = slice(field * lanes, (field + 1) * lanes)
            values = [
                turned(turn_ref, place, here, (back_f[place, here, side], back_f[place, there, side]), 1.0)
                for place in range(outer)
            ]
            for low, (real_part, imag_part) in enumerate(sixteen(values, 1.0, half)):
                out_ref[low, 0, field, 0, here, :] = real_part
                out_ref[low, 0, field, 1, here, :] = imag_part


def inverse_rows_kernel(in_ref, twiddle_ref, table_ref, first_ref, second_ref, back_f):
    half, _, _, _, slab, lanes = in_ref.shape
    outer = 2 * half
    table = (table_ref[0], table_ref[1])
    for field, out_ref in enumerate((first_ref, second_ref)):
        joined = [
            jnp.concatenate([in_ref[place // 2, place % 2, field, part] for place in range(outer)], axis=0)
            for part in range(2)
        ]
        back_f[...] = dot3(bf16_pair(jnp.concatenate(joined, axis=1)), table)
        for line in range(slab // TR):
            here = slice(line * TR, (line + 1) * TR)
            values = []
            for place in range(outer):
                spot = slice(place * slab + line * TR, place * slab + (line + 1) * TR)
                real_part = back_f[spot, :lanes]
                imag_part = back_f[spot, lanes:]
                if place:
                    cosine = twiddle_ref[0, place : place + 1, :]
                    sine = twiddle_ref[1, place : place + 1, :]
                    real_part, imag_part = (
                        real_part * cosine - imag_part * sine,
                        real_part * sine + imag_part * cosine,
                    )
                values.append((real_part, imag_part))
            for place, (real_part, imag_part) in enumerate(sixteen(values, 1.0)):
                out_ref[0, here, place * lanes : (place + 1) * lanes] = real_part
                out_ref[1, here, place * lanes : (place + 1) * lanes] = imag_part


VMEM = pl.BlockSpec(memory_space=pltpu.VMEM)
SMEM = pl.BlockSpec(memory_space=pltpu.SMEM)


def room(mib):
    return pltpu.CompilerParams(vmem_limit_bytes=mib * 1024 * 1024)


def in_hbm(value):
    return pltpu.with_memory_space_constraint(value, pltpu.HBM)


def whole(shape):
    return pl.BlockSpec(shape, lambda step: (0,) * len(shape))


def slot_tiles(table, held, per_owner, cap):
    local_tiles = table.shape[-1]
    mine = table // per_owner == held
    earlier = jnp.arange(local_tiles)[:, None] < jnp.arange(local_tiles)[None, :]
    rank = jnp.sum(jnp.where(mine[..., :, None] & earlier, 1, 0), axis=-2)
    chosen = mine[..., None, :] & (rank[..., None, :] == jnp.arange(cap)[:, None])
    spot = table - held * per_owner
    return jnp.sum(jnp.where(chosen, spot[..., None, :], 0), axis=-1)


def cube_exchange(value):
    return lax.all_to_all(value, ("shell", "low"), split_axis=0, concat_axis=0, tiled=True)


def local_cube(block_tile, cell_index, masses, plane_coef, plane_dist, source_inv):
    half = lax.axis_size("low")
    groups = 2 * half
    shell = lax.axis_index("shell")
    upper = lax.axis_index("upper")
    low = lax.axis_index("low")
    planes, local_tiles, per_tile = cell_index.shape
    slab = L // groups
    outer = L // TC
    per_owner = slab // TR * outer
    cap = max(1, 2 * local_tiles // groups)
    chunks = per_tile // TC
    lines = 2 * chunks * cap * planes
    part = (shell + low) % 2
    held = part * half + low
    order = [((s // half + s % 2) % 2) * half + s % half for s in range(groups)]

    raw = pl.pallas_call(
        widen_kernel,
        in_specs=[VMEM, VMEM],
        out_specs=VMEM,
        out_shape=jax.ShapeDtypeStruct((2, planes, local_tiles, per_tile), jnp.float32),
        compiler_params=room(8),
        name="widen",
    )(in_hbm(cell_index), in_hbm(masses))
    raw_far = lax.ppermute(raw, "upper", [(0, 1), (1, 0)])

    here = jnp.stack([upper * half + low, (1 - upper) * half + low, shell, 1 - shell, low, upper]).astype(jnp.int32)

    def pack(which, lists):
        return pl.pallas_call(
            partial(pack_kernel, half, cap, per_owner, which),
            in_specs=[SMEM, SMEM, VMEM],
            out_specs=VMEM,
            out_shape=jax.ShapeDtypeStruct((groups, lines + 8, TC), jnp.float32),
            scratch_shapes=[pltpu.SMEM((groups,), jnp.int32)] * planes,
            compiler_params=room(12),
            name="pack",
        )(here, block_tile, lists)

    near = cube_exchange(pack(0, raw))
    far = cube_exchange(pack(1, raw_far))

    note = jnp.concatenate(
        [block_tile.astype(jnp.float32), plane_coef[:, None], (plane_coef * plane_dist)[:, None], source_inv[:, None]],
        axis=1,
    )
    other = lax.ppermute(note, "shell", [(0, 1), (1, 0)])
    both = jnp.where(shell == 0, jnp.concatenate([note, other]), jnp.concatenate([other, note]))
    tiles = slot_tiles(
        both[:, : groups * local_tiles].astype(jnp.int32).reshape(2 * planes, groups, local_tiles), held, per_owner, cap
    )
    tiles = tiles.reshape(2 * planes, 2, half, cap)
    near_slots = lax.dynamic_index_in_dim(tiles, upper, axis=1, keepdims=False).reshape(-1)
    far_slots = lax.dynamic_index_in_dim(tiles, 1 - upper, axis=1, keepdims=False).reshape(-1)
    maps = jnp.arange(2 * planes)
    weight = jnp.where(
        maps[None, :] <= maps[:, None], both[None, :, -3] - both[:, -1][:, None] * both[None, :, -2], 0.0
    )
    weight = jnp.concatenate([weight, jnp.sum(weight, axis=1, keepdims=True)], axis=1)

    filters = pl.pallas_call(
        partial(filters_kernel, L),
        grid=(2,),
        in_specs=[SMEM],
        out_specs=pl.BlockSpec((1, 2, outer, slab, TC), lambda step: (step, 0, 0, 0, 0)),
        out_shape=pltpu.HBM((2, 2, outer, slab, TC), jnp.float32),
        compiler_params=room(16),
        name="filters",
    )(here)
    near_dens = pl.pallas_call(
        partial(deposit_kernel, cap, chunks),
        in_specs=[SMEM, VMEM],
        out_specs=VMEM,
        out_shape=pltpu.HBM((2 * planes, per_owner, TR, TC), jnp.float32),
        compiler_params=room(16),
        name="deposit",
    )(near_slots, near)
    twiddle = jnp.asarray(twiddle_pair(outer, TC))
    turn = jnp.asarray(twiddle_pair(outer, TC).transpose(0, 2, 1))
    minus = jnp.asarray(dft_block(TC, -1.0))
    plus = jnp.asarray(dft_block(TC, 1.0))
    field = jax.ShapeDtypeStruct((planes, slab, L), jnp.float32)
    some = 2 * TR
    conv_mine, conv_other, row_sent = pl.pallas_call(
        partial(rows_kernel, cap, chunks),
        grid=(slab // some,),
        in_specs=[
            SMEM,
            SMEM,
            SMEM,
            pl.BlockSpec(memory_space=pltpu.HBM),
            pl.BlockSpec((groups, 8, TC), lambda step: (0, lines // 8, 0)),
            whole(far.shape),
            whole(twiddle.shape),
            whole(minus.shape),
        ],
        out_specs=(
            pl.BlockSpec((planes, some, L), lambda step: (0, step, 0)),
            pl.BlockSpec((planes, some, L), lambda step: (0, step, 0)),
            pl.BlockSpec((groups, 2, 2, some, TC), lambda step: (0, 0, 0, step, 0)),
        ),
        out_shape=(
            pltpu.HBM(field.shape, field.dtype),
            pltpu.HBM(field.shape, field.dtype),
            pltpu.HBM((groups, 2, 2, slab, TC), jnp.float32),
        ),
        scratch_shapes=[
            pltpu.VMEM((2, outer * some, 2 * TC), jnp.bfloat16),
            pltpu.VMEM((2, outer * some, 2 * TC), jnp.bfloat16),
            pltpu.VMEM((2 * planes, per_owner, TR, TC), jnp.float32),
            pltpu.VMEM((2 * planes, per_owner, TR, TC), jnp.float32),
            pltpu.VMEM((2 * planes, some // TR * outer, TR, TC), jnp.float32),
            pltpu.SemaphoreType.DMA(()),
        ],
        compiler_params=room(28),
        name="rows",
    )(weight, here, far_slots, in_hbm(near_dens), near, far, twiddle, minus)
    arrived = lax.all_to_all(row_sent, ("shell", "low"), split_axis=0, concat_axis=0, tiled=True)
    swaps = []
    for side in range(2):
        for top in range(2):
            for at in range(half):
                if (side + at) % 2 == top:
                    swaps.append(((side * 2 + top) * half + at, ((1 - side) * 2 + top) * half + at))
    conv_held = lax.ppermute(conv_other, ("shell", "upper", "low"), swaps)
    convergence = jnp.where(part == upper, conv_mine, conv_held)
    col_sent = pl.pallas_call(
        partial(columns_kernel, order),
        grid=(2,),
        in_specs=[
            pl.BlockSpec(memory_space=pltpu.HBM),
            pl.BlockSpec((groups, 1, 2, slab, TC), lambda step: (0, step, 0, 0, 0)),
            whole(turn.shape),
            whole(plus.shape),
            whole(minus.shape),
        ],
        out_specs=pl.BlockSpec((half, 1, 2, 2, slab, TC), lambda step: (0, step, 0, 0, 0, 0)),
        out_shape=pltpu.HBM((half, 2, 2, 2, slab, TC), jnp.float32),
        scratch_shapes=[
            pltpu.VMEM((2 * slab, L), jnp.bfloat16),
            pltpu.VMEM((2 * slab, L), jnp.bfloat16),
            pltpu.VMEM((2 * slab, L), jnp.float32),
            pltpu.VMEM((outer, 2 * slab, 2 * TC), jnp.float32),
            pltpu.VMEM((2, outer, slab, TC), jnp.float32),
            pltpu.SemaphoreType.DMA(()),
        ],
        compiler_params=room(32),
        name="columns",
    )(in_hbm(filters), arrived, turn, plus, minus)
    landed = lax.all_to_all(col_sent, "low", split_axis=0, concat_axis=0, tiled=True)
    shear_one, shear_two = pl.pallas_call(
        inverse_rows_kernel,
        grid=(slab // some,),
        in_specs=[
            pl.BlockSpec((half, 2, 2, 2, some, TC), lambda step: (0, 0, 0, 0, step, 0)),
            whole(twiddle.shape),
            whole(plus.shape),
        ],
        out_specs=(
            pl.BlockSpec((planes, some, L), lambda step: (0, step, 0)),
            pl.BlockSpec((planes, some, L), lambda step: (0, step, 0)),
        ),
        out_shape=(field, field),
        scratch_shapes=[pltpu.VMEM((outer * some, 2 * TC), jnp.float32)],
        compiler_params=room(24),
        name="inverse_rows",
    )(landed, twiddle, plus)
    return (convergence, shear_one, shear_two)


def solution(mesh):
    shells, groups = (mesh.shape["shell"], mesh.shape["pix"])
    body, pix = (local, "pix")
    if shells == 2 and groups * TC == L:
        body, pix = (local_cube, ("upper", "low"))
        mesh = type(mesh)(mesh.devices.reshape(shells, 2, groups // 2), ("shell", "upper", "low"))
    placed = (P("shell", None), P("shell", pix, None), P("shell", pix, None), P("shell"), P("shell"), P("shell"))
    out = P("shell", pix, None)

    def step(*arrays):
        return body(*arrays)

    return jax.shard_map(step, mesh=mesh, in_specs=placed, out_specs=(out, out, out), check_vma=False)
```

```python
from functools import partial
import math

import jax
import jax.numpy as jnp
import numpy as np
from jax import lax
from jax.experimental import pallas as pl
from jax.experimental.pallas import tpu as pltpu
from jax.sharding import PartitionSpec as P

L = 2048
TR = 16
TC = 128


HIGHEST = lax.Precision.HIGHEST


def entering(value, axis, join, neutral):
    count, mine = (lax.axis_size(axis), lax.axis_index(axis))
    pieces = jax.tree.map(lambda part: lax.all_gather(part, axis), value)
    running = jax.tree.map(
        lambda part, zero: jnp.full_like(part, 0) + jnp.asarray(zero, part.dtype), value, neutral
    )

    def lap(position, running):
        longer = join(running, jax.tree.map(lambda part: part[position], pieces))
        return jax.tree.map(lambda new, old: jnp.where(position < mine, new, old), longer, running)

    return lax.fori_loop(0, count - 1, lap, running)


def dft_table(left_size, right_size, period, sign_value):
    left_idx = jnp.arange(left_size)[:, None]
    right_idx = jnp.arange(right_size)[None, :]
    angle = 2.0 * math.pi / period * (left_idx * right_idx % period).astype(jnp.float32)
    return (jnp.cos(angle), sign_value * jnp.sin(angle))


def mix_outer(table, real_part, imag_part):
    cosine, sine_part = table
    contract = partial(jnp.einsum, "ab,...bc->...ac", precision=HIGHEST)
    return (
        contract(cosine, real_part) - contract(sine_part, imag_part),
        contract(sine_part, real_part) + contract(cosine, imag_part),
    )


def mix_inner(table, real_part, imag_part):
    cosine, sine_part = table
    product = partial(jnp.matmul, precision=HIGHEST)
    return (
        product(real_part, cosine) - product(imag_part, sine_part),
        product(real_part, sine_part) + product(imag_part, cosine),
    )


def twist(table, real_part, imag_part):
    cosine, sine_part = table
    return (real_part * cosine - imag_part * sine_part, real_part * sine_part + imag_part * cosine)


def transform_last(real_part, imag_part, sign_value):
    length = real_part.shape[-1]
    inner = math.gcd(length, 128)
    outer = length // inner
    leading = real_part.shape[:-1]
    real_part = real_part.reshape(leading + (outer, inner))
    imag_part = imag_part.reshape(leading + (outer, inner))
    outer_table = dft_table(outer, outer, outer, sign_value)
    inner_table = dft_table(inner, inner, inner, sign_value)
    twiddle = dft_table(outer, inner, length, sign_value)
    if sign_value < 0:
        real_part, imag_part = mix_outer(outer_table, real_part, imag_part)
        real_part, imag_part = twist(twiddle, real_part, imag_part)
        real_part, imag_part = mix_inner(inner_table, real_part, imag_part)
    else:
        real_part, imag_part = mix_inner(inner_table, real_part, imag_part)
        real_part, imag_part = twist(twiddle, real_part, imag_part)
        real_part, imag_part = mix_outer(outer_table, real_part, imag_part)
    return (real_part.reshape(leading + (length,)), imag_part.reshape(leading + (length,)))


def frequency_of(position, length):
    inner = math.gcd(length, 128)
    outer = length // inner
    frequency = position // inner + outer * (position % inner)
    signed = jnp.where(frequency >= length // 2, frequency - length, frequency).astype(jnp.float32)
    keep_mask = (frequency != length // 2).astype(jnp.float32)
    return (signed, keep_mask)


def add_pairs(earlier_pair, later_pair):
    return (earlier_pair[0] + later_pair[0], earlier_pair[1] + later_pair[1])


def deposit_group(item):
    cell_ids, weights = item
    tile_rows = cell_ids // TC
    tile_cols = cell_ids % TC
    row_hot = jnp.where(
        tile_rows[:, None, :] == jnp.arange(TR)[None, :, None],
        weights[:, None, :],
        jnp.zeros((), jnp.bfloat16),
    )
    col_hot = (tile_cols[:, :, None] == jnp.arange(TC)[None, None, :]).astype(jnp.bfloat16)
    return jnp.einsum("grk,gkc->grc", row_hot, col_hot, preferred_element_type=jnp.float32)


def rows_to_sending(packed, groups, slab, cols_own):
    count, fields = (packed.shape[0], packed.shape[1])
    return (
        packed.reshape(count, fields, slab, groups, cols_own)
        .transpose(3, 0, 1, 4, 2)
        .reshape(groups, count, fields, cols_own * slab)
    )


def arrived_to_columns(arrived, groups, slab, cols_own):
    count, fields = (arrived.shape[1], arrived.shape[2])
    return (
        arrived.reshape(groups, count, fields, cols_own, slab)
        .transpose(1, 2, 3, 0, 4)
        .reshape(count, fields, cols_own, groups * slab)
    )


def columns_to_sending(stacked, groups, slab, cols_own):
    count, fields = (stacked.shape[0], stacked.shape[1])
    return (
        stacked.reshape(count, fields, cols_own, groups, slab)
        .transpose(3, 0, 1, 2, 4)
        .reshape(groups, count, fields, cols_own * slab)
    )


def landed_to_rows(landed, groups, slab, cols_own):
    count, fields = (landed.shape[1], landed.shape[2])
    return (
        landed.reshape(groups, count, fields, cols_own, slab)
        .transpose(1, 2, 4, 0, 3)
        .reshape(count, fields, slab, groups * cols_own)
    )


def local(block_tile, cell_index, masses, plane_coef, plane_dist, source_inv):
    groups = lax.axis_size("pix")
    my_index = lax.axis_index("pix")
    planes, local_tiles, per_tile = cell_index.shape
    slab = L // groups
    per_owner = slab // TR * (L // TC)
    cap = max(1, 2 * local_tiles // groups)
    flat = TR * TC
    batch_tiles = 8
    deposited = lax.map(
        deposit_group,
        (cell_index.reshape(-1, batch_tiles, per_tile), masses.reshape(-1, batch_tiles, per_tile)),
    )
    tile_sums = deposited.reshape(planes, local_tiles, flat)
    table = block_tile.reshape(planes, groups, local_tiles)
    owner = table // per_owner
    earlier = jnp.arange(local_tiles)[:, None] < jnp.arange(local_tiles)[None, :]
    same_owner = owner[:, :, :, None] == owner[:, :, None, :]
    rank = jnp.sum(jnp.where(same_owner & earlier[None, None], 1, 0), axis=2)
    slot = owner * cap + rank
    my_slots = lax.dynamic_index_in_dim(slot, my_index, axis=1, keepdims=False)
    slot_grid = jnp.arange(groups)[:, None] * cap + jnp.arange(cap)[None, :]
    send_hot = (my_slots[:, None, None, :] == slot_grid[None, :, :, None]).astype(jnp.float32)
    outgoing = jnp.einsum("pnct,ptf->npcf", send_hot, tile_sums, precision=HIGHEST)
    incoming = lax.all_to_all(outgoing, "pix", split_axis=0, concat_axis=0, tiled=True)
    local_index = table - my_index * per_owner
    is_mine = owner == my_index
    tile_hot = (is_mine[..., None] & (local_index[..., None] == jnp.arange(per_owner))).astype(
        jnp.float32
    )
    slot_hot = (rank[..., None] == jnp.arange(cap)).astype(jnp.float32)
    placing = jnp.einsum("pstl,pstc->plsc", tile_hot, slot_hot, precision=HIGHEST)
    slab_tiles = jnp.einsum("plsc,spcf->plf", placing, incoming, precision=HIGHEST)
    density = (
        slab_tiles.reshape(planes, slab // TR, L // TC, TR, TC)
        .transpose(0, 1, 3, 2, 4)
        .reshape(planes, slab, L)
    )
    total = lax.psum(jnp.sum(density, axis=(1, 2)), "pix")
    contrast = density / (total / (L * L))[:, None, None] - 1.0
    near_local = jnp.cumsum(plane_coef[:, None, None] * contrast, axis=0)
    far_local = jnp.cumsum((plane_coef * plane_dist)[:, None, None] * contrast, axis=0)
    blank = jnp.zeros((slab, L), jnp.float32)
    near_before, far_before = entering(
        (near_local[-1], far_local[-1]), "shell", add_pairs, (blank, blank)
    )
    convergence = near_before + near_local - source_inv[:, None, None] * (far_before + far_local)
    cols_own = L // groups
    wave_x, keep_x = frequency_of(my_index * cols_own + jnp.arange(cols_own), L)
    wave_y, keep_y = frequency_of(jnp.arange(L), L)
    wave_x = wave_x[:, None]
    wave_y = wave_y[None, :]
    both_keep = keep_x[:, None] * keep_y[None, :]
    wave_power = jnp.maximum(wave_x * wave_x + wave_y * wave_y, 1.0)
    kernel_one = both_keep * (wave_x * wave_x - wave_y * wave_y) / wave_power
    kernel_two = both_keep * 2.0 * wave_x * wave_y / wave_power
    scale = 1.0 / (L * L)
    spec_real, spec_imag = transform_last(convergence[0::2], convergence[1::2], -1.0)
    sending = rows_to_sending(jnp.stack([spec_real, spec_imag], axis=1), groups, slab, cols_own)
    arrived = lax.all_to_all(sending, "pix", split_axis=0, concat_axis=0, tiled=True)
    columns = arrived_to_columns(arrived, groups, slab, cols_own)
    row_real, row_imag = transform_last(columns[:, 0], columns[:, 1], -1.0)
    first_real, first_imag = transform_last(row_real * kernel_one, row_imag * kernel_one, 1.0)
    second_real, second_imag = transform_last(row_real * kernel_two, row_imag * kernel_two, 1.0)
    stacked = jnp.stack([first_real, first_imag, second_real, second_imag], axis=1)
    landed = lax.all_to_all(
        columns_to_sending(stacked, groups, slab, cols_own),
        "pix",
        split_axis=0,
        concat_axis=0,
        tiled=True,
    )
    row_layout = landed_to_rows(landed, groups, slab, cols_own)
    even_one, odd_one = transform_last(row_layout[:, 0], row_layout[:, 1], 1.0)
    even_two, odd_two = transform_last(row_layout[:, 2], row_layout[:, 3], 1.0)
    shear_one = jnp.stack([even_one, odd_one], axis=1).reshape(planes, slab, L)
    shear_two = jnp.stack([even_two, odd_two], axis=1).reshape(planes, slab, L)
    return (convergence, shear_one * scale, shear_two * scale)


def bf16_pair(value):
    high = value.astype(jnp.bfloat16)
    return (high, (value - high.astype(jnp.float32)).astype(jnp.bfloat16))


def dft_block(size, sign_value):
    turn = 2.0 * np.pi / size * (np.outer(np.arange(size), np.arange(size)) % size)
    cosine, sine = (np.cos(turn), sign_value * np.sin(turn))
    whole = np.block([[cosine, sine], [-sine, cosine]]).astype(np.float32)
    high = whole.astype(jnp.bfloat16)
    low = (whole - high.astype(np.float32)).astype(jnp.bfloat16)
    return np.stack([high, low])


def twiddle_pair(outer, inner):
    turn = 2.0 * np.pi / (outer * inner) * np.outer(np.arange(outer), np.arange(inner))
    return np.stack([np.cos(turn), np.sin(turn)]).astype(np.float32)


def quarter(values, sign_value):
    (ar, ai), (br, bi), (cr, ci), (dr, di) = values
    pr, pi, mr, mi = (ar + cr, ai + ci, ar - cr, ai - ci)
    qr, qi, nr, ni = (br + dr, bi + di, br - dr, bi - di)
    if sign_value < 0:
        return [(pr + qr, pi + qi), (mr + ni, mi - nr), (pr - qr, pi - qi), (mr - ni, mi + nr)]
    return [(pr + qr, pi + qi), (mr - ni, mi + nr), (pr - qr, pi - qi), (mr + ni, mi - nr)]


def rotate(value, step, sign_value):
    real_part, imag_part = value
    if step == 0:
        return value
    if step == 4:
        return (-sign_value * imag_part, sign_value * real_part)
    cosine = math.cos(2.0 * math.pi * step / 16)
    sine = sign_value * math.sin(2.0 * math.pi * step / 16)
    return (real_part * cosine - imag_part * sine, real_part * sine + imag_part * cosine)


def sixteen(values, sign_value, count=16):
    inner = [quarter([values[4 * a + b] for a in range(4)], sign_value) for b in range(4)]
    result = [None] * 16
    for k in range(4):
        turned_values = [rotate(inner[b][k], b * k, sign_value) for b in range(4)]
        for place, value in enumerate(quarter(turned_values, sign_value)):
            result[k + 4 * place] = value
    return result[:count]


def dot3(left, right):
    mul = partial(jnp.dot, preferred_element_type=jnp.float32)
    (left_high, left_low), (right_high, right_low) = (left, right)
    return mul(left_high, right_high) + (mul(left_low, right_high) + mul(left_high, right_low))


def widen_kernel(cell_ref, mass_ref, all_ref, first_ref):
    cells = cell_ref[...].astype(jnp.float32)
    weights = mass_ref[...].astype(jnp.float32)
    all_ref[0] = cells
    all_ref[1] = weights
    first_ref[0] = cells[:1]
    first_ref[1] = weights[:1]


def divided(value, count):
    return value >> (count.bit_length() - 1) if count & (count - 1) == 0 else lax.div(value, count)


def pack_kernel(half, cap, per_owner, which, at_ref, table_ref, raw_ref, out_ref, *count_refs):
    _, planes, local_tiles, per_tile = raw_ref.shape
    groups = out_ref.shape[0]
    chunks = per_tile // TC
    lines = 2 * chunks * cap
    out_ref[...] = jnp.zeros(out_ref.shape, jnp.float32)
    base = at_ref[which] * local_tiles
    for place in range(groups):
        for count_ref in count_refs:
            count_ref[place] = 0

    @pl.loop(0, local_tiles // 8)
    def _(bunch):
        here = pl.ds(pl.multiple_of(bunch * 8, 8), 8)
        lists = [[raw_ref[kind, plane, here, :] for kind in range(2)] for plane in range(planes)]
        for at in range(8):
            for plane, count_ref in enumerate(count_refs):
                owner = divided(table_ref[plane, base + bunch * 8 + at], per_owner)
                upper = divided(owner, half)
                low = owner - upper * half
                place = ((upper + low) & 1) * half + low
                rank = count_ref[place]
                count_ref[place] = rank + 1
                for kind, values in enumerate(lists[plane]):
                    for chunk in range(chunks):
                        row = plane * lines + kind * chunks * cap + chunk * cap + rank
                        out_ref[place, pl.ds(row, 1), :] = values[at : at + 1, chunk * TC : (chunk + 1) * TC]

    if out_ref.shape[1] == planes * lines:
        return
    for plane in range(planes):
        total = jnp.sum(raw_ref[1, plane], axis=0, keepdims=True)
        total = jnp.sum(total, axis=1, keepdims=True)
        line = jnp.broadcast_to(total, (1, TC))
        for place in range(groups):
            out_ref[place, planes * lines + plane : planes * lines + plane + 1, :] = line


def deposit_into(cap, chunks, out_ref, out_planes, slots_ref, slot_planes, recv_ref, starts):
    half = recv_ref.shape[0] // 2
    width = 32
    bunch = 4
    parts = TC // width
    low = lax.broadcasted_iota(jnp.int32, (TR, TC), 0).astype(jnp.float32)
    lines = [(low + float(TR * part)).astype(jnp.bfloat16) for part in range(parts)]
    one = jnp.ones((TR, TC), jnp.bfloat16)
    none = jnp.zeros((TR, TC), jnp.bfloat16)

    def spread(value, slot):
        return jnp.broadcast_to(value[slot : slot + 1, :], (TR, TC)).astype(jnp.bfloat16)

    for out_plane, slot_plane, (sender, start) in zip(out_planes, slot_planes, starts):

        @pl.loop(0, half, unroll=True)
        def _(source):
            place = sender * half + source
            cells = [recv_ref[place, start + k * cap : start + (k + 1) * cap, :] for k in range(chunks)]
            weights = [
                recv_ref[place, start + (chunks + k) * cap : start + (chunks + k + 1) * cap, :] for k in range(chunks)
            ]
            rows = [jnp.floor(cell * (1.0 / TC)) for cell in cells]
            strips = [jnp.floor(cell * (1.0 / width)) for cell in cells]
            cols = [cell - strip * float(width) for cell, strip in zip(cells, strips)]
            rows = [row + (strip - row * float(parts)) * float(TR) for row, strip in zip(rows, strips)]
            sums = []
            for first in range(0, cap, bunch):
                row_hot = []
                col_hot = []
                for k in range(chunks):
                    row_lines = []
                    col_lines = []
                    for slot in range(first, first + bunch):
                        row = spread(rows[k], slot)
                        weight = spread(weights[k], slot)
                        row_lines += [jnp.where(lines[at] == row, weight, none) for at in range(parts)]
                        col = spread(cols[k], slot)
                        col_lines += [jnp.where(lines[at] == col, one, none) for at in range(width // TR)]
                    row_hot.append(jnp.concatenate(row_lines, axis=0))
                    col_hot.append(jnp.concatenate(col_lines, axis=0))
                done = lax.dot_general(
                    jnp.concatenate(row_hot, axis=1),
                    jnp.concatenate(col_hot, axis=1),
                    (((1,), (1,)), ((), ())),
                    preferred_element_type=jnp.float32,
                )
                for at in range(bunch):
                    base = at * TR * parts
                    side = slice(at * width, (at + 1) * width)
                    strips_of = [done[base + j * TR : base + (j + 1) * TR, side] for j in range(parts)]
                    sums.append(jnp.concatenate(strips_of, axis=1))
            for slot in range(cap):
                tile = slots_ref[(slot_plane * half + source) * cap + slot]
                out_ref[out_plane, tile] = out_ref[out_plane, tile] + sums[slot]


def deposit_kernel(cap, chunks, near_slots_ref, near_ref, far_slots_ref, far_ref, out_ref):
    out_ref[...] = jnp.zeros(out_ref.shape, jnp.float32)
    lines = 2 * chunks * cap
    every = range(4)
    near_starts = [(plane // 2, (plane % 2) * lines) for plane in every]
    deposit_into(cap, chunks, out_ref, every, near_slots_ref, every, near_ref, near_starts)
    deposit_into(cap, chunks, out_ref, (0, 2), far_slots_ref, (0, 2), far_ref, ((0, 0), (1, 0)))


def rows_kernel(
    cap, chunks, weight_ref, at_ref, slots_ref, some_dens_ref, near_ref, far_ref, twiddle_ref, table_ref,
    mine_ref, other_ref, out_ref, high_ref, low_ref, far_dens_ref, dens_ref, maps_ref, copied,
):
    step = pl.program_id(0)

    @pl.when(step == 0)
    def _():
        fetch = pltpu.make_async_copy(some_dens_ref, dens_ref, copied)
        fetch.start()
        far_dens_ref[...] = jnp.zeros(far_dens_ref.shape, jnp.float32)
        deposit_into(cap, chunks, far_dens_ref, (0, 1), slots_ref, (1, 3), far_ref, ((0, 0), (1, 0)))
        fetch.wait()

    planes, slab, length = mine_ref.shape
    all_planes = dens_ref.shape[0]
    first_line = 2 * cap * chunks
    outer = length // TC
    first_tile = step * (slab // TR * outer)
    half = near_ref.shape[0] // 2
    scales = []
    for plane in range(all_planes):
        line = plane % planes
        total = jnp.zeros((1, TC), jnp.float32)
        for source in range(half):
            place = (plane // planes) * half + source
            total = total + near_ref[place, line : line + 1, :]
            total = total + far_ref[place, first_line + line : first_line + line + 1, :]
        scales.append(float(length * length) / total)
    factors = [
        [jnp.broadcast_to(weight_ref[i, j] * scales[j], (TR, TC)) for j in range(i + 1)] for i in range(all_planes)
    ]
    shift = [weight_ref[i, all_planes] for i in range(all_planes)]
    first_shell = at_ref[2] == 0
    for line in range(slab // TR):
        here = slice(line * TR, (line + 1) * TR)
        for col in range(outer):
            at = line * outer + col
            tiles = [dens_ref[j, first_tile + at] for j in range(all_planes)]
            for j in range(1, all_planes, 2):
                tiles[j] = tiles[j] + far_dens_ref[j // 2, first_tile + at]
            maps = []
            for i in range(all_planes):
                field = tiles[0] * factors[i][0]
                for j in range(1, i + 1):
                    field = field + tiles[j] * factors[i][j]
                maps.append(field - shift[i])
                maps_ref[i, at] = maps[i]
            side = slice(col * TC, (col + 1) * TC)
            for i in range(planes):
                mine_ref[i, here, side] = jnp.where(first_shell, maps[i], maps[planes + i])
                other_ref[i, here, side] = jnp.where(first_shell, maps[planes + i], maps[i])

    table = (table_ref[0], table_ref[1])
    for pair in range(all_planes // 2):
        for line in range(slab // TR):
            values = [tuple(maps_ref[2 * pair + i, line * outer + col] for i in range(2)) for col in range(outer)]
            for place, (real_part, imag_part) in enumerate(sixteen(values, -1.0)):
                if place:
                    cosine = twiddle_ref[0, place : place + 1, :]
                    sine = twiddle_ref[1, place : place + 1, :]
                    real_part, imag_part = (
                        real_part * cosine + imag_part * sine,
                        imag_part * cosine - real_part * sine,
                    )
                spot = slice(place * slab + line * TR, place * slab + (line + 1) * TR)
                for at, value in enumerate((real_part, imag_part)):
                    high, low = bf16_pair(value)
                    high_ref[pair, spot, at * TC : (at + 1) * TC] = high
                    low_ref[pair, spot, at * TC : (at + 1) * TC] = low

        done = dot3((high_ref[pair], low_ref[pair]), table)
        for place in range(outer):
            here = slice(place * slab, (place + 1) * slab)
            out_ref[pair * half + place // 2, place % 2, 0] = done[here, :TC]
            out_ref[pair * half + place // 2, place % 2, 1] = done[here, TC:]


def turned(turn_ref, place, here, value, sign_value):
    if place == 0:
        return value
    real_part, imag_part = value
    shape = real_part.shape
    cosine = jnp.broadcast_to(turn_ref[0, here, place : place + 1], shape)
    sine = jnp.broadcast_to(turn_ref[1, here, place : place + 1], shape) * sign_value
    return (real_part * cosine - imag_part * sine, real_part * sine + imag_part * cosine)


def filters_kernel(length, at_ref, out_ref):
    _, _, outer, inner, lanes = out_ref.shape
    middle = length // 2
    wave_v = lax.broadcasted_iota(jnp.int32, (inner, lanes), 1) * outer + (2 * at_ref[4] + pl.program_id(0))
    keep_v = wave_v != middle
    sv = jnp.where(wave_v >= middle, wave_v - length, wave_v).astype(jnp.float32)
    line_u = lax.broadcasted_iota(jnp.int32, (inner, lanes), 0) * outer
    flip = jnp.where(at_ref[5] > 0, -1.0, 1.0)
    for place in range(outer):
        wave_u = line_u + place
        su = jnp.where(wave_u >= middle, wave_u - length, wave_u).astype(jnp.float32)
        scale = 1.0 / (float(length) * float(length))
        keep = jnp.where(keep_v & (wave_u != middle), scale * flip if place % 2 else scale, 0.0)
        factor = keep / jnp.maximum(sv * sv + su * su, 1.0)
        out_ref[0, 0, place] = factor * (sv * sv - su * su)
        out_ref[0, 1, place] = factor * (2.0 * sv * su)


def columns_kernel(
    order, filters_ref, in_ref, turn_ref, forward_ref, back_ref, out_ref,
    high_ref, low_ref, spectrum_ref, back_f, filter_ref, copied,
):
    fetch = pltpu.make_async_copy(filters_ref.at[pl.program_id(0)], filter_ref, copied)
    fetch.start()
    outer, _, _, inner, lanes = in_ref.shape
    forward = (forward_ref[0], forward_ref[1])
    back = (back_ref[0], back_ref[1])

    @pl.loop(0, inner // TR, unroll=True)
    def _(line):
        here = pl.ds(line * TR, TR)
        there = pl.ds(inner + line * TR, TR)
        values = [(in_ref[place, 0, 0, here, :], in_ref[place, 0, 1, here, :]) for place in order]
        for place, value in enumerate(sixteen(values, -1.0)):
            for spot, part in zip((here, there), turned(turn_ref, place, here, value, -1.0)):
                high, low = bf16_pair(part)
                high_ref[spot, place * lanes : (place + 1) * lanes] = high
                low_ref[spot, place * lanes : (place + 1) * lanes] = low

    for bunch in range(outer // 2):
        span = slice(bunch * 2 * lanes, (bunch + 1) * 2 * lanes)
        spectrum_ref[:, span] = dot3(forward, (high_ref[:, span], low_ref[:, span]))

    fetch.wait()
    for place in range(outer):
        side = slice(place * lanes, (place + 1) * lanes)
        first = filter_ref[0, place]
        second = filter_ref[1, place]
        real_part = spectrum_ref[:inner, side]
        imag_part = spectrum_ref[inner:, side]
        stacked = jnp.concatenate(
            [
                jnp.concatenate([real_part * first, real_part * second], axis=1),
                jnp.concatenate([imag_part * first, imag_part * second], axis=1),
            ],
            axis=0,
        )
        back_f[place] = dot3(back, bf16_pair(stacked))

    half = outer // 2

    @pl.loop(0, inner // TR, unroll=True)
    def _(line):
        here = pl.ds(line * TR, TR)
        there = pl.ds(inner + line * TR, TR)
        for field in range(2):
            side = slice(field * lanes, (field + 1) * lanes)
            values = [
                turned(turn_ref, place, here, (back_f[place, here, side], back_f[place, there, side]), 1.0)
                for place in range(outer)
            ]
            for low, (real_part, imag_part) in enumerate(sixteen(values, 1.0, half)):
                out_ref[low, 0, field, 0, here, :] = real_part
                out_ref[low, 0, field, 1, here, :] = imag_part


def inverse_rows_kernel(in_ref, twiddle_ref, table_ref, first_ref, second_ref, back_f):
    half, _, _, _, slab, lanes = in_ref.shape
    outer = 2 * half
    table = (table_ref[0], table_ref[1])
    for field, out_ref in enumerate((first_ref, second_ref)):
        joined = [
            jnp.concatenate([in_ref[place // 2, place % 2, field, part] for place in range(outer)], axis=0)
            for part in range(2)
        ]
        back_f[...] = dot3(bf16_pair(jnp.concatenate(joined, axis=1)), table)
        for line in range(slab // TR):
            here = slice(line * TR, (line + 1) * TR)
            values = []
            for place in range(outer):
                spot = slice(place * slab + line * TR, place * slab + (line + 1) * TR)
                real_part = back_f[spot, :lanes]
                imag_part = back_f[spot, lanes:]
                if place:
                    cosine = twiddle_ref[0, place : place + 1, :]
                    sine = twiddle_ref[1, place : place + 1, :]
                    real_part, imag_part = (
                        real_part * cosine - imag_part * sine,
                        real_part * sine + imag_part * cosine,
                    )
                values.append((real_part, imag_part))
            for place, (real_part, imag_part) in enumerate(sixteen(values, 1.0)):
                out_ref[0, here, place * lanes : (place + 1) * lanes] = real_part
                out_ref[1, here, place * lanes : (place + 1) * lanes] = imag_part


VMEM = pl.BlockSpec(memory_space=pltpu.VMEM)
SMEM = pl.BlockSpec(memory_space=pltpu.SMEM)


def room(mib):
    return pltpu.CompilerParams(vmem_limit_bytes=mib * 1024 * 1024)


def in_hbm(value):
    return pltpu.with_memory_space_constraint(value, pltpu.HBM)


def whole(shape):
    return pl.BlockSpec(shape, lambda step: (0,) * len(shape))


def slot_tiles(table, held, per_owner, cap):
    local_tiles = table.shape[-1]
    mine = table // per_owner == held
    earlier = jnp.arange(local_tiles)[:, None] < jnp.arange(local_tiles)[None, :]
    rank = jnp.sum(jnp.where(mine[..., :, None] & earlier, 1, 0), axis=-2)
    chosen = mine[..., None, :] & (rank[..., None, :] == jnp.arange(cap)[:, None])
    spot = table - held * per_owner
    return jnp.sum(jnp.where(chosen, spot[..., None, :], 0), axis=-1)


def cube_exchange(value):
    return lax.all_to_all(value, ("shell", "low"), split_axis=0, concat_axis=0, tiled=True)


def local_cube(block_tile, cell_index, masses, plane_coef, plane_dist, source_inv):
    half = lax.axis_size("low")
    groups = 2 * half
    shell = lax.axis_index("shell")
    upper = lax.axis_index("upper")
    low = lax.axis_index("low")
    planes, local_tiles, per_tile = cell_index.shape
    slab = L // groups
    outer = L // TC
    per_owner = slab // TR * outer
    cap = max(1, 2 * local_tiles // groups)
    chunks = per_tile // TC
    lines = 2 * chunks * cap
    part = (shell + low) % 2
    held = part * half + low
    order = [((s // half + s % 2) % 2) * half + s % half for s in range(groups)]

    raw, raw_first = pl.pallas_call(
        widen_kernel,
        in_specs=[VMEM, VMEM],
        out_specs=(VMEM, VMEM),
        out_shape=(
            jax.ShapeDtypeStruct((2, planes, local_tiles, per_tile), jnp.float32),
            jax.ShapeDtypeStruct((2, 1, local_tiles, per_tile), jnp.float32),
        ),
        compiler_params=room(8),
        name="widen",
    )(in_hbm(cell_index), in_hbm(masses))
    raw_far = lax.ppermute(raw_first, "upper", [(0, 1), (1, 0)])
    here = jnp.stack([upper * half + low, (1 - upper) * half + low, shell, 1 - shell, low, upper]).astype(jnp.int32)

    def pack(which, lists, spare):
        count = lists.shape[1]
        return pl.pallas_call(
            partial(pack_kernel, half, cap, per_owner, which),
            in_specs=[SMEM, SMEM, VMEM],
            out_specs=VMEM,
            out_shape=jax.ShapeDtypeStruct((groups, count * lines + spare, TC), jnp.float32),
            scratch_shapes=[pltpu.SMEM((groups,), jnp.int32)] * count,
            compiler_params=room(12),
            name="pack",
        )(here, block_tile, lists)

    near = cube_exchange(pack(0, raw, 8))
    far_second = lax.ppermute(near[:, lines:, :], "upper", [(0, 1), (1, 0)])
    far_first = cube_exchange(pack(1, raw_far, 0))

    note = jnp.concatenate(
        [block_tile.astype(jnp.float32), plane_coef[:, None], (plane_coef * plane_dist)[:, None], source_inv[:, None]],
        axis=1,
    )
    other = lax.ppermute(note, "shell", [(0, 1), (1, 0)])
    both = jnp.where(shell == 0, jnp.concatenate([note, other]), jnp.concatenate([other, note]))
    tiles = slot_tiles(
        both[:, : groups * local_tiles].astype(jnp.int32).reshape(2 * planes, groups, local_tiles), held, per_owner, cap
    )
    tiles = tiles.reshape(2 * planes, 2, half, cap)
    near_slots = lax.dynamic_index_in_dim(tiles, upper, axis=1, keepdims=False).reshape(-1)
    far_slots = lax.dynamic_index_in_dim(tiles, 1 - upper, axis=1, keepdims=False).reshape(-1)
    maps = jnp.arange(2 * planes)
    weight = jnp.where(
        maps[None, :] <= maps[:, None], both[None, :, -3] - both[:, -1][:, None] * both[None, :, -2], 0.0
    )
    weight = jnp.concatenate([weight, jnp.sum(weight, axis=1, keepdims=True)], axis=1)

    filters = pl.pallas_call(
        partial(filters_kernel, L),
        grid=(2,),
        in_specs=[SMEM],
        out_specs=pl.BlockSpec((1, 2, outer, slab, TC), lambda step: (step, 0, 0, 0, 0)),
        out_shape=pltpu.HBM((2, 2, outer, slab, TC), jnp.float32),
        compiler_params=room(16),
        name="filters",
    )(here)
    some_dens = pl.pallas_call(
        partial(deposit_kernel, cap, chunks),
        in_specs=[SMEM, VMEM, SMEM, VMEM],
        out_specs=VMEM,
        out_shape=pltpu.HBM((2 * planes, per_owner, TR, TC), jnp.float32),
        compiler_params=room(16),
        name="deposit",
    )(near_slots, near, far_slots, far_first)
    twiddle = jnp.asarray(twiddle_pair(outer, TC))
    turn = jnp.asarray(twiddle_pair(outer, TC).transpose(0, 2, 1))
    minus = jnp.asarray(dft_block(TC, -1.0))
    plus = jnp.asarray(dft_block(TC, 1.0))
    field = jax.ShapeDtypeStruct((planes, slab, L), jnp.float32)
    some = 2 * TR
    conv_mine, conv_other, row_sent = pl.pallas_call(
        partial(rows_kernel, cap, chunks),
        grid=(slab // some,),
        in_specs=[
            SMEM,
            SMEM,
            SMEM,
            pl.BlockSpec(memory_space=pltpu.HBM),
            pl.BlockSpec((groups, 8, TC), lambda step: (0, planes * lines // 8, 0)),
            whole(far_second.shape),
            whole(twiddle.shape),
            whole(minus.shape),
        ],
        out_specs=(
            pl.BlockSpec((planes, some, L), lambda step: (0, step, 0)),
            pl.BlockSpec((planes, some, L), lambda step: (0, step, 0)),
            pl.BlockSpec((groups, 2, 2, some, TC), lambda step: (0, 0, 0, step, 0)),
        ),
        out_shape=(
            pltpu.HBM(field.shape, field.dtype),
            pltpu.HBM(field.shape, field.dtype),
            pltpu.HBM((groups, 2, 2, slab, TC), jnp.float32),
        ),
        scratch_shapes=[
            pltpu.VMEM((2, outer * some, 2 * TC), jnp.bfloat16),
            pltpu.VMEM((2, outer * some, 2 * TC), jnp.bfloat16),
            pltpu.VMEM((planes, per_owner, TR, TC), jnp.float32),
            pltpu.VMEM((2 * planes, per_owner, TR, TC), jnp.float32),
            pltpu.VMEM((2 * planes, some // TR * outer, TR, TC), jnp.float32),
            pltpu.SemaphoreType.DMA(()),
        ],
        compiler_params=room(28),
        name="rows",
    )(weight, here, far_slots, in_hbm(some_dens), near, far_second, twiddle, minus)
    arrived = lax.all_to_all(row_sent, ("shell", "low"), split_axis=0, concat_axis=0, tiled=True)
    swaps = []
    for side in range(2):
        for top in range(2):
            for at in range(half):
                if (side + at) % 2 == top:
                    swaps.append(((side * 2 + top) * half + at, ((1 - side) * 2 + top) * half + at))
    conv_held = lax.ppermute(conv_other, ("shell", "upper", "low"), swaps)
    convergence = jnp.where(part == upper, conv_mine, conv_held)
    col_sent = pl.pallas_call(
        partial(columns_kernel, order),
        grid=(2,),
        in_specs=[
            pl.BlockSpec(memory_space=pltpu.HBM),
            pl.BlockSpec((groups, 1, 2, slab, TC), lambda step: (0, step, 0, 0, 0)),
            whole(turn.shape),
            whole(plus.shape),
            whole(minus.shape),
        ],
        out_specs=pl.BlockSpec((half, 1, 2, 2, slab, TC), lambda step: (0, step, 0, 0, 0, 0)),
        out_shape=pltpu.HBM((half, 2, 2, 2, slab, TC), jnp.float32),
        scratch_shapes=[
            pltpu.VMEM((2 * slab, L), jnp.bfloat16),
            pltpu.VMEM((2 * slab, L), jnp.bfloat16),
            pltpu.VMEM((2 * slab, L), jnp.float32),
            pltpu.VMEM((outer, 2 * slab, 2 * TC), jnp.float32),
            pltpu.VMEM((2, outer, slab, TC), jnp.float32),
            pltpu.SemaphoreType.DMA(()),
        ],
        compiler_params=room(32),
        name="columns",
    )(in_hbm(filters), arrived, turn, plus, minus)
    landed = lax.all_to_all(col_sent, "low", split_axis=0, concat_axis=0, tiled=True)
    shear_one, shear_two = pl.pallas_call(
        inverse_rows_kernel,
        grid=(slab // some,),
        in_specs=[
            pl.BlockSpec((half, 2, 2, 2, some, TC), lambda step: (0, 0, 0, 0, step, 0)),
            whole(twiddle.shape),
            whole(plus.shape),
        ],
        out_specs=(
            pl.BlockSpec((planes, some, L), lambda step: (0, step, 0)),
            pl.BlockSpec((planes, some, L), lambda step: (0, step, 0)),
        ),
        out_shape=(field, field),
        scratch_shapes=[pltpu.VMEM((outer * some, 2 * TC), jnp.float32)],
        compiler_params=room(24),
        name="inverse_rows",
    )(landed, twiddle, plus)
    return (convergence, shear_one, shear_two)


def solution(mesh):
    shells, groups = (mesh.shape["shell"], mesh.shape["pix"])
    body, pix = (local, "pix")
    if shells == 2 and groups * TC == L:
        body, pix = (local_cube, ("upper", "low"))
        mesh = type(mesh)(mesh.devices.reshape(shells, 2, groups // 2), ("shell", "upper", "low"))
    placed = (P("shell", None), P("shell", pix, None), P("shell", pix, None), P("shell"), P("shell"), P("shell"))
    out = P("shell", pix, None)

    def step(*arrays):
        return body(*arrays)

    return jax.shard_map(step, mesh=mesh, in_specs=placed, out_specs=(out, out, out), check_vma=False)
```

```python
from functools import partial
import math

import jax
import jax.numpy as jnp
import numpy as np
from jax import lax
from jax.experimental import pallas as pl
from jax.experimental.pallas import tpu as pltpu
from jax.sharding import PartitionSpec as P

L = 2048
TR = 16
TC = 128


HIGHEST = lax.Precision.HIGHEST


def entering(value, axis, join, neutral):
    count, mine = (lax.axis_size(axis), lax.axis_index(axis))
    pieces = jax.tree.map(lambda part: lax.all_gather(part, axis), value)
    running = jax.tree.map(
        lambda part, zero: jnp.full_like(part, 0) + jnp.asarray(zero, part.dtype), value, neutral
    )

    def lap(position, running):
        longer = join(running, jax.tree.map(lambda part: part[position], pieces))
        return jax.tree.map(lambda new, old: jnp.where(position < mine, new, old), longer, running)

    return lax.fori_loop(0, count - 1, lap, running)


def dft_table(left_size, right_size, period, sign_value):
    left_idx = jnp.arange(left_size)[:, None]
    right_idx = jnp.arange(right_size)[None, :]
    angle = 2.0 * math.pi / period * (left_idx * right_idx % period).astype(jnp.float32)
    return (jnp.cos(angle), sign_value * jnp.sin(angle))


def mix_outer(table, real_part, imag_part):
    cosine, sine_part = table
    contract = partial(jnp.einsum, "ab,...bc->...ac", precision=HIGHEST)
    return (
        contract(cosine, real_part) - contract(sine_part, imag_part),
        contract(sine_part, real_part) + contract(cosine, imag_part),
    )


def mix_inner(table, real_part, imag_part):
    cosine, sine_part = table
    product = partial(jnp.matmul, precision=HIGHEST)
    return (
        product(real_part, cosine) - product(imag_part, sine_part),
        product(real_part, sine_part) + product(imag_part, cosine),
    )


def twist(table, real_part, imag_part):
    cosine, sine_part = table
    return (real_part * cosine - imag_part * sine_part, real_part * sine_part + imag_part * cosine)


def transform_last(real_part, imag_part, sign_value):
    length = real_part.shape[-1]
    inner = math.gcd(length, 128)
    outer = length // inner
    leading = real_part.shape[:-1]
    real_part = real_part.reshape(leading + (outer, inner))
    imag_part = imag_part.reshape(leading + (outer, inner))
    outer_table = dft_table(outer, outer, outer, sign_value)
    inner_table = dft_table(inner, inner, inner, sign_value)
    twiddle = dft_table(outer, inner, length, sign_value)
    if sign_value < 0:
        real_part, imag_part = mix_outer(outer_table, real_part, imag_part)
        real_part, imag_part = twist(twiddle, real_part, imag_part)
        real_part, imag_part = mix_inner(inner_table, real_part, imag_part)
    else:
        real_part, imag_part = mix_inner(inner_table, real_part, imag_part)
        real_part, imag_part = twist(twiddle, real_part, imag_part)
        real_part, imag_part = mix_outer(outer_table, real_part, imag_part)
    return (real_part.reshape(leading + (length,)), imag_part.reshape(leading + (length,)))


def frequency_of(position, length):
    inner = math.gcd(length, 128)
    outer = length // inner
    frequency = position // inner + outer * (position % inner)
    signed = jnp.where(frequency >= length // 2, frequency - length, frequency).astype(jnp.float32)
    keep_mask = (frequency != length // 2).astype(jnp.float32)
    return (signed, keep_mask)


def add_pairs(earlier_pair, later_pair):
    return (earlier_pair[0] + later_pair[0], earlier_pair[1] + later_pair[1])


def deposit_group(item):
    cell_ids, weights = item
    tile_rows = cell_ids // TC
    tile_cols = cell_ids % TC
    row_hot = jnp.where(
        tile_rows[:, None, :] == jnp.arange(TR)[None, :, None],
        weights[:, None, :],
        jnp.zeros((), jnp.bfloat16),
    )
    col_hot = (tile_cols[:, :, None] == jnp.arange(TC)[None, None, :]).astype(jnp.bfloat16)
    return jnp.einsum("grk,gkc->grc", row_hot, col_hot, preferred_element_type=jnp.float32)


def rows_to_sending(packed, groups, slab, cols_own):
    count, fields = (packed.shape[0], packed.shape[1])
    return (
        packed.reshape(count, fields, slab, groups, cols_own)
        .transpose(3, 0, 1, 4, 2)
        .reshape(groups, count, fields, cols_own * slab)
    )


def arrived_to_columns(arrived, groups, slab, cols_own):
    count, fields = (arrived.shape[1], arrived.shape[2])
    return (
        arrived.reshape(groups, count, fields, cols_own, slab)
        .transpose(1, 2, 3, 0, 4)
        .reshape(count, fields, cols_own, groups * slab)
    )


def columns_to_sending(stacked, groups, slab, cols_own):
    count, fields = (stacked.shape[0], stacked.shape[1])
    return (
        stacked.reshape(count, fields, cols_own, groups, slab)
        .transpose(3, 0, 1, 2, 4)
        .reshape(groups, count, fields, cols_own * slab)
    )


def landed_to_rows(landed, groups, slab, cols_own):
    count, fields = (landed.shape[1], landed.shape[2])
    return (
        landed.reshape(groups, count, fields, cols_own, slab)
        .transpose(1, 2, 4, 0, 3)
        .reshape(count, fields, slab, groups * cols_own)
    )


def local(block_tile, cell_index, masses, plane_coef, plane_dist, source_inv):
    groups = lax.axis_size("pix")
    my_index = lax.axis_index("pix")
    planes, local_tiles, per_tile = cell_index.shape
    slab = L // groups
    per_owner = slab // TR * (L // TC)
    cap = max(1, 2 * local_tiles // groups)
    flat = TR * TC
    batch_tiles = 8
    deposited = lax.map(
        deposit_group,
        (cell_index.reshape(-1, batch_tiles, per_tile), masses.reshape(-1, batch_tiles, per_tile)),
    )
    tile_sums = deposited.reshape(planes, local_tiles, flat)
    table = block_tile.reshape(planes, groups, local_tiles)
    owner = table // per_owner
    earlier = jnp.arange(local_tiles)[:, None] < jnp.arange(local_tiles)[None, :]
    same_owner = owner[:, :, :, None] == owner[:, :, None, :]
    rank = jnp.sum(jnp.where(same_owner & earlier[None, None], 1, 0), axis=2)
    slot = owner * cap + rank
    my_slots = lax.dynamic_index_in_dim(slot, my_index, axis=1, keepdims=False)
    slot_grid = jnp.arange(groups)[:, None] * cap + jnp.arange(cap)[None, :]
    send_hot = (my_slots[:, None, None, :] == slot_grid[None, :, :, None]).astype(jnp.float32)
    outgoing = jnp.einsum("pnct,ptf->npcf", send_hot, tile_sums, precision=HIGHEST)
    incoming = lax.all_to_all(outgoing, "pix", split_axis=0, concat_axis=0, tiled=True)
    local_index = table - my_index * per_owner
    is_mine = owner == my_index
    tile_hot = (is_mine[..., None] & (local_index[..., None] == jnp.arange(per_owner))).astype(
        jnp.float32
    )
    slot_hot = (rank[..., None] == jnp.arange(cap)).astype(jnp.float32)
    placing = jnp.einsum("pstl,pstc->plsc", tile_hot, slot_hot, precision=HIGHEST)
    slab_tiles = jnp.einsum("plsc,spcf->plf", placing, incoming, precision=HIGHEST)
    density = (
        slab_tiles.reshape(planes, slab // TR, L // TC, TR, TC)
        .transpose(0, 1, 3, 2, 4)
        .reshape(planes, slab, L)
    )
    total = lax.psum(jnp.sum(density, axis=(1, 2)), "pix")
    contrast = density / (total / (L * L))[:, None, None] - 1.0
    near_local = jnp.cumsum(plane_coef[:, None, None] * contrast, axis=0)
    far_local = jnp.cumsum((plane_coef * plane_dist)[:, None, None] * contrast, axis=0)
    blank = jnp.zeros((slab, L), jnp.float32)
    near_before, far_before = entering(
        (near_local[-1], far_local[-1]), "shell", add_pairs, (blank, blank)
    )
    convergence = near_before + near_local - source_inv[:, None, None] * (far_before + far_local)
    cols_own = L // groups
    wave_x, keep_x = frequency_of(my_index * cols_own + jnp.arange(cols_own), L)
    wave_y, keep_y = frequency_of(jnp.arange(L), L)
    wave_x = wave_x[:, None]
    wave_y = wave_y[None, :]
    both_keep = keep_x[:, None] * keep_y[None, :]
    wave_power = jnp.maximum(wave_x * wave_x + wave_y * wave_y, 1.0)
    kernel_one = both_keep * (wave_x * wave_x - wave_y * wave_y) / wave_power
    kernel_two = both_keep * 2.0 * wave_x * wave_y / wave_power
    scale = 1.0 / (L * L)
    spec_real, spec_imag = transform_last(convergence[0::2], convergence[1::2], -1.0)
    sending = rows_to_sending(jnp.stack([spec_real, spec_imag], axis=1), groups, slab, cols_own)
    arrived = lax.all_to_all(sending, "pix", split_axis=0, concat_axis=0, tiled=True)
    columns = arrived_to_columns(arrived, groups, slab, cols_own)
    row_real, row_imag = transform_last(columns[:, 0], columns[:, 1], -1.0)
    first_real, first_imag = transform_last(row_real * kernel_one, row_imag * kernel_one, 1.0)
    second_real, second_imag = transform_last(row_real * kernel_two, row_imag * kernel_two, 1.0)
    stacked = jnp.stack([first_real, first_imag, second_real, second_imag], axis=1)
    landed = lax.all_to_all(
        columns_to_sending(stacked, groups, slab, cols_own),
        "pix",
        split_axis=0,
        concat_axis=0,
        tiled=True,
    )
    row_layout = landed_to_rows(landed, groups, slab, cols_own)
    even_one, odd_one = transform_last(row_layout[:, 0], row_layout[:, 1], 1.0)
    even_two, odd_two = transform_last(row_layout[:, 2], row_layout[:, 3], 1.0)
    shear_one = jnp.stack([even_one, odd_one], axis=1).reshape(planes, slab, L)
    shear_two = jnp.stack([even_two, odd_two], axis=1).reshape(planes, slab, L)
    return (convergence, shear_one * scale, shear_two * scale)


def bf16_pair(value):
    high = value.astype(jnp.bfloat16)
    return (high, (value - high.astype(jnp.float32)).astype(jnp.bfloat16))


def dft_block(size, sign_value):
    turn = 2.0 * np.pi / size * (np.outer(np.arange(size), np.arange(size)) % size)
    cosine, sine = (np.cos(turn), sign_value * np.sin(turn))
    whole = np.block([[cosine, sine], [-sine, cosine]]).astype(np.float32)
    high = whole.astype(jnp.bfloat16)
    low = (whole - high.astype(np.float32)).astype(jnp.bfloat16)
    return np.stack([high, low])


def twiddle_pair(outer, inner):
    turn = 2.0 * np.pi / (outer * inner) * np.outer(np.arange(outer), np.arange(inner))
    return np.stack([np.cos(turn), np.sin(turn)]).astype(np.float32)


def quarter(values, sign_value):
    (ar, ai), (br, bi), (cr, ci), (dr, di) = values
    pr, pi, mr, mi = (ar + cr, ai + ci, ar - cr, ai - ci)
    qr, qi, nr, ni = (br + dr, bi + di, br - dr, bi - di)
    if sign_value < 0:
        return [(pr + qr, pi + qi), (mr + ni, mi - nr), (pr - qr, pi - qi), (mr - ni, mi + nr)]
    return [(pr + qr, pi + qi), (mr - ni, mi + nr), (pr - qr, pi - qi), (mr + ni, mi - nr)]


def rotate(value, step, sign_value):
    real_part, imag_part = value
    if step == 0:
        return value
    if step == 4:
        return (-sign_value * imag_part, sign_value * real_part)
    cosine = math.cos(2.0 * math.pi * step / 16)
    sine = sign_value * math.sin(2.0 * math.pi * step / 16)
    return (real_part * cosine - imag_part * sine, real_part * sine + imag_part * cosine)


def sixteen(values, sign_value, count=16):
    inner = [quarter([values[4 * a + b] for a in range(4)], sign_value) for b in range(4)]
    result = [None] * 16
    for k in range(4):
        turned_values = [rotate(inner[b][k], b * k, sign_value) for b in range(4)]
        for place, value in enumerate(quarter(turned_values, sign_value)):
            result[k + 4 * place] = value
    return result[:count]


def dot3(left, right):
    mul = partial(jnp.dot, preferred_element_type=jnp.float32)
    (left_high, left_low), (right_high, right_low) = (left, right)
    return mul(left_high, right_high) + (mul(left_low, right_high) + mul(left_high, right_low))


def widen_kernel(cell_ref, mass_ref, all_ref, first_ref):
    cells = cell_ref[...].astype(jnp.float32)
    weights = mass_ref[...].astype(jnp.float32)
    all_ref[0] = cells
    all_ref[1] = weights
    first_ref[0] = cells[:1]
    first_ref[1] = weights[:1]


def divided(value, count):
    return value >> (count.bit_length() - 1) if count & (count - 1) == 0 else lax.div(value, count)


def pack_kernel(half, cap, per_owner, which, at_ref, table_ref, raw_ref, out_ref, *count_refs):
    _, planes, local_tiles, per_tile = raw_ref.shape
    groups = out_ref.shape[0]
    chunks = per_tile // TC
    lines = 2 * chunks * cap
    out_ref[...] = jnp.zeros(out_ref.shape, jnp.float32)
    base = at_ref[which] * local_tiles
    for place in range(groups):
        for count_ref in count_refs:
            count_ref[place] = 0

    @pl.loop(0, local_tiles // 8)
    def _(bunch):
        here = pl.ds(pl.multiple_of(bunch * 8, 8), 8)
        lists = [[raw_ref[kind, plane, here, :] for kind in range(2)] for plane in range(planes)]
        for at in range(8):
            for plane, count_ref in enumerate(count_refs):
                owner = divided(table_ref[plane, base + bunch * 8 + at], per_owner)
                upper = divided(owner, half)
                low = owner - upper * half
                place = ((upper + low) & 1) * half + low
                rank = count_ref[place]
                count_ref[place] = rank + 1
                for kind, values in enumerate(lists[plane]):
                    for chunk in range(chunks):
                        row = plane * lines + kind * chunks * cap + chunk * cap + rank
                        out_ref[place, pl.ds(row, 1), :] = values[at : at + 1, chunk * TC : (chunk + 1) * TC]

    if out_ref.shape[1] == planes * lines:
        return
    for plane in range(planes):
        total = jnp.sum(raw_ref[1, plane], axis=0, keepdims=True)
        total = jnp.sum(total, axis=1, keepdims=True)
        line = jnp.broadcast_to(total, (1, TC))
        for place in range(groups):
            out_ref[place, planes * lines + plane : planes * lines + plane + 1, :] = line


def deposit_into(cap, chunks, out_ref, out_planes, slots_ref, slot_planes, recv_ref, starts):
    half = recv_ref.shape[0] // 2
    width = 32
    bunch = 4
    parts = TC // width
    low = lax.broadcasted_iota(jnp.int32, (TR, TC), 0).astype(jnp.float32)
    lines = [(low + float(TR * part)).astype(jnp.bfloat16) for part in range(parts)]
    one = jnp.ones((TR, TC), jnp.bfloat16)
    none = jnp.zeros((TR, TC), jnp.bfloat16)

    def spread(value, slot):
        return jnp.broadcast_to(value[slot : slot + 1, :], (TR, TC)).astype(jnp.bfloat16)

    for out_plane, slot_plane, (sender, start) in zip(out_planes, slot_planes, starts):

        @pl.loop(0, half, unroll=True)
        def _(source):
            place = sender * half + source
            cells = [recv_ref[place, start + k * cap : start + (k + 1) * cap, :] for k in range(chunks)]
            weights = [
                recv_ref[place, start + (chunks + k) * cap : start + (chunks + k + 1) * cap, :] for k in range(chunks)
            ]
            rows = [jnp.floor(cell * (1.0 / TC)) for cell in cells]
            strips = [jnp.floor(cell * (1.0 / width)) for cell in cells]
            cols = [cell - strip * float(width) for cell, strip in zip(cells, strips)]
            rows = [row + (strip - row * float(parts)) * float(TR) for row, strip in zip(rows, strips)]
            sums = []
            for first in range(0, cap, bunch):
                row_hot = []
                col_hot = []
                for k in range(chunks):
                    row_lines = []
                    col_lines = []
                    for slot in range(first, first + bunch):
                        row = spread(rows[k], slot)
                        weight = spread(weights[k], slot)
                        row_lines += [jnp.where(lines[at] == row, weight, none) for at in range(parts)]
                        col = spread(cols[k], slot)
                        col_lines += [jnp.where(lines[at] == col, one, none) for at in range(width // TR)]
                    row_hot.append(jnp.concatenate(row_lines, axis=0))
                    col_hot.append(jnp.concatenate(col_lines, axis=0))
                done = lax.dot_general(
                    jnp.concatenate(row_hot, axis=1),
                    jnp.concatenate(col_hot, axis=1),
                    (((1,), (1,)), ((), ())),
                    preferred_element_type=jnp.float32,
                )
                for at in range(bunch):
                    base = at * TR * parts
                    side = slice(at * width, (at + 1) * width)
                    strips_of = [done[base + j * TR : base + (j + 1) * TR, side] for j in range(parts)]
                    sums.append(jnp.concatenate(strips_of, axis=1))
            for slot in range(cap):
                tile = slots_ref[(slot_plane * half + source) * cap + slot]
                out_ref[out_plane, tile] = out_ref[out_plane, tile] + sums[slot]


def deposit_kernel(cap, chunks, slots_ref, near_ref, out_ref):
    out_ref[...] = jnp.zeros(out_ref.shape, jnp.float32)
    lines = 2 * chunks * cap
    every = range(4)
    starts = [(plane // 2, (plane % 2) * lines) for plane in every]
    deposit_into(cap, chunks, out_ref, every, slots_ref, every, near_ref, starts)


def deposit_first_kernel(cap, chunks, slots_ref, first_ref, out_ref):
    out_ref[...] = jnp.zeros(out_ref.shape, jnp.float32)
    deposit_into(cap, chunks, out_ref, (0, 1), slots_ref, (0, 2), first_ref, ((0, 0), (1, 0)))


def rows_kernel(
    cap, chunks, weight_ref, at_ref, slots_ref, near_dens_ref, first_dens_ref, near_ref, far_ref, twiddle_ref, table_ref,
    mine_ref, other_ref, out_ref, high_ref, low_ref, far_dens_ref, dens_ref, first_ref, maps_ref, copied, copied_first,
):
    step = pl.program_id(0)

    @pl.when(step == 0)
    def _():
        fetch = pltpu.make_async_copy(near_dens_ref, dens_ref, copied)
        fetch.start()
        fetch_first = pltpu.make_async_copy(first_dens_ref, first_ref, copied_first)
        fetch_first.start()
        far_dens_ref[...] = jnp.zeros(far_dens_ref.shape, jnp.float32)
        deposit_into(cap, chunks, far_dens_ref, (0, 1), slots_ref, (1, 3), far_ref, ((0, 0), (1, 0)))
        fetch.wait()
        fetch_first.wait()

    planes, slab, length = mine_ref.shape
    all_planes = dens_ref.shape[0]
    first_line = 2 * cap * chunks
    outer = length // TC
    first_tile = step * (slab // TR * outer)
    half = near_ref.shape[0] // 2
    scales = []
    for plane in range(all_planes):
        line = plane % planes
        total = jnp.zeros((1, TC), jnp.float32)
        for source in range(half):
            place = (plane // planes) * half + source
            total = total + near_ref[place, line : line + 1, :]
            total = total + far_ref[place, first_line + line : first_line + line + 1, :]
        scales.append(float(length * length) / total)
    factors = [
        [jnp.broadcast_to(weight_ref[i, j] * scales[j], (TR, TC)) for j in range(i + 1)] for i in range(all_planes)
    ]
    shift = [weight_ref[i, all_planes] for i in range(all_planes)]
    first_shell = at_ref[2] == 0
    for line in range(slab // TR):
        here = slice(line * TR, (line + 1) * TR)
        for col in range(outer):
            at = line * outer + col
            rest = (first_ref, far_dens_ref)
            tiles = [dens_ref[j, first_tile + at] + rest[j % 2][j // 2, first_tile + at] for j in range(all_planes)]
            maps = []
            for i in range(all_planes):
                field = tiles[0] * factors[i][0]
                for j in range(1, i + 1):
                    field = field + tiles[j] * factors[i][j]
                maps.append(field - shift[i])
                maps_ref[i, at] = maps[i]
            side = slice(col * TC, (col + 1) * TC)
            for i in range(planes):
                mine_ref[i, here, side] = jnp.where(first_shell, maps[i], maps[planes + i])
                other_ref[i, here, side] = jnp.where(first_shell, maps[planes + i], maps[i])

    table = (table_ref[0], table_ref[1])
    for pair in range(all_planes // 2):
        for line in range(slab // TR):
            values = [tuple(maps_ref[2 * pair + i, line * outer + col] for i in range(2)) for col in range(outer)]
            for place, (real_part, imag_part) in enumerate(sixteen(values, -1.0)):
                if place:
                    cosine = twiddle_ref[0, place : place + 1, :]
                    sine = twiddle_ref[1, place : place + 1, :]
                    real_part, imag_part = (
                        real_part * cosine + imag_part * sine,
                        imag_part * cosine - real_part * sine,
                    )
                spot = slice(place * slab + line * TR, place * slab + (line + 1) * TR)
                for at, value in enumerate((real_part, imag_part)):
                    high, low = bf16_pair(value)
                    high_ref[pair, spot, at * TC : (at + 1) * TC] = high
                    low_ref[pair, spot, at * TC : (at + 1) * TC] = low

        done = dot3((high_ref[pair], low_ref[pair]), table)
        for place in range(outer):
            here = slice(place * slab, (place + 1) * slab)
            out_ref[pair * half + place // 2, place % 2, 0] = done[here, :TC]
            out_ref[pair * half + place // 2, place % 2, 1] = done[here, TC:]


def turned(turn_ref, place, here, value, sign_value):
    if place == 0:
        return value
    real_part, imag_part = value
    shape = real_part.shape
    cosine = jnp.broadcast_to(turn_ref[0, here, place : place + 1], shape)
    sine = jnp.broadcast_to(turn_ref[1, here, place : place + 1], shape) * sign_value
    return (real_part * cosine - imag_part * sine, real_part * sine + imag_part * cosine)


def filters_kernel(length, at_ref, out_ref):
    _, _, outer, inner, lanes = out_ref.shape
    middle = length // 2
    wave_v = lax.broadcasted_iota(jnp.int32, (inner, lanes), 1) * outer + (2 * at_ref[4] + pl.program_id(0))
    keep_v = wave_v != middle
    sv = jnp.where(wave_v >= middle, wave_v - length, wave_v).astype(jnp.float32)
    line_u = lax.broadcasted_iota(jnp.int32, (inner, lanes), 0) * outer
    flip = jnp.where(at_ref[5] > 0, -1.0, 1.0)
    for place in range(outer):
        wave_u = line_u + place
        su = jnp.where(wave_u >= middle, wave_u - length, wave_u).astype(jnp.float32)
        scale = 1.0 / (float(length) * float(length))
        keep = jnp.where(keep_v & (wave_u != middle), scale * flip if place % 2 else scale, 0.0)
        factor = keep / jnp.maximum(sv * sv + su * su, 1.0)
        out_ref[0, 0, place] = factor * (sv * sv - su * su)
        out_ref[0, 1, place] = factor * (2.0 * sv * su)


def columns_kernel(
    order, filters_ref, in_ref, turn_ref, forward_ref, back_ref, out_ref,
    high_ref, low_ref, spectrum_ref, back_f, filter_ref, copied,
):
    fetch = pltpu.make_async_copy(filters_ref.at[pl.program_id(0)], filter_ref, copied)
    fetch.start()
    outer, _, _, inner, lanes = in_ref.shape
    forward = (forward_ref[0], forward_ref[1])
    back = (back_ref[0], back_ref[1])

    @pl.loop(0, inner // TR, unroll=True)
    def _(line):
        here = pl.ds(line * TR, TR)
        there = pl.ds(inner + line * TR, TR)
        values = [(in_ref[place, 0, 0, here, :], in_ref[place, 0, 1, here, :]) for place in order]
        for place, value in enumerate(sixteen(values, -1.0)):
            for spot, part in zip((here, there), turned(turn_ref, place, here, value, -1.0)):
                high, low = bf16_pair(part)
                high_ref[spot, place * lanes : (place + 1) * lanes] = high
                low_ref[spot, place * lanes : (place + 1) * lanes] = low

    for bunch in range(outer // 2):
        span = slice(bunch * 2 * lanes, (bunch + 1) * 2 * lanes)
        spectrum_ref[:, span] = dot3(forward, (high_ref[:, span], low_ref[:, span]))

    fetch.wait()
    for place in range(outer):
        side = slice(place * lanes, (place + 1) * lanes)
        first = filter_ref[0, place]
        second = filter_ref[1, place]
        real_part = spectrum_ref[:inner, side]
        imag_part = spectrum_ref[inner:, side]
        stacked = jnp.concatenate(
            [
                jnp.concatenate([real_part * first, real_part * second], axis=1),
                jnp.concatenate([imag_part * first, imag_part * second], axis=1),
            ],
            axis=0,
        )
        back_f[place] = dot3(back, bf16_pair(stacked))

    half = outer // 2

    @pl.loop(0, inner // TR, unroll=True)
    def _(line):
        here = pl.ds(line * TR, TR)
        there = pl.ds(inner + line * TR, TR)
        for field in range(2):
            side = slice(field * lanes, (field + 1) * lanes)
            values = [
                turned(turn_ref, place, here, (back_f[place, here, side], back_f[place, there, side]), 1.0)
                for place in range(outer)
            ]
            for low, (real_part, imag_part) in enumerate(sixteen(values, 1.0, half)):
                out_ref[low, 0, field, 0, here, :] = real_part
                out_ref[low, 0, field, 1, here, :] = imag_part


def inverse_rows_kernel(in_ref, twiddle_ref, table_ref, first_ref, second_ref, back_f):
    half, _, _, _, slab, lanes = in_ref.shape
    outer = 2 * half
    table = (table_ref[0], table_ref[1])
    for field, out_ref in enumerate((first_ref, second_ref)):
        joined = [
            jnp.concatenate([in_ref[place // 2, place % 2, field, part] for place in range(outer)], axis=0)
            for part in range(2)
        ]
        back_f[...] = dot3(bf16_pair(jnp.concatenate(joined, axis=1)), table)
        for line in range(slab // TR):
            here = slice(line * TR, (line + 1) * TR)
            values = []
            for place in range(outer):
                spot = slice(place * slab + line * TR, place * slab + (line + 1) * TR)
                real_part = back_f[spot, :lanes]
                imag_part = back_f[spot, lanes:]
                if place:
                    cosine = twiddle_ref[0, place : place + 1, :]
                    sine = twiddle_ref[1, place : place + 1, :]
                    real_part, imag_part = (
                        real_part * cosine - imag_part * sine,
                        real_part * sine + imag_part * cosine,
                    )
                values.append((real_part, imag_part))
            for place, (real_part, imag_part) in enumerate(sixteen(values, 1.0)):
                out_ref[0, here, place * lanes : (place + 1) * lanes] = real_part
                out_ref[1, here, place * lanes : (place + 1) * lanes] = imag_part


VMEM = pl.BlockSpec(memory_space=pltpu.VMEM)
SMEM = pl.BlockSpec(memory_space=pltpu.SMEM)


def room(mib):
    return pltpu.CompilerParams(vmem_limit_bytes=mib * 1024 * 1024)


def in_hbm(value):
    return pltpu.with_memory_space_constraint(value, pltpu.HBM)


def whole(shape):
    return pl.BlockSpec(shape, lambda step: (0,) * len(shape))


def slot_tiles(table, held, per_owner, cap):
    local_tiles = table.shape[-1]
    mine = table // per_owner == held
    earlier = jnp.arange(local_tiles)[:, None] < jnp.arange(local_tiles)[None, :]
    rank = jnp.sum(jnp.where(mine[..., :, None] & earlier, 1, 0), axis=-2)
    chosen = mine[..., None, :] & (rank[..., None, :] == jnp.arange(cap)[:, None])
    spot = table - held * per_owner
    return jnp.sum(jnp.where(chosen, spot[..., None, :], 0), axis=-1)


def cube_exchange(value):
    return lax.all_to_all(value, ("shell", "low"), split_axis=0, concat_axis=0, tiled=True)


def local_cube(block_tile, cell_index, masses, plane_coef, plane_dist, source_inv):
    half = lax.axis_size("low")
    groups = 2 * half
    shell = lax.axis_index("shell")
    upper = lax.axis_index("upper")
    low = lax.axis_index("low")
    planes, local_tiles, per_tile = cell_index.shape
    slab = L // groups
    outer = L // TC
    per_owner = slab // TR * outer
    cap = max(1, 2 * local_tiles // groups)
    chunks = per_tile // TC
    lines = 2 * chunks * cap
    part = (shell + low) % 2
    held = part * half + low
    order = [((s // half + s % 2) % 2) * half + s % half for s in range(groups)]

    raw, raw_first = pl.pallas_call(
        widen_kernel,
        in_specs=[VMEM, VMEM],
        out_specs=(VMEM, VMEM),
        out_shape=(
            jax.ShapeDtypeStruct((2, planes, local_tiles, per_tile), jnp.float32),
            jax.ShapeDtypeStruct((2, 1, local_tiles, per_tile), jnp.float32),
        ),
        compiler_params=room(8),
        name="widen",
    )(in_hbm(cell_index), in_hbm(masses))
    raw_far = lax.ppermute(raw_first, "upper", [(0, 1), (1, 0)])
    here = jnp.stack([upper * half + low, (1 - upper) * half + low, shell, 1 - shell, low, upper]).astype(jnp.int32)

    def pack(which, lists, spare):
        count = lists.shape[1]
        return pl.pallas_call(
            partial(pack_kernel, half, cap, per_owner, which),
            in_specs=[SMEM, SMEM, VMEM],
            out_specs=VMEM,
            out_shape=jax.ShapeDtypeStruct((groups, count * lines + spare, TC), jnp.float32),
            scratch_shapes=[pltpu.SMEM((groups,), jnp.int32)] * count,
            compiler_params=room(12),
            name="pack",
        )(here, block_tile, lists)

    near = cube_exchange(pack(0, raw, 8))
    far_second = lax.ppermute(near[:, lines:, :], "upper", [(0, 1), (1, 0)])
    far_first = cube_exchange(pack(1, raw_far, 0))

    note = jnp.concatenate(
        [block_tile.astype(jnp.float32), plane_coef[:, None], (plane_coef * plane_dist)[:, None], source_inv[:, None]],
        axis=1,
    )
    other = lax.ppermute(note, "shell", [(0, 1), (1, 0)])
    both = jnp.where(shell == 0, jnp.concatenate([note, other]), jnp.concatenate([other, note]))
    tiles = slot_tiles(
        both[:, : groups * local_tiles].astype(jnp.int32).reshape(2 * planes, groups, local_tiles), held, per_owner, cap
    )
    tiles = tiles.reshape(2 * planes, 2, half, cap)
    near_slots = lax.dynamic_index_in_dim(tiles, upper, axis=1, keepdims=False).reshape(-1)
    far_slots = lax.dynamic_index_in_dim(tiles, 1 - upper, axis=1, keepdims=False).reshape(-1)
    maps = jnp.arange(2 * planes)
    weight = jnp.where(
        maps[None, :] <= maps[:, None], both[None, :, -3] - both[:, -1][:, None] * both[None, :, -2], 0.0
    )
    weight = jnp.concatenate([weight, jnp.sum(weight, axis=1, keepdims=True)], axis=1)

    filters = pl.pallas_call(
        partial(filters_kernel, L),
        grid=(2,),
        in_specs=[SMEM],
        out_specs=pl.BlockSpec((1, 2, outer, slab, TC), lambda step: (step, 0, 0, 0, 0)),
        out_shape=pltpu.HBM((2, 2, outer, slab, TC), jnp.float32),
        compiler_params=room(16),
        name="filters",
    )(here)
    near_dens = pl.pallas_call(
        partial(deposit_kernel, cap, chunks),
        in_specs=[SMEM, VMEM],
        out_specs=VMEM,
        out_shape=pltpu.HBM((2 * planes, per_owner, TR, TC), jnp.float32),
        compiler_params=room(16),
        name="deposit",
    )(near_slots, near)
    first_dens = pl.pallas_call(
        partial(deposit_first_kernel, cap, chunks),
        in_specs=[SMEM, VMEM],
        out_specs=VMEM,
        out_shape=pltpu.HBM((planes, per_owner, TR, TC), jnp.float32),
        compiler_params=room(16),
        name="deposit_first",
    )(far_slots, far_first)
    twiddle = jnp.asarray(twiddle_pair(outer, TC))
    turn = jnp.asarray(twiddle_pair(outer, TC).transpose(0, 2, 1))
    minus = jnp.asarray(dft_block(TC, -1.0))
    plus = jnp.asarray(dft_block(TC, 1.0))
    field = jax.ShapeDtypeStruct((planes, slab, L), jnp.float32)
    some = 2 * TR
    conv_mine, conv_other, row_sent = pl.pallas_call(
        partial(rows_kernel, cap, chunks),
        grid=(slab // some,),
        in_specs=[
            SMEM,
            SMEM,
            SMEM,
            pl.BlockSpec(memory_space=pltpu.HBM),
            pl.BlockSpec(memory_space=pltpu.HBM),
            pl.BlockSpec((groups, 8, TC), lambda step: (0, planes * lines // 8, 0)),
            whole(far_second.shape),
            whole(twiddle.shape),
            whole(minus.shape),
        ],
        out_specs=(
            pl.BlockSpec((planes, some, L), lambda step: (0, step, 0)),
            pl.BlockSpec((planes, some, L), lambda step: (0, step, 0)),
            pl.BlockSpec((groups, 2, 2, some, TC), lambda step: (0, 0, 0, step, 0)),
        ),
        out_shape=(
            pltpu.HBM(field.shape, field.dtype),
            pltpu.HBM(field.shape, field.dtype),
            pltpu.HBM((groups, 2, 2, slab, TC), jnp.float32),
        ),
        scratch_shapes=[
            pltpu.VMEM((2, outer * some, 2 * TC), jnp.bfloat16),
            pltpu.VMEM((2, outer * some, 2 * TC), jnp.bfloat16),
            pltpu.VMEM((planes, per_owner, TR, TC), jnp.float32),
            pltpu.VMEM((2 * planes, per_owner, TR, TC), jnp.float32),
            pltpu.VMEM((planes, per_owner, TR, TC), jnp.float32),
            pltpu.VMEM((2 * planes, some // TR * outer, TR, TC), jnp.float32),
            pltpu.SemaphoreType.DMA(()),
            pltpu.SemaphoreType.DMA(()),
        ],
        compiler_params=room(28),
        name="rows",
    )(weight, here, far_slots, in_hbm(near_dens), in_hbm(first_dens), near, far_second, twiddle, minus)
    arrived = lax.all_to_all(row_sent, ("shell", "low"), split_axis=0, concat_axis=0, tiled=True)
    swaps = []
    for side in range(2):
        for top in range(2):
            for at in range(half):
                if (side + at) % 2 == top:
                    swaps.append(((side * 2 + top) * half + at, ((1 - side) * 2 + top) * half + at))
    conv_held = lax.ppermute(conv_other, ("shell", "upper", "low"), swaps)
    convergence = jnp.where(part == upper, conv_mine, conv_held)
    col_sent = pl.pallas_call(
        partial(columns_kernel, order),
        grid=(2,),
        in_specs=[
            pl.BlockSpec(memory_space=pltpu.HBM),
            pl.BlockSpec((groups, 1, 2, slab, TC), lambda step: (0, step, 0, 0, 0)),
            whole(turn.shape),
            whole(plus.shape),
            whole(minus.shape),
        ],
        out_specs=pl.BlockSpec((half, 1, 2, 2, slab, TC), lambda step: (0, step, 0, 0, 0, 0)),
        out_shape=pltpu.HBM((half, 2, 2, 2, slab, TC), jnp.float32),
        scratch_shapes=[
            pltpu.VMEM((2 * slab, L), jnp.bfloat16),
            pltpu.VMEM((2 * slab, L), jnp.bfloat16),
            pltpu.VMEM((2 * slab, L), jnp.float32),
            pltpu.VMEM((outer, 2 * slab, 2 * TC), jnp.float32),
            pltpu.VMEM((2, outer, slab, TC), jnp.float32),
            pltpu.SemaphoreType.DMA(()),
        ],
        compiler_params=room(32),
        name="columns",
    )(in_hbm(filters), arrived, turn, plus, minus)
    landed = lax.all_to_all(col_sent, "low", split_axis=0, concat_axis=0, tiled=True)
    shear_one, shear_two = pl.pallas_call(
        inverse_rows_kernel,
        grid=(slab // some,),
        in_specs=[
            pl.BlockSpec((half, 2, 2, 2, some, TC), lambda step: (0, 0, 0, 0, step, 0)),
            whole(twiddle.shape),
            whole(plus.shape),
        ],
        out_specs=(
            pl.BlockSpec((planes, some, L), lambda step: (0, step, 0)),
            pl.BlockSpec((planes, some, L), lambda step: (0, step, 0)),
        ),
        out_shape=(field, field),
        scratch_shapes=[pltpu.VMEM((outer * some, 2 * TC), jnp.float32)],
        compiler_params=room(24),
        name="inverse_rows",
    )(landed, twiddle, plus)
    return (convergence, shear_one, shear_two)


def solution(mesh):
    shells, groups = (mesh.shape["shell"], mesh.shape["pix"])
    body, pix = (local, "pix")
    if shells == 2 and groups * TC == L:
        body, pix = (local_cube, ("upper", "low"))
        mesh = type(mesh)(mesh.devices.reshape(shells, 2, groups // 2), ("shell", "upper", "low"))
    placed = (P("shell", None), P("shell", pix, None), P("shell", pix, None), P("shell"), P("shell"), P("shell"))
    out = P("shell", pix, None)

    def step(*arrays):
        return body(*arrays)

    return jax.shard_map(step, mesh=mesh, in_specs=placed, out_specs=(out, out, out), check_vma=False)
```
